8 devices in a mesh: dp: 1 (over z), tp: 8 (over y, x, core).
Axes of the slice: x: 2, y: 2, z: 1, core: 2. Of those that a mesh axis runs over, the one named last changes fastest.
Arguments:
- x_in: bfloat16 [1536, 2048], P('dp')
- g_norm: bfloat16 [2048], replicated
- w_q: bfloat16 [2048, 2048], P(None, 'tp')
- w_k: bfloat16 [2048, 1024], replicated
- w_v: bfloat16 [2048, 1024], replicated
- w_o: bfloat16 [2048, 2048], P('tp')
- w_gate: bfloat16 [2048, 6144], P(None, 'tp')
- w_up: bfloat16 [2048, 6144], P(None, 'tp')
- w_down: bfloat16 [6144, 2048], P('tp')
Outputs:
- output 1: bfloat16 [1536, 2048], P('dp')
- output 2: bfloat16 [1536, 8, 128], P('dp', 'tp')
- output 3: bfloat16 [1536, 8, 128], P('dp', 'tp')
All inputs are finite; a program needn't handle non-finite values.
Results may differ from the reference program's by a relative error of at most 0.0113708.
Values are sent between devices in bfloat16 or wider.
A program may use at most 1 GiB of HBM per device.

```python
import math
import jax
import jax.numpy as jnp
from jax import lax

TOKENS = 1536
D = 2048
HEADS = 16
KV_HEADS = 8
HEAD = 128
FF = 6144
KV_SLOTS = 8
QBLOCK = 128

ROPE_BASE = 500000.0
NORM_EPS = 1e-5


def setup_inputs(seed: int = 0, part: int = 0) -> dict:
    key_list = jax.random.split(jax.random.key(seed), 10)
    part_key = jax.random.fold_in(key_list[9], part)
    q_gain = math.sqrt(math.log(TOKENS / 16.0)) / 1.09
    x_val = 0.7 * jax.random.normal(part_key, (TOKENS, D), jnp.float32)
    g_val = jnp.exp(0.7 * jax.random.normal(key_list[0], (D,), jnp.float32) - 0.49)
    w_q = jax.random.normal(key_list[1], (D, HEADS * HEAD), jnp.float32) * (q_gain / math.sqrt(D))
    w_k = jax.random.normal(key_list[2], (D, KV_HEADS * HEAD), jnp.float32) / math.sqrt(D)
    w_v = jax.random.normal(key_list[3], (D, KV_HEADS * HEAD), jnp.float32) / math.sqrt(D)
    w_o = jax.random.normal(key_list[4], (HEADS * HEAD, D), jnp.float32) * (3.0 / math.sqrt(HEADS * HEAD))
    w_gate = jax.random.normal(key_list[5], (D, FF), jnp.float32) / math.sqrt(D)
    w_up = jax.random.normal(key_list[6], (D, FF), jnp.float32) / math.sqrt(D)
    w_down = jax.random.normal(key_list[7], (FF, D), jnp.float32) / math.sqrt(FF)
    return {'x_in': x_val.astype(jnp.bfloat16), 'g_norm': g_val.astype(jnp.bfloat16), 'w_q': w_q.astype(jnp.bfloat16), 'w_k': w_k.astype(jnp.bfloat16), 'w_v': w_v.astype(jnp.bfloat16), 'w_o': w_o.astype(jnp.bfloat16), 'w_gate': w_gate.astype(jnp.bfloat16), 'w_up': w_up.astype(jnp.bfloat16), 'w_down': w_down.astype(jnp.bfloat16)}


def rope_tables(positions):
    inv_freq = ROPE_BASE ** (-jnp.arange(0, HEAD, 2, dtype=jnp.float32) / HEAD)
    angles = positions.astype(jnp.float32)[:, None] * inv_freq[None, :]
    return jnp.cos(angles), jnp.sin(angles)


def apply_rope(projected, cos_tab, sin_tab):
    half_dim = HEAD // 2
    lower_half = projected[..., :half_dim]
    upper_half = projected[..., half_dim:]
    cos_b = cos_tab[:, None, :]
    sin_b = sin_tab[:, None, :]
    return jnp.concatenate([lower_half * cos_b - upper_half * sin_b, upper_half * cos_b + lower_half * sin_b], axis=-1)


def reference(x_in, g_norm, w_q, w_k, w_v, w_o, w_gate, w_up, w_down):
    x_f32 = x_in.astype(jnp.float32)
    inv_rms = lax.rsqrt(jnp.mean(x_f32 * x_f32, axis=-1, keepdims=True) + NORM_EPS)
    normed = (x_f32 * inv_rms * g_norm.astype(jnp.float32)).astype(jnp.bfloat16)
    cos_tab, sin_tab = rope_tables(jnp.arange(TOKENS))
    q_proj = jnp.dot(normed, w_q, preferred_element_type=jnp.float32).reshape(TOKENS, HEADS, HEAD)
    k_proj = jnp.dot(normed, w_k, preferred_element_type=jnp.float32).reshape(TOKENS, KV_HEADS, HEAD)
    q_rot = apply_rope(q_proj, cos_tab, sin_tab).astype(jnp.bfloat16)
    k_rot = apply_rope(k_proj, cos_tab, sin_tab).astype(jnp.bfloat16)
    v_proj = jnp.dot(normed, w_v, preferred_element_type=jnp.float32).astype(jnp.bfloat16).reshape(TOKENS, KV_HEADS, HEAD)
    group_size = HEADS // KV_HEADS
    q_grouped = q_rot.reshape(TOKENS, KV_HEADS, group_size, HEAD)
    k_f32 = k_rot.astype(jnp.float32)
    v_f32 = v_proj.astype(jnp.float32)
    score_scale = 1.0 / math.sqrt(HEAD)
    key_pos = jnp.arange(TOKENS)

    def attend_block(block_idx):
        row_start = block_idx * QBLOCK
        q_part = lax.dynamic_slice_in_dim(q_grouped, row_start, QBLOCK, axis=0).astype(jnp.float32)
        scores = jnp.einsum('qgrd,kgd->grqk', q_part, k_f32) * score_scale
        query_pos = row_start + jnp.arange(QBLOCK)
        visible = key_pos[None, :] <= query_pos[:, None]
        scores = jnp.where(visible, scores, -1e30)
        probs = jax.nn.softmax(scores, axis=-1).astype(jnp.bfloat16).astype(jnp.float32)
        return jnp.einsum('grqk,kgd->qgrd', probs, v_f32).astype(jnp.bfloat16)

    attn_blocks = lax.map(attend_block, jnp.arange(TOKENS // QBLOCK))
    attn_out = attn_blocks.reshape(TOKENS, HEADS * HEAD)
    attn_sum = jnp.dot(attn_out, w_o, preferred_element_type=jnp.float32)
    gate_proj = jnp.dot(normed, w_gate, preferred_element_type=jnp.float32)
    up_proj = jnp.dot(normed, w_up, preferred_element_type=jnp.float32)
    hidden = (jax.nn.silu(gate_proj) * up_proj).astype(jnp.bfloat16)
    mlp_sum = jnp.dot(hidden, w_down, preferred_element_type=jnp.float32)
    y_out = (x_f32 + attn_sum + mlp_sum).astype(jnp.bfloat16)
    slot_repeat = KV_SLOTS // KV_HEADS
    k_cache = jnp.repeat(k_rot, slot_repeat, axis=1)
    v_cache = jnp.repeat(v_proj, slot_repeat, axis=1)
    return (y_out, k_cache, v_cache)
```

```python
import math
import numpy as np
import jax
import jax.numpy as jnp
from jax import lax
from jax.experimental import pallas as pl
from jax.experimental.pallas import tpu as pltpu
from jax.sharding import PartitionSpec as P

HEAD_DIM = 128
ROPE_BASE = 500000.0
NORM_EPS = 1e-5
TOKENS = 1536
WIDTH = 2048
QCOLS = 256
FFCOLS = 768
ROWS = 256
BLOCKS = TOKENS // ROWS
KDOWN = QCOLS + FFCOLS
LAG_B, LAG_C, LAG_D, LAG_E, LAG_F = 1, 2, 3, 4, 5
SCORE_SCALE = math.log2(math.e) / math.sqrt(HEAD_DIM)
F32 = jnp.float32
BF16 = jnp.bfloat16
MESH = pl.DeviceIdType.MESH

D2D_FIRST, D2D_SECOND, RED_ONE, RED_TWO, GAT_ONE, GAT_TWO, OUT_FIRST, OUT_SECOND = range(8)


def rope_tables():
    inv_freq = np.float32(ROPE_BASE) ** (-np.arange(0, HEAD_DIM, 2, dtype=np.float32) / np.float32(HEAD_DIM))
    angles = np.arange(TOKENS, dtype=np.float32)[:, None] * inv_freq.astype(np.float32)[None, :]
    cos, sin = np.cos(angles.astype(np.float64)), np.sin(angles.astype(np.float64))
    return (np.concatenate([cos, cos], axis=1).astype(np.float32), np.concatenate([-sin, sin], axis=1).astype(np.float32))


def layer_kernel(x_hbm, g_hbm, wq_hbm, wk_hbm, wv_hbm, wo_hbm, wg_hbm, wu_hbm, wd_hbm, cos_hbm, sin_hbm,
                 y_out, k_out, v_out,
                 x_v, g_v, wqkv_v, wg_v, wu_v, wod_v, cos_v, sin_v,
                 a_v, q_v, k_v, v_v, s_v, m_v, l_v, acc_v, om_v,
                 d2d_src, d2d_dst, h_send, h_keep, r1_dst, p_send, p_keep, r2_dst, y_v,
                 x_sem, w_sem, o_sem, kv_sem, ssem, rsem):
    me = lax.axis_index('tp')
    core = lax.rem(me, 2)
    xpos = lax.rem(me // 2, 2)
    ypos = me // 4
    sibling = me + 1 - 2 * core
    xpeer = me + 2 - 4 * xpos
    ypeer = me + 4 - 8 * ypos
    p1 = xpos + core * (ypos - xpos)
    p2 = ypos + core * (xpos - ypos)
    n1 = xpeer + core * (ypeer - xpeer)
    n2 = ypeer + core * (xpeer - ypeer)

    def rows_of(b):
        return pl.ds(pl.multiple_of(b * ROWS, ROWS), ROWS)

    def load_x(b):
        return pltpu.make_async_copy(x_hbm.at[rows_of(b), :], x_v.at[rows_of(b), :], x_sem.at[b])

    kv_cols = pl.ds(pl.multiple_of(me * HEAD_DIM, HEAD_DIM), HEAD_DIM)
    loads = [
        pltpu.make_async_copy(g_hbm, g_v, w_sem.at[0]),
        pltpu.make_async_copy(wk_hbm.at[:, kv_cols], wqkv_v.at[:, pl.ds(QCOLS, HEAD_DIM)], w_sem.at[1]),
        pltpu.make_async_copy(wv_hbm.at[:, kv_cols], wqkv_v.at[:, pl.ds(QCOLS + HEAD_DIM, HEAD_DIM)], w_sem.at[2]),
        pltpu.make_async_copy(wq_hbm, wqkv_v.at[:, pl.ds(0, QCOLS)], w_sem.at[3]),
        pltpu.make_async_copy(cos_hbm, cos_v, w_sem.at[4]),
        pltpu.make_async_copy(sin_hbm, sin_v, w_sem.at[5]),
        pltpu.make_async_copy(wg_hbm, wg_v, w_sem.at[6]),
        pltpu.make_async_copy(wu_hbm, wu_v, w_sem.at[7]),
        pltpu.make_async_copy(wo_hbm, wod_v.at[pl.ds(0, QCOLS), :], w_sem.at[8]),
        pltpu.make_async_copy(wd_hbm, wod_v.at[pl.ds(QCOLS, FFCOLS), :], w_sem.at[9]),
    ]
    load_x(0).start()
    for copy in loads:
        copy.start()
    for b in range(1, BLOCKS):
        load_x(b).start()

    barrier = pltpu.get_barrier_semaphore()
    for peer in (sibling, xpeer, ypeer):
        pl.semaphore_signal(barrier, inc=1, device_id={'tp': peer}, device_id_type=MESH)

    def remote(kind, b, src, dst, peer):
        return pltpu.make_async_remote_copy(src_ref=src, dst_ref=dst, send_sem=ssem.at[kind, b], recv_sem=rsem.at[kind, b],
                                            device_id={'tp': peer}, device_id_type=MESH)

    mine = core * 4 + p1 * 2
    other = core * 4 + (1 - p1) * 2

    def copy_of(kind, b):
        if kind == D2D_FIRST or kind == D2D_SECOND:
            return remote(kind, b, d2d_src.at[b, kind], d2d_dst.at[b, kind], sibling)
        if kind == RED_ONE:
            return remote(kind, b, h_send.at[b], r1_dst.at[b], n1)
        if kind == RED_TWO:
            return remote(kind, b, p_send.at[b], r2_dst.at[b], n2)
        if kind == GAT_ONE:
            piece = mine + p2
            return remote(kind, b, y_v.at[b, piece], y_v.at[b, piece], n2)
        if kind == GAT_TWO:
            return remote(kind, b, y_v.at[b, pl.ds(mine, 2)], y_v.at[b, pl.ds(mine, 2)], n1)
        first = mine if kind == OUT_FIRST else other
        return remote(kind, b, y_v.at[b, pl.ds(first, 2)], y_v.at[b, pl.ds(first, 2)], sibling)

    def store_y(b, piece):
        return pltpu.make_async_copy(y_v.at[b, piece], y_out.at[rows_of(b), pl.ds(pl.multiple_of(piece * 256, 256), 256)],
                                     o_sem.at[b, piece])

    def store_kv(b):
        return (pltpu.make_async_copy(k_v.at[rows_of(b), :], k_out.at[rows_of(b), :], kv_sem.at[0, b]),
                pltpu.make_async_copy(v_v.at[rows_of(b), :], v_out.at[rows_of(b), :], kv_sem.at[1, b]))

    def project(b):
        load_x(b).wait()

        @pl.when(b == 0)
        def _():
            for copy in loads[:1]:
                copy.wait()

        def norm_rows(r, carry):
            sl = pl.ds(pl.multiple_of(b * ROWS + r * 16, 16), 16)
            x_f = x_v[sl, :].astype(F32)
            inv = lax.rsqrt(jnp.mean(x_f * x_f, axis=-1, keepdims=True) + NORM_EPS)
            a_v[pl.ds(pl.multiple_of(r * 16, 16), 16), :] = (x_f * inv * g_v[...].astype(F32)).astype(BF16)
            return carry

        lax.fori_loop(0, ROWS // 16, norm_rows, 0, unroll=4)

        @pl.when(b == 0)
        def _():
            for copy in loads[1:6]:
                copy.wait()

        cos, sin = cos_v[rows_of(b), :], sin_v[rows_of(b), :]
        qkv = jnp.dot(a_v[...], wqkv_v[...], preferred_element_type=F32)

        def rope(h):
            return (h * cos + pltpu.roll(h, HEAD_DIM // 2, 1) * sin).astype(BF16)

        q_v[pl.ds(0, ROWS), :] = rope(qkv[:, 0:128])
        q_v[pl.ds(ROWS, ROWS), :] = rope(qkv[:, 128:256])
        k_v[rows_of(b), :] = rope(qkv[:, 256:384])
        v_v[rows_of(b), :] = qkv[:, 384:512].astype(BF16)
        for copy in store_kv(b):
            copy.start()

    def attend(b):
        def tile(j):
            return pl.ds(pl.multiple_of(j * ROWS, ROWS), ROWS)

        def scores(j):
            s = lax.dot_general(q_v[...], k_v[tile(j), :], (((1,), (1,)), ((), ())), preferred_element_type=F32)
            return s * SCORE_SCALE

        qpos = lax.broadcasted_iota(jnp.int32, (2 * ROWS, ROWS), 0)
        kpos = lax.broadcasted_iota(jnp.int32, (2 * ROWS, ROWS), 1)
        t = jnp.where(kpos <= lax.rem(qpos, ROWS), scores(b), -1e30)
        s_v[:, tile(b)] = t
        m_v[...] = jnp.maximum(t[:, :128], t[:, 128:])

        def score_tile(j, carry):
            t = scores(j)
            s_v[:, tile(j)] = t
            m_v[...] = jnp.maximum(m_v[...], jnp.maximum(t[:, :128], t[:, 128:]))
            return carry

        lax.fori_loop(0, b, score_tile, 0)
        m_v[...] = jnp.broadcast_to(jnp.max(m_v[...], axis=1, keepdims=True), (2 * ROWS, 128))
        l_v[...] = jnp.zeros_like(l_v)

        def exp_tile(j, carry):
            m = m_v[...]
            e0 = jnp.exp2(s_v[:, pl.ds(pl.multiple_of(j * ROWS, ROWS), 128)] - m)
            e1 = jnp.exp2(s_v[:, pl.ds(pl.multiple_of(j * ROWS + 128, 128), 128)] - m)
            s_v[:, pl.ds(pl.multiple_of(j * ROWS, ROWS), 128)] = e0
            s_v[:, pl.ds(pl.multiple_of(j * ROWS + 128, 128), 128)] = e1
            l_v[...] += e0 + e1
            return carry

        lax.fori_loop(0, b + 1, exp_tile, 0)
        l_v[...] = jnp.broadcast_to(1.0 / jnp.sum(l_v[...], axis=1, keepdims=True), (2 * ROWS, 128))
        acc_v[...] = jnp.zeros_like(acc_v)

        def value_tile(j, carry):
            r = l_v[...]
            p = (s_v[:, tile(j)] * jnp.concatenate([r, r], axis=1)).astype(BF16)
            acc_v[...] += jnp.dot(p, v_v[tile(j), :], preferred_element_type=F32)
            return carry

        lax.fori_loop(0, b + 1, value_tile, 0)
        om_v[:, 0:128] = acc_v[0:ROWS, :].astype(BF16)
        om_v[:, 128:256] = acc_v[ROWS:, :].astype(BF16)

    def gate_up(b):
        @pl.when(b == 0)
        def _():
            for copy in loads[6:8]:
                copy.wait()

        for n in range(FFCOLS // 256):
            cols = pl.ds(n * 256, 256)
            gate = jnp.dot(a_v[...], wg_v[:, cols], preferred_element_type=F32)
            up = jnp.dot(a_v[...], wu_v[:, cols], preferred_element_type=F32)
            om_v[:, pl.ds(QCOLS + n * 256, 256)] = (gate * (1.0 / (1.0 + jnp.exp(-gate))) * up).astype(BF16)

    def down(half, quarter):
        cols = pl.ds(pl.multiple_of(half * 1024 + quarter * 512, 512), 512)
        return jnp.dot(om_v[...], wod_v[:, cols], preferred_element_type=F32)

    def down_other(b):
        @pl.when(b == 0)
        def _():
            for copy in loads[8:10]:
                copy.wait()
            pl.semaphore_wait(barrier, 3)

        d2d_src[b, 0] = down(1 - core, 1 - p2).astype(BF16)
        copy_of(D2D_FIRST, b).start()
        d2d_src[b, 1] = down(1 - core, p2).astype(BF16)
        copy_of(D2D_SECOND, b).start()

    def down_mine(b):
        part = down(core, 1 - p1)
        copy_of(D2D_FIRST, b).wait_recv()
        h_send[b] = (part + d2d_dst[b, 0].astype(F32)).astype(BF16)
        copy_of(RED_ONE, b).start()
        part = down(core, p1)
        copy_of(D2D_SECOND, b).wait_recv()
        h_keep[b] = part + d2d_dst[b, 1].astype(F32)

    def stage_b(b):
        copy_of(RED_ONE, b).wait_recv()
        send = pl.ds(pl.multiple_of((1 - p2) * 256, 256), 256)
        keep = pl.ds(pl.multiple_of(p2 * 256, 256), 256)
        p_send[b] = (h_keep[b, :, send] + r1_dst[b, :, send].astype(F32)).astype(BF16)
        copy_of(RED_TWO, b).start()
        p_keep[b] = h_keep[b, :, keep] + r1_dst[b, :, keep].astype(F32)

    def stage_c(b):
        copy_of(RED_TWO, b).wait_recv()
        piece = mine + p2
        x_f = x_v[rows_of(b), pl.ds(pl.multiple_of(piece * 256, 256), 256)].astype(F32)
        y_v[b, piece] = (x_f + (p_keep[b] + r2_dst[b].astype(F32))).astype(BF16)
        copy_of(GAT_ONE, b).start()
        store_y(b, piece).start()

    def stage_d(b):
        copy_of(GAT_ONE, b).wait_recv()
        copy_of(GAT_TWO, b).start()
        copy_of(OUT_FIRST, b).start()
        store_y(b, mine + 1 - p2).start()

    def stage_e(b):
        copy_of(GAT_TWO, b).wait_recv()
        copy_of(OUT_SECOND, b).start()
        store_y(b, other).start()
        store_y(b, other + 1).start()

    def stage_f(b):
        copy_of(OUT_FIRST, b).wait_recv()
        copy_of(OUT_SECOND, b).wait_recv()
        for piece in range(4):
            store_y(b, (1 - core) * 4 + piece).start()

    def when_block(b, stage):
        @pl.when((b >= 0) & (b < BLOCKS))
        def _():
            stage(b)

    def step(i, carry):
        @pl.when(i < BLOCKS)
        def _():
            project(i)
            attend(i)
            gate_up(i)
            down_other(i)

        when_block(i - LAG_B, stage_b)
        when_block(i - LAG_C, stage_c)
        when_block(i - LAG_D, stage_d)

        @pl.when(i < BLOCKS)
        def _():
            down_mine(i)

        when_block(i - LAG_E, stage_e)
        when_block(i - LAG_F, stage_f)
        return carry

    lax.fori_loop(0, BLOCKS + LAG_F, step, 0)

    def finish(b, carry):
        for kind in range(8):
            copy_of(kind, b).wait_send()
        for piece in range(8):
            store_y(b, piece).wait()
        for copy in store_kv(b):
            copy.wait()
        return carry

    lax.fori_loop(0, BLOCKS, finish, 0)


def solution(mesh):
    cos_np, sin_np = rope_tables()

    def local_layer(x_in, g_norm, w_q, w_k, w_v, w_o, w_gate, w_up, w_down):
        any_spec = pl.BlockSpec(memory_space=pl.ANY)
        y, k, v = pl.pallas_call(
            layer_kernel,
            out_shape=(jax.ShapeDtypeStruct((TOKENS, WIDTH), BF16), jax.ShapeDtypeStruct((TOKENS, HEAD_DIM), BF16),
                       jax.ShapeDtypeStruct((TOKENS, HEAD_DIM), BF16)),
            in_specs=[any_spec] * 11,
            out_specs=(any_spec,) * 3,
            scratch_shapes=[
                pltpu.VMEM((TOKENS, WIDTH), BF16),
                pltpu.VMEM((1, WIDTH), BF16),
                pltpu.VMEM((WIDTH, QCOLS + 2 * HEAD_DIM), BF16),
                pltpu.VMEM((WIDTH, FFCOLS), BF16),
                pltpu.VMEM((WIDTH, FFCOLS), BF16),
                pltpu.VMEM((KDOWN, WIDTH), BF16),
                pltpu.VMEM((TOKENS, HEAD_DIM), F32),
                pltpu.VMEM((TOKENS, HEAD_DIM), F32),
                pltpu.VMEM((ROWS, WIDTH), BF16),
                pltpu.VMEM((2 * ROWS, HEAD_DIM), BF16),
                pltpu.VMEM((TOKENS, HEAD_DIM), BF16),
                pltpu.VMEM((TOKENS, HEAD_DIM), BF16),
                pltpu.VMEM((2 * ROWS, TOKENS), F32),
                pltpu.VMEM((2 * ROWS, 128), F32),
                pltpu.VMEM((2 * ROWS, 128), F32),
                pltpu.VMEM((2 * ROWS, HEAD_DIM), F32),
                pltpu.VMEM((ROWS, KDOWN), BF16),
                pltpu.VMEM((BLOCKS, 2, ROWS, 512), BF16),
                pltpu.VMEM((BLOCKS, 2, ROWS, 512), BF16),
                pltpu.VMEM((BLOCKS, ROWS, 512), BF16),
                pltpu.VMEM((BLOCKS, ROWS, 512), F32),
                pltpu.VMEM((BLOCKS, ROWS, 512), BF16),
                pltpu.VMEM((BLOCKS, ROWS, 256), BF16),
                pltpu.VMEM((BLOCKS, ROWS, 256), F32),
                pltpu.VMEM((BLOCKS, ROWS, 256), BF16),
                pltpu.VMEM((BLOCKS, 8, ROWS, 256), BF16),
                pltpu.SemaphoreType.DMA((BLOCKS,)),
                pltpu.SemaphoreType.DMA((10,)),
                pltpu.SemaphoreType.DMA((BLOCKS, 8)),
                pltpu.SemaphoreType.DMA((2, BLOCKS)),
                pltpu.SemaphoreType.DMA((8, BLOCKS)),
                pltpu.SemaphoreType.DMA((8, BLOCKS)),
            ],
            compiler_params=pltpu.CompilerParams(collective_id=0, has_side_effects=True, vmem_limit_bytes=67043328),
        )(x_in, g_norm.reshape(1, WIDTH), w_q, w_k, w_v, w_o, w_gate, w_up, w_down, jnp.asarray(cos_np), jnp.asarray(sin_np))
        return y, k.reshape(TOKENS, 1, HEAD_DIM), v.reshape(TOKENS, 1, HEAD_DIM)

    return jax.shard_map(local_layer, mesh=mesh, in_specs=(P('dp', None), P(None), P(None, 'tp'), P(None, None), P(None, None), P('tp', None), P(None, 'tp'), P(None, 'tp'), P('tp', None)), out_specs=(P('dp', None), P('dp', 'tp', None), P('dp', 'tp', None)), check_vma=False)
```

```python
import math
import numpy as np
import jax
import jax.numpy as jnp
from jax import lax
from jax.experimental import pallas as pl
from jax.experimental.pallas import tpu as pltpu
from jax.sharding import PartitionSpec as P

HEAD_DIM = 128
ROPE_BASE = 500000.0
NORM_EPS = 1e-5
TOKENS = 1536
WIDTH = 2048
QCOLS = 256
FFCOLS = 768
ROWS = 256
BLOCKS = TOKENS // ROWS
KDOWN = QCOLS + FFCOLS
LAG_B, LAG_C, LAG_D, LAG_E, LAG_F = 1, 2, 3, 4, 5
SCORE_SCALE = math.log2(math.e) / math.sqrt(HEAD_DIM)
F32 = jnp.float32
BF16 = jnp.bfloat16
MESH = pl.DeviceIdType.MESH

D2D_FIRST, D2D_SECOND, RED_ONE, RED_TWO, GAT_ONE, GAT_TWO, OUT_FIRST, OUT_SECOND = range(8)


def rope_tables():
    inv_freq = np.float32(ROPE_BASE) ** (-np.arange(0, HEAD_DIM, 2, dtype=np.float32) / np.float32(HEAD_DIM))
    angles = np.arange(TOKENS, dtype=np.float32)[:, None] * inv_freq.astype(np.float32)[None, :]
    cos, sin = np.cos(angles.astype(np.float64)), np.sin(angles.astype(np.float64))
    return (np.concatenate([cos, cos], axis=1).astype(np.float32), np.concatenate([-sin, sin], axis=1).astype(np.float32))


def layer_kernel(x_hbm, g_hbm, wq_hbm, wk_hbm, wv_hbm, wo_hbm, wg_hbm, wu_hbm, wd_hbm, cos_hbm, sin_hbm,
                 y_v, k_v, v_v,
                 x_v, g_v, wqkv_v, wg_v, wu_v, wod_v, cos_v, sin_v,
                 a_v, q_v, s_v, m_v, l_v, acc_v, om_v,
                 d2d_src, d2d_dst, h_send, h_keep, r1_dst, p_send, p_keep, r2_dst,
                 x_sem, w_sem, ssem, rsem):
    me = lax.axis_index('tp')
    core = lax.rem(me, 2)
    xpos = lax.rem(me // 2, 2)
    ypos = me // 4
    sibling = me + 1 - 2 * core
    xpeer = me + 2 - 4 * xpos
    ypeer = me + 4 - 8 * ypos
    p1 = xpos + core * (ypos - xpos)
    p2 = ypos + core * (xpos - ypos)
    n1 = xpeer + core * (ypeer - xpeer)
    n2 = ypeer + core * (xpeer - ypeer)

    def rows_of(b):
        return pl.ds(pl.multiple_of(b * ROWS, ROWS), ROWS)

    def load_x(b):
        return pltpu.make_async_copy(x_hbm.at[rows_of(b), :], x_v.at[rows_of(b), :], x_sem.at[b])

    kv_cols = pl.ds(pl.multiple_of(me * HEAD_DIM, HEAD_DIM), HEAD_DIM)
    loads = [
        pltpu.make_async_copy(g_hbm, g_v, w_sem.at[0]),
        pltpu.make_async_copy(wk_hbm.at[:, kv_cols], wqkv_v.at[:, pl.ds(QCOLS, HEAD_DIM)], w_sem.at[1]),
        pltpu.make_async_copy(wv_hbm.at[:, kv_cols], wqkv_v.at[:, pl.ds(QCOLS + HEAD_DIM, HEAD_DIM)], w_sem.at[2]),
        pltpu.make_async_copy(wq_hbm, wqkv_v.at[:, pl.ds(0, QCOLS)], w_sem.at[3]),
        pltpu.make_async_copy(cos_hbm, cos_v, w_sem.at[4]),
        pltpu.make_async_copy(sin_hbm, sin_v, w_sem.at[5]),
        pltpu.make_async_copy(wg_hbm, wg_v, w_sem.at[6]),
        pltpu.make_async_copy(wu_hbm, wu_v, w_sem.at[7]),
        pltpu.make_async_copy(wo_hbm, wod_v.at[pl.ds(0, QCOLS), :], w_sem.at[8]),
        pltpu.make_async_copy(wd_hbm, wod_v.at[pl.ds(QCOLS, FFCOLS), :], w_sem.at[9]),
    ]
    load_x(0).start()
    for copy in loads:
        copy.start()
    for b in range(1, BLOCKS):
        load_x(b).start()

    barrier = pltpu.get_barrier_semaphore()
    for peer in (sibling, xpeer, ypeer):
        pl.semaphore_signal(barrier, inc=1, device_id={'tp': peer}, device_id_type=MESH)

    def remote(kind, b, src, dst, peer):
        return pltpu.make_async_remote_copy(src_ref=src, dst_ref=dst, send_sem=ssem.at[kind, b], recv_sem=rsem.at[kind, b],
                                            device_id={'tp': peer}, device_id_type=MESH)

    mine = core * 4 + p1 * 2
    other = core * 4 + (1 - p1) * 2

    def y_part(b, piece, count):
        return y_v.at[rows_of(b), pl.ds(pl.multiple_of(piece * 256, 256), count * 256)]

    def copy_of(kind, b):
        if kind == D2D_FIRST or kind == D2D_SECOND:
            return remote(kind, b, d2d_src.at[b, kind], d2d_dst.at[b, kind], sibling)
        if kind == RED_ONE:
            return remote(kind, b, h_send.at[b], r1_dst.at[b], n1)
        if kind == RED_TWO:
            return remote(kind, b, p_send.at[b], r2_dst.at[b], n2)
        if kind == GAT_ONE:
            part = y_part(b, mine + p2, 1)
            return remote(kind, b, part, part, n2)
        if kind == GAT_TWO:
            part = y_part(b, mine, 2)
            return remote(kind, b, part, part, n1)
        part = y_part(b, mine if kind == OUT_FIRST else other, 2)
        return remote(kind, b, part, part, sibling)

    def project(b):
        load_x(b).wait()

        @pl.when(b == 0)
        def _():
            for copy in loads[:1]:
                copy.wait()

        def norm_rows(r, carry):
            sl = pl.ds(pl.multiple_of(b * ROWS + r * 16, 16), 16)
            x_f = x_v[sl, :].astype(F32)
            inv = lax.rsqrt(jnp.mean(x_f * x_f, axis=-1, keepdims=True) + NORM_EPS)
            a_v[pl.ds(pl.multiple_of(r * 16, 16), 16), :] = (x_f * inv * g_v[...].astype(F32)[None, :]).astype(BF16)
            return carry

        lax.fori_loop(0, ROWS // 16, norm_rows, 0, unroll=4)

        @pl.when(b == 0)
        def _():
            for copy in loads[1:6]:
                copy.wait()

        cos, sin = cos_v[rows_of(b), :], sin_v[rows_of(b), :]
        qkv = jnp.dot(a_v[...], wqkv_v[...], preferred_element_type=F32)

        def rope(h):
            return (h * cos + pltpu.roll(h, HEAD_DIM // 2, 1) * sin).astype(BF16)

        q_v[pl.ds(0, ROWS), :] = rope(qkv[:, 0:128])
        q_v[pl.ds(ROWS, ROWS), :] = rope(qkv[:, 128:256])
        k_v[rows_of(b), :] = rope(qkv[:, 256:384])
        v_v[rows_of(b), :] = qkv[:, 384:512].astype(BF16)

    def attend(b):
        def tile(j):
            return pl.ds(pl.multiple_of(j * ROWS, ROWS), ROWS)

        def scores(j):
            s = lax.dot_general(q_v[...], k_v[tile(j), :], (((1,), (1,)), ((), ())), preferred_element_type=F32)
            return s * SCORE_SCALE

        qpos = lax.broadcasted_iota(jnp.int32, (2 * ROWS, ROWS), 0)
        kpos = lax.broadcasted_iota(jnp.int32, (2 * ROWS, ROWS), 1)
        t = jnp.where(kpos <= lax.rem(qpos, ROWS), scores(b), -1e30)
        s_v[:, tile(b)] = t
        m_v[...] = jnp.maximum(t[:, :128], t[:, 128:])

        def score_tile(j, carry):
            t = scores(j)
            s_v[:, tile(j)] = t
            m_v[...] = jnp.maximum(m_v[...], jnp.maximum(t[:, :128], t[:, 128:]))
            return carry

        lax.fori_loop(0, b, score_tile, 0)
        m_v[...] = jnp.broadcast_to(jnp.max(m_v[...], axis=1, keepdims=True), (2 * ROWS, 128))
        l_v[...] = jnp.zeros_like(l_v)

        def exp_tile(j, carry):
            m = m_v[...]
            e0 = jnp.exp2(s_v[:, pl.ds(pl.multiple_of(j * ROWS, ROWS), 128)] - m)
            e1 = jnp.exp2(s_v[:, pl.ds(pl.multiple_of(j * ROWS + 128, 128), 128)] - m)
            s_v[:, pl.ds(pl.multiple_of(j * ROWS, ROWS), 128)] = e0
            s_v[:, pl.ds(pl.multiple_of(j * ROWS + 128, 128), 128)] = e1
            l_v[...] += e0 + e1
            return carry

        lax.fori_loop(0, b + 1, exp_tile, 0)
        l_v[...] = jnp.broadcast_to(1.0 / jnp.sum(l_v[...], axis=1, keepdims=True), (2 * ROWS, 128))
        acc_v[...] = jnp.zeros_like(acc_v)

        def value_tile(j, carry):
            r = l_v[...]
            p = (s_v[:, tile(j)] * jnp.concatenate([r, r], axis=1)).astype(BF16)
            acc_v[...] += jnp.dot(p, v_v[tile(j), :], preferred_element_type=F32)
            return carry

        lax.fori_loop(0, b + 1, value_tile, 0)
        om_v[:, 0:128] = acc_v[0:ROWS, :].astype(BF16)
        om_v[:, 128:256] = acc_v[ROWS:, :].astype(BF16)

    def gate_up(b):
        @pl.when(b == 0)
        def _():
            for copy in loads[6:8]:
                copy.wait()

        for n in range(FFCOLS // 256):
            cols = pl.ds(n * 256, 256)
            gate = jnp.dot(a_v[...], wg_v[:, cols], preferred_element_type=F32)
            up = jnp.dot(a_v[...], wu_v[:, cols], preferred_element_type=F32)
            om_v[:, pl.ds(QCOLS + n * 256, 256)] = (gate * (1.0 / (1.0 + jnp.exp(-gate))) * up).astype(BF16)

    def down(half, quarter):
        cols = pl.ds(pl.multiple_of(half * 1024 + quarter * 512, 512), 512)
        return jnp.dot(om_v[...], wod_v[:, cols], preferred_element_type=F32)

    def down_other(b):
        @pl.when(b == 0)
        def _():
            for copy in loads[8:10]:
                copy.wait()
            pl.semaphore_wait(barrier, 3)

        d2d_src[b, 0] = down(1 - core, 1 - p2).astype(BF16)
        copy_of(D2D_FIRST, b).start()
        d2d_src[b, 1] = down(1 - core, p2).astype(BF16)
        copy_of(D2D_SECOND, b).start()

    def down_mine(b):
        part = down(core, 1 - p1)
        copy_of(D2D_FIRST, b).wait_recv()
        h_send[b] = (part + d2d_dst[b, 0].astype(F32)).astype(BF16)
        copy_of(RED_ONE, b).start()
        part = down(core, p1)
        copy_of(D2D_SECOND, b).wait_recv()
        h_keep[b] = part + d2d_dst[b, 1].astype(F32)

    def stage_b(b):
        copy_of(RED_ONE, b).wait_recv()
        send = pl.ds(pl.multiple_of((1 - p2) * 256, 256), 256)
        keep = pl.ds(pl.multiple_of(p2 * 256, 256), 256)
        p_send[b] = (h_keep[b, :, send] + r1_dst[b, :, send].astype(F32)).astype(BF16)
        copy_of(RED_TWO, b).start()
        p_keep[b] = h_keep[b, :, keep] + r1_dst[b, :, keep].astype(F32)

    def stage_c(b):
        copy_of(RED_TWO, b).wait_recv()
        piece = mine + p2
        cols = pl.ds(pl.multiple_of(piece * 256, 256), 256)
        x_f = x_v[rows_of(b), cols].astype(F32)
        y_v[rows_of(b), cols] = (x_f + (p_keep[b] + r2_dst[b].astype(F32))).astype(BF16)
        copy_of(GAT_ONE, b).start()

    def stage_d(b):
        copy_of(GAT_ONE, b).wait_recv()
        copy_of(GAT_TWO, b).start()
        copy_of(OUT_FIRST, b).start()

    def stage_e(b):
        copy_of(GAT_TWO, b).wait_recv()
        copy_of(OUT_SECOND, b).start()

    def stage_f(b):
        copy_of(OUT_FIRST, b).wait_recv()
        copy_of(OUT_SECOND, b).wait_recv()

    def when_block(b, stage):
        @pl.when((b >= 0) & (b < BLOCKS))
        def _():
            stage(b)

    def step(i, carry):
        @pl.when(i < BLOCKS)
        def _():
            project(i)
            attend(i)
            gate_up(i)
            down_other(i)

        when_block(i - LAG_B, stage_b)
        when_block(i - LAG_C, stage_c)
        when_block(i - LAG_D, stage_d)

        @pl.when(i < BLOCKS)
        def _():
            down_mine(i)

        when_block(i - LAG_E, stage_e)
        when_block(i - LAG_F, stage_f)
        return carry

    lax.fori_loop(0, BLOCKS + LAG_F, step, 0)

    def finish(b, carry):
        for kind in range(8):
            copy_of(kind, b).wait_send()
        return carry

    lax.fori_loop(0, BLOCKS, finish, 0)


def solution(mesh):
    cos_np, sin_np = rope_tables()

    def local_layer(x_in, g_norm, w_q, w_k, w_v, w_o, w_gate, w_up, w_down):
        any_spec = pl.BlockSpec(memory_space=pl.ANY)
        y, k, v = pl.pallas_call(
            layer_kernel,
            out_shape=(pltpu.VMEM((TOKENS, WIDTH), BF16), pltpu.VMEM((TOKENS, HEAD_DIM), BF16), pltpu.VMEM((TOKENS, HEAD_DIM), BF16)),
            in_specs=[any_spec] * 11,
            out_specs=(pl.BlockSpec(memory_space=pltpu.VMEM),) * 3,
            scratch_shapes=[
                pltpu.VMEM((TOKENS, WIDTH), BF16),
                pltpu.VMEM((WIDTH,), BF16),
                pltpu.VMEM((WIDTH, QCOLS + 2 * HEAD_DIM), BF16),
                pltpu.VMEM((WIDTH, FFCOLS), BF16),
                pltpu.VMEM((WIDTH, FFCOLS), BF16),
                pltpu.VMEM((KDOWN, WIDTH), BF16),
                pltpu.VMEM((TOKENS, HEAD_DIM), F32),
                pltpu.VMEM((TOKENS, HEAD_DIM), F32),
                pltpu.VMEM((ROWS, WIDTH), BF16),
                pltpu.VMEM((2 * ROWS, HEAD_DIM), BF16),
                pltpu.VMEM((2 * ROWS, TOKENS), F32),
                pltpu.VMEM((2 * ROWS, 128), F32),
                pltpu.VMEM((2 * ROWS, 128), F32),
                pltpu.VMEM((2 * ROWS, HEAD_DIM), F32),
                pltpu.VMEM((ROWS, KDOWN), BF16),
                pltpu.VMEM((BLOCKS, 2, ROWS, 512), BF16),
                pltpu.VMEM((BLOCKS, 2, ROWS, 512), BF16),
                pltpu.VMEM((BLOCKS, ROWS, 512), BF16),
                pltpu.VMEM((BLOCKS, ROWS, 512), F32),
                pltpu.VMEM((BLOCKS, ROWS, 512), BF16),
                pltpu.VMEM((BLOCKS, ROWS, 256), BF16),
                pltpu.VMEM((BLOCKS, ROWS, 256), F32),
                pltpu.VMEM((BLOCKS, ROWS, 256), BF16),
                pltpu.SemaphoreType.DMA((BLOCKS,)),
                pltpu.SemaphoreType.DMA((10,)),
                pltpu.SemaphoreType.DMA((8, BLOCKS)),
                pltpu.SemaphoreType.DMA((8, BLOCKS)),
            ],
            compiler_params=pltpu.CompilerParams(collective_id=0, has_side_effects=True, vmem_limit_bytes=67043328 - 8 * 1024 * 1024),
        )(x_in, g_norm, w_q, w_k, w_v, w_o, w_gate, w_up, w_down, jnp.asarray(cos_np), jnp.asarray(sin_np))
        return y, k.reshape(TOKENS, 1, HEAD_DIM), v.reshape(TOKENS, 1, HEAD_DIM)

    return jax.shard_map(local_layer, mesh=mesh, in_specs=(P('dp', None), P(None), P(None, 'tp'), P(None, None), P(None, None), P('tp', None), P(None, 'tp'), P(None, 'tp'), P('tp', None)), out_specs=(P('dp', None), P('dp', 'tp', None), P('dp', 'tp', None)), check_vma=False)
```

```python
import math
import numpy as np
import jax
import jax.numpy as jnp
from jax import lax
from jax.experimental import pallas as pl
from jax.experimental.pallas import tpu as pltpu
from jax.sharding import PartitionSpec as P

HEAD_DIM = 128
ROPE_BASE = 500000.0
NORM_EPS = 1e-5
TOKENS = 1536
WIDTH = 2048
QCOLS = 256
FFCOLS = 768
ROWS = 256
BLOCKS = TOKENS // ROWS
KDOWN = QCOLS + FFCOLS
HALF = ROWS // 2
UNITS = TOKENS // HALF
STAGE_AT = (("b", (4, 4)), ("c", (7, 7)), ("d", (10, 10)), ("e", (19, 19)), ("f", (26, 26)))
DRAIN = 1 + max(max(at) for _, at in STAGE_AT) // 5
SCORE_SCALE = math.log2(math.e) / math.sqrt(HEAD_DIM)
F32 = jnp.float32
BF16 = jnp.bfloat16
MESH = pl.DeviceIdType.MESH

D2D_FIRST, D2D_SECOND, RED_ONE, RED_TWO, GAT_ONE, GAT_TWO, OUT_FIRST, OUT_SECOND = range(8)


def rope_tables():
    inv_freq = np.float32(ROPE_BASE) ** (-np.arange(0, HEAD_DIM, 2, dtype=np.float32) / np.float32(HEAD_DIM))
    angles = np.arange(TOKENS, dtype=np.float32)[:, None] * inv_freq.astype(np.float32)[None, :]
    cos, sin = np.cos(angles.astype(np.float64)), np.sin(angles.astype(np.float64))
    return (np.concatenate([cos, cos], axis=1).astype(np.float32), np.concatenate([-sin, sin], axis=1).astype(np.float32))


def layer_kernel(x_hbm, g_hbm, wq_hbm, wk_hbm, wv_hbm, wo_hbm, wg_hbm, wu_hbm, wd_hbm, cos_hbm, sin_hbm,
                 y_v, k_v, v_v,
                 x_v, g_v, gf_v, wqkv_v, wg_v, wu_v, wod_v, cos_v, sin_v,
                 a_v, q_v, s_v, p_v, om_v,
                 d2d_src, d2d_dst, h_send, h_keep, r1_dst, p_send, p_keep, r2_dst,
                 x_sem, w_sem, ssem, rsem):
    me = lax.axis_index('tp')
    core = lax.rem(me, 2)
    xpos = lax.rem(me // 2, 2)
    ypos = me // 4
    sibling = me + 1 - 2 * core
    xpeer = me + 2 - 4 * xpos
    ypeer = me + 4 - 8 * ypos
    p1 = xpos + core * (ypos - xpos)
    p2 = ypos + core * (xpos - ypos)
    n1 = xpeer + core * (ypeer - xpeer)
    n2 = ypeer + core * (xpeer - ypeer)

    def rows_of(b):
        return pl.ds(pl.multiple_of(b * ROWS, ROWS), ROWS)

    def load(src, dst, index):
        return pltpu.make_async_copy(src, dst, w_sem.at[index])

    def load_x(b):
        return pltpu.make_async_copy(x_hbm.at[rows_of(b), :], x_v.at[rows_of(b), :], x_sem.at[b])

    kv_cols = pl.ds(pl.multiple_of(me * HEAD_DIM, HEAD_DIM), HEAD_DIM)
    early, late = pl.ds(0, ROWS), pl.ds(ROWS, TOKENS - ROWS)
    load_g = load(g_hbm, g_v, 0)
    load_qkv = [
        load(wk_hbm.at[:, kv_cols], wqkv_v.at[:, pl.ds(QCOLS, HEAD_DIM)], 1),
        load(wv_hbm.at[:, kv_cols], wqkv_v.at[:, pl.ds(QCOLS + HEAD_DIM, HEAD_DIM)], 2),
        load(wq_hbm, wqkv_v.at[:, pl.ds(0, QCOLS)], 3),
        load(cos_hbm.at[early, :], cos_v.at[early, :], 4),
        load(sin_hbm.at[early, :], sin_v.at[early, :], 5),
    ]
    load_gu = []
    for n in range(FFCOLS // 256):
        tile = pl.ds(n * 256, 256)
        load_gu.append((load(wg_hbm.at[:, tile], wg_v.at[:, tile], 6 + 2 * n), load(wu_hbm.at[:, tile], wu_v.at[:, tile], 7 + 2 * n)))
    load_od = [load(wo_hbm, wod_v.at[pl.ds(0, QCOLS), :], 12), load(wd_hbm, wod_v.at[pl.ds(QCOLS, FFCOLS), :], 13)]
    load_tab = [load(cos_hbm.at[late, :], cos_v.at[late, :], 14), load(sin_hbm.at[late, :], sin_v.at[late, :], 15)]

    load_x(0).start()
    load_g.start()
    for copy in load_qkv:
        copy.start()

    barrier = pltpu.get_barrier_semaphore()
    for peer in (sibling, xpeer, ypeer):
        pl.semaphore_signal(barrier, inc=1, device_id={'tp': peer}, device_id_type=MESH)

    def remote(kind, u, src, dst, peer):
        return pltpu.make_async_remote_copy(src_ref=src, dst_ref=dst, send_sem=ssem.at[kind, u], recv_sem=rsem.at[kind, u],
                                            device_id={'tp': peer}, device_id_type=MESH)

    mine = core * 4 + p1 * 2
    other = core * 4 + (1 - p1) * 2

    def half_rows(u):
        return pl.ds(pl.multiple_of(u * HALF, HALF), HALF)

    def y_part(u, piece, count):
        return y_v.at[half_rows(u), pl.ds(pl.multiple_of(piece * 256, 256), count * 256)]

    def copy_of(kind, u):
        if kind == D2D_FIRST or kind == D2D_SECOND:
            return remote(kind, u, d2d_src.at[u, kind], d2d_dst.at[u, kind], sibling)
        if kind == RED_ONE:
            return remote(kind, u, h_send.at[u], r1_dst.at[u], n1)
        if kind == RED_TWO:
            return remote(kind, u, p_send.at[u], r2_dst.at[u], n2)
        if kind == GAT_ONE:
            part = y_part(u, mine + p2, 1)
            return remote(kind, u, part, part, n2)
        if kind == GAT_TWO:
            part = y_part(u, mine, 2)
            return remote(kind, u, part, part, n1)
        part = y_part(u, mine if kind == OUT_FIRST else other, 2)
        return remote(kind, u, part, part, sibling)

    def project(b):
        load_x(b).wait()

        @pl.when(b == 0)
        def _():
            load_g.wait()
            gf_v[...] = jnp.broadcast_to(g_v[...].astype(F32)[None, :], (8, WIDTH))
            for pair in load_gu:
                for copy in pair:
                    copy.start()

        def norm_rows(r, carry):
            x_f = x_v[pl.ds(pl.multiple_of(b * ROWS + r * 16, 16), 16), :].astype(F32)
            inv = lax.rsqrt(jnp.mean(x_f * x_f, axis=-1, keepdims=True) + NORM_EPS)
            gain = jnp.concatenate([gf_v[...], gf_v[...]], axis=0)
            a_v[pl.ds(pl.multiple_of(r * 16, 16), 16), :] = (x_f * inv * gain).astype(BF16)
            return carry

        lax.fori_loop(0, ROWS // 16, norm_rows, 0, unroll=4)

        @pl.when(b == 0)
        def _():
            for copy in load_od:
                copy.start()
            for copy in load_qkv:
                copy.wait()
            pl.semaphore_wait(barrier, 3)

        @pl.when(b == 1)
        def _():
            for copy in load_tab:
                copy.wait()

        cos, sin = cos_v[rows_of(b), :], sin_v[rows_of(b), :]
        qkv = jnp.dot(a_v[...], wqkv_v[...], preferred_element_type=F32)

        def rope(h):
            return (h * cos + pltpu.roll(h, HEAD_DIM // 2, 1) * sin).astype(BF16)

        q_v[pl.ds(0, ROWS), :] = rope(qkv[:, 0:128])
        q_v[pl.ds(ROWS, ROWS), :] = rope(qkv[:, 128:256])
        k_v[rows_of(b), :] = rope(qkv[:, 256:384])
        v_v[rows_of(b), :] = qkv[:, 384:512].astype(BF16)

    def attend(i):
        for b in range(BLOCKS):
            @pl.when(i == b)
            def _():
                attend_block(b)

    def attend_block(b):
        def tile(j):
            return pl.ds(j * ROWS, ROWS)

        for h in range(2):
            q = q_v[pl.ds(h * ROWS, ROWS), :]
            peak = None
            for j in range(b + 1):
                s = lax.dot_general(q, k_v[tile(j), :], (((1,), (1,)), ((), ())), preferred_element_type=F32) * SCORE_SCALE
                if j == b:
                    qpos = lax.broadcasted_iota(jnp.int32, (ROWS, ROWS), 0)
                    kpos = lax.broadcasted_iota(jnp.int32, (ROWS, ROWS), 1)
                    s = jnp.where(kpos <= qpos, s, -1e30)
                s_v[h, :, tile(j)] = s
                pair = jnp.maximum(s[:, :128], s[:, 128:])
                peak = pair if peak is None else jnp.maximum(peak, pair)
            peak = jnp.max(peak, axis=1, keepdims=True)
            total = None
            for j in range(b + 1):
                e = jnp.exp2(s_v[h, :, tile(j)] - peak)
                pair = e[:, :128] + e[:, 128:]
                total = pair if total is None else total + pair
            shift = peak + jnp.log2(jnp.sum(total, axis=1, keepdims=True))
            for j in range(b + 1):
                p_v[h, :, tile(j)] = jnp.exp2(s_v[h, :, tile(j)] - shift).astype(BF16)
            keys = pl.ds(0, (b + 1) * ROWS)
            o = jnp.dot(p_v[h, :, keys], v_v[keys, :], preferred_element_type=F32)
            om_v[:, pl.ds(h * HEAD_DIM, HEAD_DIM)] = o.astype(BF16)

    def gate_up(b):
        for n in range(FFCOLS // 256):
            @pl.when(b == 0)
            def _():
                for copy in load_gu[n]:
                    copy.wait()

            cols = pl.ds(n * 256, 256)
            gate = jnp.dot(a_v[...], wg_v[:, cols], preferred_element_type=F32)
            up = jnp.dot(a_v[...], wu_v[:, cols], preferred_element_type=F32)
            om_v[:, pl.ds(QCOLS + n * 256, 256)] = (gate * (1.0 / (1.0 + jnp.exp(-gate))) * up).astype(BF16)

        @pl.when(b == 0)
        def _():
            for copy in load_tab:
                copy.start()
            for n in range(1, BLOCKS):
                load_x(n).start()

    def down(half, quarter):
        cols = pl.ds(pl.multiple_of(half * 1024 + quarter * 512, 512), 512)
        return jnp.dot(om_v[...], wod_v[:, cols], preferred_element_type=F32)

    def down_other(b):
        @pl.when(b == 0)
        def _():
            for copy in load_od:
                copy.wait()

        for kind, quarter in ((D2D_FIRST, 1 - p2), (D2D_SECOND, p2)):
            part = down(1 - core, quarter).astype(BF16)
            for s in range(2):
                d2d_src[2 * b + s, kind] = part[s * HALF:(s + 1) * HALF]
            for s in range(2):
                copy_of(kind, 2 * b + s).start()

    def down_mine(b):
        part = down(core, 1 - p1)
        for s in range(2):
            u = 2 * b + s
            with jax.named_scope("recv"):
                copy_of(D2D_FIRST, u).wait_recv()
            h_send[u] = (part[s * HALF:(s + 1) * HALF] + d2d_dst[u, 0].astype(F32)).astype(BF16)
            copy_of(RED_ONE, u).start()
        part = down(core, p1)
        for s in range(2):
            u = 2 * b + s
            with jax.named_scope("recv"):
                copy_of(D2D_SECOND, u).wait_recv()
            h_keep[u] = part[s * HALF:(s + 1) * HALF] + d2d_dst[u, 1].astype(F32)

    def stage_b(u):
        with jax.named_scope("recv"):
            copy_of(RED_ONE, u).wait_recv()
        send = pl.ds(pl.multiple_of((1 - p2) * 256, 256), 256)
        keep = pl.ds(pl.multiple_of(p2 * 256, 256), 256)
        p_send[u] = (h_keep[u, :, send] + r1_dst[u, :, send].astype(F32)).astype(BF16)
        copy_of(RED_TWO, u).start()
        p_keep[u] = h_keep[u, :, keep] + r1_dst[u, :, keep].astype(F32)

    def stage_c(u):
        with jax.named_scope("recv"):
            copy_of(RED_TWO, u).wait_recv()
        cols = pl.ds(pl.multiple_of((mine + p2) * 256, 256), 256)
        x_f = x_v[half_rows(u), cols].astype(F32)
        y_v[half_rows(u), cols] = (x_f + (p_keep[u] + r2_dst[u].astype(F32))).astype(BF16)
        copy_of(GAT_ONE, u).start()

    def stage_d(u):
        with jax.named_scope("recv"):
            copy_of(GAT_ONE, u).wait_recv()
        copy_of(GAT_TWO, u).start()
        copy_of(OUT_FIRST, u).start()

    def stage_e(u):
        with jax.named_scope("recv"):
            copy_of(GAT_TWO, u).wait_recv()
        copy_of(OUT_SECOND, u).start()

    def stage_f(u):
        with jax.named_scope("recv"):
            copy_of(OUT_FIRST, u).wait_recv()
            copy_of(OUT_SECOND, u).wait_recv()

    stages = {"b": stage_b, "c": stage_c, "d": stage_d, "e": stage_e, "f": stage_f}

    def communicate(i, point):
        for name, ats in STAGE_AT:
            for s, at in enumerate(ats):
                if (at + 4 - point) % 5 == 0:
                    b = i - (at + 4 - point) // 5

                    @pl.when((b >= 0) & (b < BLOCKS))
                    def _():
                        with jax.named_scope("stage_" + name):
                            stages[name](2 * b + s)

    def step(i, carry):
        for point, part in enumerate((project, attend, gate_up, down_other, down_mine)):
            @pl.when(i < BLOCKS)
            def _():
                with jax.named_scope(part.__name__):
                    part(i)

            communicate(i, point)
        return carry

    lax.fori_loop(0, BLOCKS + DRAIN, step, 0)

    def finish(u, carry):
        for kind in range(8):
            copy_of(kind, u).wait_send()
        return carry

    with jax.named_scope("finish"):
        lax.fori_loop(0, UNITS, finish, 0)


def store_kernel(y_v, k_v, v_v, y_out, k_out, v_out, sem):
    copies = [pltpu.make_async_copy(k_v, k_out, sem.at[0]), pltpu.make_async_copy(v_v, v_out, sem.at[1])]
    for b in range(BLOCKS):
        rows = pl.ds(b * ROWS, ROWS)
        copies.append(pltpu.make_async_copy(y_v.at[rows, :], y_out.at[rows, :], sem.at[2 + b]))
    for copy in copies:
        copy.start()
    for copy in copies:
        copy.wait()


def solution(mesh):
    cos_np, sin_np = rope_tables()

    def local_layer(x_in, g_norm, w_q, w_k, w_v, w_o, w_gate, w_up, w_down):
        any_spec = pl.BlockSpec(memory_space=pl.ANY)
        y, k, v = pl.pallas_call(
            layer_kernel,
            out_shape=(pltpu.VMEM((TOKENS, WIDTH), BF16), pltpu.VMEM((TOKENS, HEAD_DIM), BF16), pltpu.VMEM((TOKENS, HEAD_DIM), BF16)),
            in_specs=[any_spec] * 11,
            out_specs=(pl.BlockSpec(memory_space=pltpu.VMEM),) * 3,
            scratch_shapes=[
                pltpu.VMEM((TOKENS, WIDTH), BF16),
                pltpu.VMEM((WIDTH,), BF16),
                pltpu.VMEM((8, WIDTH), F32),
                pltpu.VMEM((WIDTH, QCOLS + 2 * HEAD_DIM), BF16),
                pltpu.VMEM((WIDTH, FFCOLS), BF16),
                pltpu.VMEM((WIDTH, FFCOLS), BF16),
                pltpu.VMEM((KDOWN, WIDTH), BF16),
                pltpu.VMEM((TOKENS, HEAD_DIM), F32),
                pltpu.VMEM((TOKENS, HEAD_DIM), F32),
                pltpu.VMEM((ROWS, WIDTH), BF16),
                pltpu.VMEM((2 * ROWS, HEAD_DIM), BF16),
                pltpu.VMEM((2, ROWS, TOKENS), F32),
                pltpu.VMEM((2, ROWS, TOKENS), BF16),
                pltpu.VMEM((ROWS, KDOWN), BF16),
                pltpu.VMEM((UNITS, 2, HALF, 512), BF16),
                pltpu.VMEM((UNITS, 2, HALF, 512), BF16),
                pltpu.VMEM((UNITS, HALF, 512), BF16),
                pltpu.VMEM((UNITS, HALF, 512), F32),
                pltpu.VMEM((UNITS, HALF, 512), BF16),
                pltpu.VMEM((UNITS, HALF, 256), BF16),
                pltpu.VMEM((UNITS, HALF, 256), F32),
                pltpu.VMEM((UNITS, HALF, 256), BF16),
                pltpu.SemaphoreType.DMA((BLOCKS,)),
                pltpu.SemaphoreType.DMA((16,)),
                pltpu.SemaphoreType.DMA((8, UNITS)),
                pltpu.SemaphoreType.DMA((8, UNITS)),
            ],
            compiler_params=pltpu.CompilerParams(collective_id=0, has_side_effects=True, vmem_limit_bytes=67043328 - 8 * 1024 * 1024),
        )(x_in, g_norm, w_q, w_k, w_v, w_o, w_gate, w_up, w_down, jnp.asarray(cos_np), jnp.asarray(sin_np))
        y, k, v = pl.pallas_call(
            store_kernel,
            out_shape=(jax.ShapeDtypeStruct((TOKENS, WIDTH), BF16), jax.ShapeDtypeStruct((TOKENS, HEAD_DIM), BF16),
                       jax.ShapeDtypeStruct((TOKENS, HEAD_DIM), BF16)),
            in_specs=[any_spec] * 3,
            out_specs=(any_spec,) * 3,
            scratch_shapes=[pltpu.SemaphoreType.DMA((2 + BLOCKS,))],
            compiler_params=pltpu.CompilerParams(vmem_limit_bytes=1024 * 1024),
        )(*(pltpu.with_memory_space_constraint(part, pltpu.VMEM) for part in (y, k, v)))
        return y, k.reshape(TOKENS, 1, HEAD_DIM), v.reshape(TOKENS, 1, HEAD_DIM)

    return jax.shard_map(local_layer, mesh=mesh, in_specs=(P('dp', None), P(None), P(None, 'tp'), P(None, None), P(None, None), P('tp', None), P(None, 'tp'), P(None, 'tp'), P('tp', None)), out_specs=(P('dp', None), P('dp', 'tp', None), P('dp', 'tp', None)), check_vma=False)
```

```python
import math
import numpy as np
import jax
import jax.numpy as jnp
from jax import lax
from jax.experimental import pallas as pl
from jax.experimental.pallas import tpu as pltpu
from jax.sharding import PartitionSpec as P

HEAD_DIM = 128
ROPE_BASE = 500000.0
NORM_EPS = 1e-5
TOKENS = 1536
WIDTH = 2048
QCOLS = 256
FFCOLS = 768
ROWS = 256
BLOCKS = TOKENS // ROWS
KDOWN = QCOLS + FFCOLS
HALF = ROWS // 2
UNITS = TOKENS // HALF
STAGE_AT = (("b", (4, 4)), ("c", (7, 7)), ("d", (10, 10)), ("e", (19, 19)), ("f", (26, 26)))
DRAIN = 1 + max(max(at) for _, at in STAGE_AT) // 5
SCORE_SCALE = math.log2(math.e) / math.sqrt(HEAD_DIM)
F32 = jnp.float32
BF16 = jnp.bfloat16
MESH = pl.DeviceIdType.MESH

D2D_FIRST, D2D_SECOND, RED_ONE, RED_TWO, GAT_ONE, GAT_TWO, OUT_FIRST, OUT_SECOND = range(8)


def rope_tables():
    inv_freq = np.float32(ROPE_BASE) ** (-np.arange(0, HEAD_DIM, 2, dtype=np.float32) / np.float32(HEAD_DIM))
    angles = np.arange(TOKENS, dtype=np.float32)[:, None] * inv_freq.astype(np.float32)[None, :]
    cos, sin = np.cos(angles.astype(np.float64)), np.sin(angles.astype(np.float64))
    return (np.concatenate([cos, cos], axis=1).astype(np.float32), np.concatenate([-sin, sin], axis=1).astype(np.float32))


def layer_kernel(x_hbm, g_hbm, wq_hbm, wk_hbm, wv_hbm, wo_hbm, wg_hbm, wu_hbm, wd_hbm, cos_hbm, sin_hbm,
                 y_v, k_v, v_v,
                 x_v, g_v, gf_v, wqkv_v, wg_v, wu_v, wod_v, cos_v, sin_v,
                 a_v, q_v, s_v, p_v, om_v,
                 d2d_src, d2d_dst, h_send, h_keep, r1_dst, p_send, p_keep, r2_dst,
                 x_sem, w_sem, ssem, rsem):
    me = lax.axis_index('tp')
    core = lax.rem(me, 2)
    xpos = lax.rem(me // 2, 2)
    ypos = me // 4
    sibling = me + 1 - 2 * core
    xpeer = me + 2 - 4 * xpos
    ypeer = me + 4 - 8 * ypos
    p1 = xpos + core * (ypos - xpos)
    p2 = ypos + core * (xpos - ypos)
    n1 = xpeer + core * (ypeer - xpeer)
    n2 = ypeer + core * (xpeer - ypeer)

    def rows_of(b):
        return pl.ds(pl.multiple_of(b * ROWS, ROWS), ROWS)

    def load(src, dst, index):
        return pltpu.make_async_copy(src, dst, w_sem.at[index])

    def load_x(b):
        return pltpu.make_async_copy(x_hbm.at[rows_of(b), :], x_v.at[rows_of(b), :], x_sem.at[b])

    kv_cols = pl.ds(pl.multiple_of(me * HEAD_DIM, HEAD_DIM), HEAD_DIM)
    early, late = pl.ds(0, ROWS), pl.ds(ROWS, TOKENS - ROWS)
    load_g = load(g_hbm, g_v, 0)
    load_qkv = [
        load(wk_hbm.at[:, kv_cols], wqkv_v.at[:, pl.ds(QCOLS, HEAD_DIM)], 1),
        load(wv_hbm.at[:, kv_cols], wqkv_v.at[:, pl.ds(QCOLS + HEAD_DIM, HEAD_DIM)], 2),
        load(wq_hbm, wqkv_v.at[:, pl.ds(0, QCOLS)], 3),
        load(cos_hbm.at[early, :], cos_v.at[early, :], 4),
        load(sin_hbm.at[early, :], sin_v.at[early, :], 5),
    ]
    load_gu = []
    for n in range(FFCOLS // 256):
        tile = pl.ds(n * 256, 256)
        load_gu.append((load(wg_hbm.at[:, tile], wg_v.at[:, tile], 6 + 2 * n), load(wu_hbm.at[:, tile], wu_v.at[:, tile], 7 + 2 * n)))
    load_od = [load(wo_hbm, wod_v.at[pl.ds(0, QCOLS), :], 12), load(wd_hbm, wod_v.at[pl.ds(QCOLS, FFCOLS), :], 13)]
    load_tab = [load(cos_hbm.at[late, :], cos_v.at[late, :], 14), load(sin_hbm.at[late, :], sin_v.at[late, :], 15)]

    load_x(0).start()
    load_g.start()
    for copy in load_qkv:
        copy.start()

    barrier = pltpu.get_barrier_semaphore()
    for peer in (sibling, xpeer, ypeer):
        pl.semaphore_signal(barrier, inc=1, device_id={'tp': peer}, device_id_type=MESH)

    def remote(kind, u, src, dst, peer):
        return pltpu.make_async_remote_copy(src_ref=src, dst_ref=dst, send_sem=ssem.at[kind, u], recv_sem=rsem.at[kind, u],
                                            device_id={'tp': peer}, device_id_type=MESH)

    mine = core * 4 + p1 * 2
    other = core * 4 + (1 - p1) * 2

    def half_rows(u):
        return pl.ds(pl.multiple_of(u * HALF, HALF), HALF)

    def y_part(u, piece, count):
        return y_v.at[half_rows(u), pl.ds(pl.multiple_of(piece * 256, 256), count * 256)]

    def copy_of(kind, u):
        if kind == D2D_FIRST or kind == D2D_SECOND:
            return remote(kind, u, d2d_src.at[u, kind], d2d_dst.at[u, kind], sibling)
        if kind == RED_ONE:
            return remote(kind, u, h_send.at[u], r1_dst.at[u], n1)
        if kind == RED_TWO:
            return remote(kind, u, p_send.at[u], r2_dst.at[u], n2)
        if kind == GAT_ONE:
            part = y_part(u, mine + p2, 1)
            return remote(kind, u, part, part, n2)
        if kind == GAT_TWO:
            part = y_part(u, mine, 2)
            return remote(kind, u, part, part, n1)
        part = y_part(u, mine if kind == OUT_FIRST else other, 2)
        return remote(kind, u, part, part, sibling)

    def norm_rows(b, r):
        x_f = x_v[pl.ds(pl.multiple_of(b * ROWS + r * 16, 16), 16), :].astype(F32)
        inv = lax.rsqrt(jnp.mean(x_f * x_f, axis=-1, keepdims=True) + NORM_EPS)
        gain = jnp.concatenate([gf_v[...], gf_v[...]], axis=0)
        a_v[lax.rem(b, 2), pl.ds(r * 16, 16), :] = (x_f * inv * gain).astype(BF16)

    def project(b):
        @pl.when(b == 0)
        def _():
            with jax.named_scope("wait_x"):
                load_x(0).wait()
                load_g.wait()
            gf_v[...] = jnp.broadcast_to(g_v[...].astype(F32)[None, :], (8, WIDTH))
            for pair in load_gu:
                for copy in pair:
                    copy.start()
            load_x(1).start()
            for r in range(ROWS // 16):
                norm_rows(0, r)
            for copy in load_od:
                copy.start()
            with jax.named_scope("wait_w"):
                for copy in load_qkv:
                    copy.wait()
            with jax.named_scope("wait_barrier"):
                pl.semaphore_wait(barrier, 3)

        @pl.when(b == 1)
        def _():
            for copy in load_tab:
                copy.wait()

        @pl.when(b < BLOCKS - 1)
        def _():
            load_x(b + 1).wait()

        cos, sin = cos_v[rows_of(b), :], sin_v[rows_of(b), :]
        qkv = jnp.dot(a_v[lax.rem(b, 2)], wqkv_v[...], preferred_element_type=F32)

        def rope(h):
            return (h * cos + pltpu.roll(h, HEAD_DIM // 2, 1) * sin).astype(BF16)

        q_v[pl.ds(0, ROWS), :] = rope(qkv[:, 0:128])
        q_v[pl.ds(ROWS, ROWS), :] = rope(qkv[:, 128:256])
        k_v[rows_of(b), :] = rope(qkv[:, 256:384])
        v_v[rows_of(b), :] = qkv[:, 384:512].astype(BF16)

    def attend(i):
        for b in range(BLOCKS):
            @pl.when(i == b)
            def _():
                attend_block(b)

    def attend_block(b):
        def tile(j):
            return pl.ds(j * ROWS, ROWS)

        for h in range(2):
            q = q_v[pl.ds(h * ROWS, ROWS), :]
            peak = None
            for j in range(b + 1):
                s = lax.dot_general(q, k_v[tile(j), :], (((1,), (1,)), ((), ())), preferred_element_type=F32) * SCORE_SCALE
                if j == b:
                    qpos = lax.broadcasted_iota(jnp.int32, (ROWS, ROWS), 0)
                    kpos = lax.broadcasted_iota(jnp.int32, (ROWS, ROWS), 1)
                    s = jnp.where(kpos <= qpos, s, -1e30)
                s_v[h, :, tile(j)] = s
                pair = jnp.maximum(s[:, :128], s[:, 128:])
                peak = pair if peak is None else jnp.maximum(peak, pair)
            peak = jnp.max(peak, axis=1, keepdims=True)
            total = None
            for j in range(b + 1):
                e = jnp.exp2(s_v[h, :, tile(j)] - peak)
                pair = e[:, :128] + e[:, 128:]
                total = pair if total is None else total + pair
            shift = peak + jnp.log2(jnp.sum(total, axis=1, keepdims=True))
            for j in range(b + 1):
                p_v[h, :, tile(j)] = jnp.exp2(s_v[h, :, tile(j)] - shift).astype(BF16)
            keys = pl.ds(0, (b + 1) * ROWS)
            o = jnp.dot(p_v[h, :, keys], v_v[keys, :], preferred_element_type=F32)
            om_v[:, pl.ds(h * HEAD_DIM, HEAD_DIM)] = o.astype(BF16)

    def gate_up_tile(b, n):
        cols = pl.ds(n * 256, 256)
        normed = a_v[lax.rem(b, 2)]
        gate = jnp.dot(normed, wg_v[:, cols], preferred_element_type=F32)
        up = jnp.dot(normed, wu_v[:, cols], preferred_element_type=F32)
        om_v[:, pl.ds(QCOLS + n * 256, 256)] = (gate * (1.0 / (1.0 + jnp.exp(-gate))) * up).astype(BF16)

    def gate_up(b):
        @pl.when(b == 0)
        def _():
            for n in range(FFCOLS // 256):
                for copy in load_gu[n]:
                    copy.wait()
            for copy in load_tab:
                copy.start()
            for n in range(2, BLOCKS):
                load_x(n).start()

        after = jnp.minimum(b + 1, BLOCKS - 1)
        steps = ROWS // 16
        tiles = FFCOLS // 256
        for n in range(tiles):
            gate_up_tile(b, n)
            for r in range(n * steps // tiles, (n + 1) * steps // tiles):
                norm_rows(after, r)

    def down(half, quarter):
        cols = pl.ds(pl.multiple_of(half * 1024 + quarter * 512, 512), 512)
        return jnp.dot(om_v[...], wod_v[:, cols], preferred_element_type=F32)

    def down_other(b):
        @pl.when(b == 0)
        def _():
            for copy in load_od:
                copy.wait()

        for kind, quarter in ((D2D_FIRST, 1 - p2), (D2D_SECOND, p2)):
            part = down(1 - core, quarter).astype(BF16)
            for s in range(2):
                d2d_src[2 * b + s, kind] = part[s * HALF:(s + 1) * HALF]
            for s in range(2):
                copy_of(kind, 2 * b + s).start()

    def down_mine(b):
        part = down(core, 1 - p1)
        for s in range(2):
            u = 2 * b + s
            with jax.named_scope("recv"):
                copy_of(D2D_FIRST, u).wait_recv()
            h_send[u] = (part[s * HALF:(s + 1) * HALF] + d2d_dst[u, 0].astype(F32)).astype(BF16)
            copy_of(RED_ONE, u).start()
        part = down(core, p1)
        for s in range(2):
            u = 2 * b + s
            with jax.named_scope("recv"):
                copy_of(D2D_SECOND, u).wait_recv()
            h_keep[u] = part[s * HALF:(s + 1) * HALF] + d2d_dst[u, 1].astype(F32)

    def stage_b(u):
        with jax.named_scope("recv"):
            copy_of(RED_ONE, u).wait_recv()
        send = pl.ds(pl.multiple_of((1 - p2) * 256, 256), 256)
        keep = pl.ds(pl.multiple_of(p2 * 256, 256), 256)
        p_send[u] = (h_keep[u, :, send] + r1_dst[u, :, send].astype(F32)).astype(BF16)
        copy_of(RED_TWO, u).start()
        p_keep[u] = h_keep[u, :, keep] + r1_dst[u, :, keep].astype(F32)

    def stage_c(u):
        with jax.named_scope("recv"):
            copy_of(RED_TWO, u).wait_recv()
        cols = pl.ds(pl.multiple_of((mine + p2) * 256, 256), 256)
        x_f = x_v[half_rows(u), cols].astype(F32)
        y_v[half_rows(u), cols] = (x_f + (p_keep[u] + r2_dst[u].astype(F32))).astype(BF16)
        copy_of(GAT_ONE, u).start()

    def stage_d(u):
        with jax.named_scope("recv"):
            copy_of(GAT_ONE, u).wait_recv()
        copy_of(GAT_TWO, u).start()
        copy_of(OUT_FIRST, u).start()

    def stage_e(u):
        with jax.named_scope("recv"):
            copy_of(GAT_TWO, u).wait_recv()
        copy_of(OUT_SECOND, u).start()

    def stage_f(u):
        with jax.named_scope("recv"):
            copy_of(OUT_FIRST, u).wait_recv()
            copy_of(OUT_SECOND, u).wait_recv()

    stages = {"b": stage_b, "c": stage_c, "d": stage_d, "e": stage_e, "f": stage_f}

    def communicate(i, point):
        for name, ats in STAGE_AT:
            for s, at in enumerate(ats):
                if (at + 4 - point) % 5 == 0:
                    b = i - (at + 4 - point) // 5

                    @pl.when((b >= 0) & (b < BLOCKS))
                    def _():
                        with jax.named_scope("stage_" + name):
                            stages[name](2 * b + s)

    def step(i, carry):
        for point, part in enumerate((project, attend, gate_up, down_other, down_mine)):
            @pl.when(i < BLOCKS)
            def _():
                with jax.named_scope(part.__name__):
                    part(i)

            communicate(i, point)
        return carry

    lax.fori_loop(0, BLOCKS + DRAIN, step, 0)

    def finish(u, carry):
        for kind in range(8):
            copy_of(kind, u).wait_send()
        return carry

    with jax.named_scope("finish"):
        lax.fori_loop(0, UNITS, finish, 0)


def store_kernel(y_v, k_v, v_v, y_out, k_out, v_out, sem):
    copies = [pltpu.make_async_copy(k_v, k_out, sem.at[0]), pltpu.make_async_copy(v_v, v_out, sem.at[1])]
    for b in range(BLOCKS):
        rows = pl.ds(b * ROWS, ROWS)
        copies.append(pltpu.make_async_copy(y_v.at[rows, :], y_out.at[rows, :], sem.at[2 + b]))
    for copy in copies:
        copy.start()
    for copy in copies:
        copy.wait()


def solution(mesh):
    cos_np, sin_np = rope_tables()

    def local_layer(x_in, g_norm, w_q, w_k, w_v, w_o, w_gate, w_up, w_down):
        any_spec = pl.BlockSpec(memory_space=pl.ANY)
        y, k, v = pl.pallas_call(
            layer_kernel,
            out_shape=(pltpu.VMEM((TOKENS, WIDTH), BF16), pltpu.VMEM((TOKENS, HEAD_DIM), BF16), pltpu.VMEM((TOKENS, HEAD_DIM), BF16)),
            in_specs=[any_spec] * 11,
            out_specs=(pl.BlockSpec(memory_space=pltpu.VMEM),) * 3,
            scratch_shapes=[
                pltpu.VMEM((TOKENS, WIDTH), BF16),
                pltpu.VMEM((WIDTH,), BF16),
                pltpu.VMEM((8, WIDTH), F32),
                pltpu.VMEM((WIDTH, QCOLS + 2 * HEAD_DIM), BF16),
                pltpu.VMEM((WIDTH, FFCOLS), BF16),
                pltpu.VMEM((WIDTH, FFCOLS), BF16),
                pltpu.VMEM((KDOWN, WIDTH), BF16),
                pltpu.VMEM((TOKENS, HEAD_DIM), F32),
                pltpu.VMEM((TOKENS, HEAD_DIM), F32),
                pltpu.VMEM((2, ROWS, WIDTH), BF16),
                pltpu.VMEM((2 * ROWS, HEAD_DIM), BF16),
                pltpu.VMEM((2, ROWS, TOKENS), F32),
                pltpu.VMEM((2, ROWS, TOKENS), BF16),
                pltpu.VMEM((ROWS, KDOWN), BF16),
                pltpu.VMEM((UNITS, 2, HALF, 512), BF16),
                pltpu.VMEM((UNITS, 2, HALF, 512), BF16),
                pltpu.VMEM((UNITS, HALF, 512), BF16),
                pltpu.VMEM((UNITS, HALF, 512), F32),
                pltpu.VMEM((UNITS, HALF, 512), BF16),
                pltpu.VMEM((UNITS, HALF, 256), BF16),
                pltpu.VMEM((UNITS, HALF, 256), F32),
                pltpu.VMEM((UNITS, HALF, 256), BF16),
                pltpu.SemaphoreType.DMA((BLOCKS,)),
                pltpu.SemaphoreType.DMA((16,)),
                pltpu.SemaphoreType.DMA((8, UNITS)),
                pltpu.SemaphoreType.DMA((8, UNITS)),
            ],
            compiler_params=pltpu.CompilerParams(collective_id=0, has_side_effects=True, vmem_limit_bytes=67043328 - 8 * 1024 * 1024),
        )(x_in, g_norm, w_q, w_k, w_v, w_o, w_gate, w_up, w_down, jnp.asarray(cos_np), jnp.asarray(sin_np))
        y, k, v = pl.pallas_call(
            store_kernel,
            out_shape=(jax.ShapeDtypeStruct((TOKENS, WIDTH), BF16), jax.ShapeDtypeStruct((TOKENS, HEAD_DIM), BF16),
                       jax.ShapeDtypeStruct((TOKENS, HEAD_DIM), BF16)),
            in_specs=[any_spec] * 3,
            out_specs=(any_spec,) * 3,
            scratch_shapes=[pltpu.SemaphoreType.DMA((2 + BLOCKS,))],
            compiler_params=pltpu.CompilerParams(vmem_limit_bytes=1024 * 1024),
        )(*(pltpu.with_memory_space_constraint(part, pltpu.VMEM) for part in (y, k, v)))
        return y, k.reshape(TOKENS, 1, HEAD_DIM), v.reshape(TOKENS, 1, HEAD_DIM)

    return jax.shard_map(local_layer, mesh=mesh, in_specs=(P('dp', None), P(None), P(None, 'tp'), P(None, None), P(None, None), P('tp', None), P(None, 'tp'), P(None, 'tp'), P('tp', None)), out_specs=(P('dp', None), P('dp', 'tp', None), P('dp', 'tp', None)), check_vma=False)
```

```python
import math
import numpy as np
import jax
import jax.numpy as jnp
from jax import lax
from jax.experimental import pallas as pl
from jax.experimental.pallas import tpu as pltpu
from jax.sharding import PartitionSpec as P

HEAD_DIM = 128
ROPE_BASE = 500000.0
NORM_EPS = 1e-5
TOKENS = 1536
WIDTH = 2048
QCOLS = 256
FFCOLS = 768
ROWS = 256
BLOCKS = TOKENS // ROWS
KDOWN = QCOLS + FFCOLS
HALF = ROWS // 2
UNITS = TOKENS // HALF
STAGE_AT = (("b", (4, 4)), ("c", (7, 7)), ("d", (10, 10)), ("e", (19, 19)), ("f", (26, 26)))
DRAIN = 1 + max(max(at) for _, at in STAGE_AT) // 5
SCORE_SCALE = math.log2(math.e) / math.sqrt(HEAD_DIM)
F32 = jnp.float32
BF16 = jnp.bfloat16
MESH = pl.DeviceIdType.MESH

D2D_FIRST, D2D_SECOND, RED_ONE, RED_TWO, GAT_ONE, GAT_TWO, OUT_FIRST, OUT_SECOND = range(8)


def rope_table():
    inv_freq = np.float32(ROPE_BASE) ** (-np.arange(0, HEAD_DIM, 2, dtype=np.float32) / np.float32(HEAD_DIM))
    angles = np.arange(TOKENS, dtype=np.float32)[:, None] * inv_freq.astype(np.float32)[None, :]
    angles = angles.astype(np.float64)
    return np.concatenate([np.cos(angles), np.sin(angles)], axis=1).astype(np.float32)


def layer_kernel(x_hbm, g_hbm, wq_hbm, wk_hbm, wv_hbm, wo_hbm, wg_hbm, wu_hbm, wd_hbm, tab_hbm,
                 y_v, k_v, v_v,
                 x_v, g_v, gf_v, wqkv_v, wg_v, wu_v, wod_v, tab_v,
                 a_v, q_v, s_v, p_v, om_v,
                 d2d_src, d2d_dst, h_send, h_keep, r1_dst, p_send, p_keep, r2_dst,
                 x_sem, w_sem, ssem, rsem):
    me = lax.axis_index('tp')
    core = lax.rem(me, 2)
    xpos = lax.rem(me // 2, 2)
    ypos = me // 4
    sibling = me + 1 - 2 * core
    xpeer = me + 2 - 4 * xpos
    ypeer = me + 4 - 8 * ypos
    p1 = xpos + core * (ypos - xpos)
    p2 = ypos + core * (xpos - ypos)
    n1 = xpeer + core * (ypeer - xpeer)
    n2 = ypeer + core * (xpeer - ypeer)

    def rows_of(b):
        return pl.ds(pl.multiple_of(b * ROWS, ROWS), ROWS)

    def load(src, dst, index):
        return pltpu.make_async_copy(src, dst, w_sem.at[index])

    def load_x(b):
        return pltpu.make_async_copy(x_hbm.at[rows_of(b), :], x_v.at[rows_of(b), :], x_sem.at[b])

    def load_first(n):
        rows = pl.ds(n * 64, 64)
        return pltpu.make_async_copy(x_hbm.at[rows, :], x_v.at[rows, :], x_sem.at[0 if n == 0 else BLOCKS - 1 + n])

    kv_cols = pl.ds(pl.multiple_of(me * HEAD_DIM, HEAD_DIM), HEAD_DIM)
    early, late = pl.ds(0, ROWS), pl.ds(ROWS, TOKENS - ROWS)
    load_g = load(g_hbm, g_v, 0)
    load_qkv = [
        load(wk_hbm.at[:, kv_cols], wqkv_v.at[:, pl.ds(QCOLS, HEAD_DIM)], 1),
        load(wv_hbm.at[:, kv_cols], wqkv_v.at[:, pl.ds(QCOLS + HEAD_DIM, HEAD_DIM)], 2),
        load(wq_hbm, wqkv_v.at[:, pl.ds(0, QCOLS)], 3),
        load(tab_hbm.at[early, :], tab_v.at[early, :], 4),
    ]
    load_gu = []
    for n in range(FFCOLS // 256):
        tile = pl.ds(n * 256, 256)
        load_gu.append((load(wg_hbm.at[:, tile], wg_v.at[:, tile], 6 + 2 * n), load(wu_hbm.at[:, tile], wu_v.at[:, tile], 7 + 2 * n)))
    load_od = [load(wo_hbm, wod_v.at[pl.ds(0, QCOLS), :], 12), load(wd_hbm, wod_v.at[pl.ds(QCOLS, FFCOLS), :], 13)]
    load_tab = load(tab_hbm.at[late, :], tab_v.at[late, :], 5)

    load_g.start()
    for n in range(4):
        load_first(n).start()

    barrier = pltpu.get_barrier_semaphore()
    for peer in (sibling, xpeer, ypeer):
        pl.semaphore_signal(barrier, inc=1, device_id={'tp': peer}, device_id_type=MESH)

    def remote(kind, u, src, dst, peer):
        return pltpu.make_async_remote_copy(src_ref=src, dst_ref=dst, send_sem=ssem.at[kind, u], recv_sem=rsem.at[kind, u],
                                            device_id={'tp': peer}, device_id_type=MESH)

    mine = core * 4 + p1 * 2
    other = core * 4 + (1 - p1) * 2

    def half_rows(u):
        return pl.ds(pl.multiple_of(u * HALF, HALF), HALF)

    def y_part(u, piece, count):
        return y_v.at[half_rows(u), pl.ds(pl.multiple_of(piece * 256, 256), count * 256)]

    def copy_of(kind, u):
        if kind == D2D_FIRST or kind == D2D_SECOND:
            return remote(kind, u, d2d_src.at[u, kind], d2d_dst.at[u, kind], sibling)
        if kind == RED_ONE:
            return remote(kind, u, h_send.at[u], r1_dst.at[u], n1)
        if kind == RED_TWO:
            return remote(kind, u, p_send.at[u], r2_dst.at[u], n2)
        if kind == GAT_ONE:
            part = y_part(u, mine + p2, 1)
            return remote(kind, u, part, part, n2)
        if kind == GAT_TWO:
            part = y_part(u, mine, 2)
            return remote(kind, u, part, part, n1)
        part = y_part(u, mine if kind == OUT_FIRST else other, 2)
        return remote(kind, u, part, part, sibling)

    def norm_rows(b, r):
        x_f = x_v[pl.ds(pl.multiple_of(b * ROWS + r * 16, 16), 16), :].astype(F32)
        inv = lax.rsqrt(jnp.mean(x_f * x_f, axis=-1, keepdims=True) + NORM_EPS)
        gain = jnp.concatenate([gf_v[...], gf_v[...]], axis=0)
        a_v[b % 2, pl.ds(r * 16, 16), :] = (x_f * inv * gain).astype(BF16)

    def project(b):
        @pl.when(b == 0)
        def _():
            load_g.wait()
            gf_v[...] = jnp.broadcast_to(g_v[...].astype(F32)[None, :], (8, WIDTH))
            for n in range(4):
                load_first(n).wait()
                if n == 0:
                    for copy in load_qkv:
                        copy.start()
                if n == 2:
                    for pair in load_gu:
                        for copy in pair:
                            copy.start()
                for r in range(n * 4, n * 4 + 4):
                    norm_rows(0, r)
            for copy in load_od:
                copy.start()
            load_x(1).start()
            for copy in load_qkv:
                copy.wait()
            pl.semaphore_wait(barrier, 3)

        @pl.when(b == 1)
        def _():
            load_tab.wait()

        tab = tab_v[rows_of(b), :]
        swapped = pltpu.roll(tab, HEAD_DIM // 2, 1)
        low = lax.broadcasted_iota(jnp.int32, tab.shape, 1) < HEAD_DIM // 2
        cos = jnp.where(low, tab, swapped)
        sin = jnp.where(low, -swapped, tab)
        qkv = jnp.dot(a_v[lax.rem(b, 2)], wqkv_v[...], preferred_element_type=F32)

        def rope(h):
            return (h * cos + pltpu.roll(h, HEAD_DIM // 2, 1) * sin).astype(BF16)

        q_v[pl.ds(0, ROWS), :] = rope(qkv[:, 0:128])
        q_v[pl.ds(ROWS, ROWS), :] = rope(qkv[:, 128:256])
        k_v[rows_of(b), :] = rope(qkv[:, 256:384])
        v_v[rows_of(b), :] = qkv[:, 384:512].astype(BF16)

    def attention(b):
        def tile(j):
            return pl.ds(j * ROWS, ROWS)

        heads = range(2)
        peak, total, shift = [None] * 2, [None] * 2, [None] * 2
        for j in range(b + 1):
            for h in heads:
                q = q_v[pl.ds(h * ROWS, ROWS), :]
                s = lax.dot_general(q, k_v[tile(j), :], (((1,), (1,)), ((), ())), preferred_element_type=F32) * SCORE_SCALE
                if j == b:
                    qpos = lax.broadcasted_iota(jnp.int32, (ROWS, ROWS), 0)
                    kpos = lax.broadcasted_iota(jnp.int32, (ROWS, ROWS), 1)
                    s = jnp.where(kpos <= qpos, s, -1e30)
                s_v[h, :, tile(j)] = s
                pair = jnp.maximum(s[:, :128], s[:, 128:])
                peak[h] = pair if j == 0 else jnp.maximum(peak[h], pair)
                yield
        for h in heads:
            peak[h] = jnp.max(peak[h], axis=1, keepdims=True)
        for j in range(b + 1):
            for h in heads:
                e = jnp.exp2(s_v[h, :, tile(j)] - peak[h])
                pair = e[:, :128] + e[:, 128:]
                total[h] = pair if j == 0 else total[h] + pair
                yield
        for h in heads:
            shift[h] = peak[h] + jnp.log2(jnp.sum(total[h], axis=1, keepdims=True))
        for j in range(b + 1):
            for h in heads:
                p_v[h, :, tile(j)] = jnp.exp2(s_v[h, :, tile(j)] - shift[h]).astype(BF16)
                yield
        keys = pl.ds(0, (b + 1) * ROWS)
        for h in heads:
            o = jnp.dot(p_v[h, :, keys], v_v[keys, :], preferred_element_type=F32)
            om_v[:, pl.ds(h * HEAD_DIM, HEAD_DIM)] = o.astype(BF16)
            yield

    def gate_up(b):
        normed = a_v.at[b % 2]
        for n in range(FFCOLS // 256):
            if b == 0:
                for copy in load_gu[n]:
                    copy.wait()
            cols = pl.ds(n * 256, 256)
            gate = jnp.dot(normed[...], wg_v[:, cols], preferred_element_type=F32)
            yield
            up = jnp.dot(normed[...], wu_v[:, cols], preferred_element_type=F32)
            om_v[:, pl.ds(QCOLS + n * 256, 256)] = (gate * (1.0 / (1.0 + jnp.exp(-gate))) * up).astype(BF16)
            yield

    def next_norm(b):
        for r in range(ROWS // 16):
            norm_rows(b + 1, r)
            yield

    def mix_block(b):
        works = [(gate_up(b), 6), (attention(b), 6 * (b + 1) + 2)]
        if b == 0:
            load_tab.start()
            for n in range(2, BLOCKS):
                load_x(n).start()
        if b < BLOCKS - 1:
            works.append((next_norm(b), ROWS // 16))
            load_x(b + 1).wait()
        turns = sorted((k / count, index) for index, (_, count) in enumerate(works) for k in range(count))
        for _, index in turns:
            next(works[index][0])
        for work, _ in works:
            for _ in work:
                pass

    def mix(i):
        for b in range(BLOCKS):
            @pl.when(i == b)
            def _():
                mix_block(b)

    def down(half, quarter):
        cols = pl.ds(pl.multiple_of(half * 1024 + quarter * 512, 512), 512)
        return jnp.dot(om_v[...], wod_v[:, cols], preferred_element_type=F32)

    def down_other(b):
        @pl.when(b == 0)
        def _():
            for copy in load_od:
                copy.wait()

        for kind, quarter in ((D2D_FIRST, 1 - p2), (D2D_SECOND, p2)):
            part = down(1 - core, quarter).astype(BF16)
            for s in range(2):
                d2d_src[2 * b + s, kind] = part[s * HALF:(s + 1) * HALF]
            for s in range(2):
                copy_of(kind, 2 * b + s).start()

    def down_mine(b):
        part = down(core, 1 - p1)
        for s in range(2):
            u = 2 * b + s
            with jax.named_scope("recv"):
                copy_of(D2D_FIRST, u).wait_recv()
            h_send[u] = (part[s * HALF:(s + 1) * HALF] + d2d_dst[u, 0].astype(F32)).astype(BF16)
            copy_of(RED_ONE, u).start()
        part = down(core, p1)
        for s in range(2):
            u = 2 * b + s
            with jax.named_scope("recv"):
                copy_of(D2D_SECOND, u).wait_recv()
            h_keep[u] = part[s * HALF:(s + 1) * HALF] + d2d_dst[u, 1].astype(F32)

    def stage_b(u):
        with jax.named_scope("recv"):
            copy_of(RED_ONE, u).wait_recv()
        send = pl.ds(pl.multiple_of((1 - p2) * 256, 256), 256)
        keep = pl.ds(pl.multiple_of(p2 * 256, 256), 256)
        p_send[u] = (h_keep[u, :, send] + r1_dst[u, :, send].astype(F32)).astype(BF16)
        copy_of(RED_TWO, u).start()
        p_keep[u] = h_keep[u, :, keep] + r1_dst[u, :, keep].astype(F32)

    def stage_c(u):
        with jax.named_scope("recv"):
            copy_of(RED_TWO, u).wait_recv()
        cols = pl.ds(pl.multiple_of((mine + p2) * 256, 256), 256)
        x_f = x_v[half_rows(u), cols].astype(F32)
        y_v[half_rows(u), cols] = (x_f + (p_keep[u] + r2_dst[u].astype(F32))).astype(BF16)
        copy_of(GAT_ONE, u).start()

    def stage_d(u):
        with jax.named_scope("recv"):
            copy_of(GAT_ONE, u).wait_recv()
        copy_of(GAT_TWO, u).start()
        copy_of(OUT_FIRST, u).start()

    def stage_e(u):
        with jax.named_scope("recv"):
            copy_of(GAT_TWO, u).wait_recv()
        copy_of(OUT_SECOND, u).start()

    def stage_f(u):
        with jax.named_scope("recv"):
            copy_of(OUT_FIRST, u).wait_recv()
            copy_of(OUT_SECOND, u).wait_recv()

    stages = {"b": stage_b, "c": stage_c, "d": stage_d, "e": stage_e, "f": stage_f}

    def communicate(i, point):
        for name, ats in STAGE_AT:
            for s, at in enumerate(ats):
                if (at + 4 - point) % 5 == 0:
                    b = i - (at + 4 - point) // 5

                    @pl.when((b >= 0) & (b < BLOCKS))
                    def _():
                        with jax.named_scope("stage_" + name):
                            stages[name](2 * b + s)

    def step(i, carry):
        for point, part in enumerate((project, None, mix, down_other, down_mine)):
            if part is not None:
                @pl.when(i < BLOCKS)
                def _():
                    with jax.named_scope(part.__name__):
                        part(i)

            communicate(i, point)
        return carry

    lax.fori_loop(0, BLOCKS + DRAIN, step, 0)

    def finish(u, carry):
        for kind in range(8):
            copy_of(kind, u).wait_send()
        return carry

    with jax.named_scope("finish"):
        lax.fori_loop(0, UNITS, finish, 0)


def store_kernel(y_v, k_v, v_v, y_out, k_out, v_out, sem):
    copies = [pltpu.make_async_copy(k_v, k_out, sem.at[0]), pltpu.make_async_copy(v_v, v_out, sem.at[1])]
    for b in range(BLOCKS):
        rows = pl.ds(b * ROWS, ROWS)
        copies.append(pltpu.make_async_copy(y_v.at[rows, :], y_out.at[rows, :], sem.at[2 + b]))
    for copy in copies:
        copy.start()
    for copy in copies:
        copy.wait()


def solution(mesh):
    table = rope_table()

    def local_layer(x_in, g_norm, w_q, w_k, w_v, w_o, w_gate, w_up, w_down):
        any_spec = pl.BlockSpec(memory_space=pl.ANY)
        y, k, v = pl.pallas_call(
            layer_kernel,
            out_shape=(pltpu.VMEM((TOKENS, WIDTH), BF16), pltpu.VMEM((TOKENS, HEAD_DIM), BF16), pltpu.VMEM((TOKENS, HEAD_DIM), BF16)),
            in_specs=[any_spec] * 10,
            out_specs=(pl.BlockSpec(memory_space=pltpu.VMEM),) * 3,
            scratch_shapes=[
                pltpu.VMEM((TOKENS, WIDTH), BF16),
                pltpu.VMEM((WIDTH,), BF16),
                pltpu.VMEM((8, WIDTH), F32),
                pltpu.VMEM((WIDTH, QCOLS + 2 * HEAD_DIM), BF16),
                pltpu.VMEM((WIDTH, FFCOLS), BF16),
                pltpu.VMEM((WIDTH, FFCOLS), BF16),
                pltpu.VMEM((KDOWN, WIDTH), BF16),
                pltpu.VMEM((TOKENS, HEAD_DIM), F32),
                pltpu.VMEM((2, ROWS, WIDTH), BF16),
                pltpu.VMEM((2 * ROWS, HEAD_DIM), BF16),
                pltpu.VMEM((2, ROWS, TOKENS), F32),
                pltpu.VMEM((2, ROWS, TOKENS), BF16),
                pltpu.VMEM((ROWS, KDOWN), BF16),
                pltpu.VMEM((UNITS, 2, HALF, 512), BF16),
                pltpu.VMEM((UNITS, 2, HALF, 512), BF16),
                pltpu.VMEM((UNITS, HALF, 512), BF16),
                pltpu.VMEM((UNITS, HALF, 512), F32),
                pltpu.VMEM((UNITS, HALF, 512), BF16),
                pltpu.VMEM((UNITS, HALF, 256), BF16),
                pltpu.VMEM((UNITS, HALF, 256), F32),
                pltpu.VMEM((UNITS, HALF, 256), BF16),
                pltpu.SemaphoreType.DMA((BLOCKS + 3,)),
                pltpu.SemaphoreType.DMA((14,)),
                pltpu.SemaphoreType.DMA((8, UNITS)),
                pltpu.SemaphoreType.DMA((8, UNITS)),
            ],
            compiler_params=pltpu.CompilerParams(collective_id=0, has_side_effects=True, vmem_limit_bytes=67043328 - 8 * 1024 * 1024),
        )(x_in, g_norm, w_q, w_k, w_v, w_o, w_gate, w_up, w_down, jnp.asarray(table))
        y, k, v = pl.pallas_call(
            store_kernel,
            out_shape=(jax.ShapeDtypeStruct((TOKENS, WIDTH), BF16), jax.ShapeDtypeStruct((TOKENS, HEAD_DIM), BF16),
                       jax.ShapeDtypeStruct((TOKENS, HEAD_DIM), BF16)),
            in_specs=[any_spec] * 3,
            out_specs=(any_spec,) * 3,
            scratch_shapes=[pltpu.SemaphoreType.DMA((2 + BLOCKS,))],
            compiler_params=pltpu.CompilerParams(vmem_limit_bytes=1024 * 1024),
        )(*(pltpu.with_memory_space_constraint(part, pltpu.VMEM) for part in (y, k, v)))
        return y, k.reshape(TOKENS, 1, HEAD_DIM), v.reshape(TOKENS, 1, HEAD_DIM)

    return jax.shard_map(local_layer, mesh=mesh, in_specs=(P('dp', None), P(None), P(None, 'tp'), P(None, None), P(None, None), P('tp', None), P(None, 'tp'), P(None, 'tp'), P('tp', None)), out_specs=(P('dp', None), P('dp', 'tp', None), P('dp', 'tp', None)), check_vma=False)
```

```python
import math
import numpy as np
import jax
import jax.numpy as jnp
from jax import lax
from jax.experimental import pallas as pl
from jax.experimental.pallas import tpu as pltpu
from jax.sharding import PartitionSpec as P

HEAD_DIM = 128
ROPE_BASE = 500000.0
NORM_EPS = 1e-5
TOKENS = 1536
WIDTH = 2048
QCOLS = 256
FFCOLS = 768
ROWS = 256
BLOCKS = TOKENS // ROWS
KDOWN = QCOLS + FFCOLS
HALF = ROWS // 2
UNITS = TOKENS // HALF
STAGE_AT = (("b", (4, 4)), ("c", (8, 8)), ("d", (11, 11)), ("e", (19, 19)), ("f", (26, 26)))
DRAIN = 1 + max(max(at) for _, at in STAGE_AT) // 5
SCORE_SCALE = math.log2(math.e) / math.sqrt(HEAD_DIM)
F32 = jnp.float32
BF16 = jnp.bfloat16
MESH = pl.DeviceIdType.MESH

D2D_FIRST, D2D_SECOND, RED_ONE, RED_TWO, GAT_ONE, GAT_TWO, OUT_FIRST, OUT_SECOND = range(8)


def rope_table():
    inv_freq = np.float32(ROPE_BASE) ** (-np.arange(0, HEAD_DIM, 2, dtype=np.float32) / np.float32(HEAD_DIM))
    angles = np.arange(TOKENS, dtype=np.float32)[:, None] * inv_freq.astype(np.float32)[None, :]
    angles = angles.astype(np.float64)
    return np.concatenate([np.cos(angles), np.sin(angles)], axis=1).astype(np.float32)


def layer_kernel(x_hbm, g_hbm, wq_hbm, wk_hbm, wv_hbm, wo_hbm, wg_hbm, wu_hbm, wd_hbm, tab_hbm,
                 y_v, k_v, v_v,
                 x_v, g_v, gf_v, wqkv_v, wg_v, wu_v, wod_v, tab_v,
                 a_v, q_v, s_v, p_v, om_v,
                 d2d_src, d2d_dst, h_send, h_keep, r1_dst, p_send, p_keep, r2_dst,
                 x_sem, w_sem, ssem, rsem):
    me = lax.axis_index('tp')
    core = lax.rem(me, 2)
    xpos = lax.rem(me // 2, 2)
    ypos = me // 4
    sibling = me + 1 - 2 * core
    xpeer = me + 2 - 4 * xpos
    ypeer = me + 4 - 8 * ypos
    p1 = xpos + core * (ypos - xpos)
    p2 = ypos + core * (xpos - ypos)
    n1 = xpeer + core * (ypeer - xpeer)
    n2 = ypeer + core * (xpeer - ypeer)

    def rows_of(b):
        return pl.ds(pl.multiple_of(b * ROWS, ROWS), ROWS)

    def load(src, dst, index):
        return pltpu.make_async_copy(src, dst, w_sem.at[index])

    def load_x(b):
        return pltpu.make_async_copy(x_hbm.at[rows_of(b), :], x_v.at[rows_of(b), :], x_sem.at[b])

    def load_first(n):
        rows = pl.ds(n * 64, 64)
        return pltpu.make_async_copy(x_hbm.at[rows, :], x_v.at[rows, :], x_sem.at[0 if n == 0 else BLOCKS - 1 + n])

    kv_cols = pl.ds(pl.multiple_of(me * HEAD_DIM, HEAD_DIM), HEAD_DIM)
    early, late = pl.ds(0, ROWS), pl.ds(ROWS, TOKENS - ROWS)
    load_g = load(g_hbm, g_v, 0)
    load_qkv = [
        load(wk_hbm.at[:, kv_cols], wqkv_v.at[:, pl.ds(QCOLS, HEAD_DIM)], 1),
        load(wv_hbm.at[:, kv_cols], wqkv_v.at[:, pl.ds(QCOLS + HEAD_DIM, HEAD_DIM)], 2),
        load(wq_hbm, wqkv_v.at[:, pl.ds(0, QCOLS)], 3),
        load(tab_hbm.at[early, :], tab_v.at[early, :], 4),
    ]
    load_gu = []
    for n in range(FFCOLS // 256):
        tile = pl.ds(n * 256, 256)
        load_gu.append((load(wg_hbm.at[:, tile], wg_v.at[:, tile], 6 + 2 * n), load(wu_hbm.at[:, tile], wu_v.at[:, tile], 7 + 2 * n)))
    load_od = [load(wo_hbm, wod_v.at[pl.ds(0, QCOLS), :], 12), load(wd_hbm, wod_v.at[pl.ds(QCOLS, FFCOLS), :], 13)]
    load_tab = load(tab_hbm.at[late, :], tab_v.at[late, :], 5)

    load_g.start()
    for n in range(4):
        load_first(n).start()
    for copy in load_qkv:
        copy.start()

    barrier = pltpu.get_barrier_semaphore()
    for peer in (sibling, xpeer, ypeer):
        pl.semaphore_signal(barrier, inc=1, device_id={'tp': peer}, device_id_type=MESH)

    def remote(kind, u, src, dst, peer):
        return pltpu.make_async_remote_copy(src_ref=src, dst_ref=dst, send_sem=ssem.at[kind, u], recv_sem=rsem.at[kind, u],
                                            device_id={'tp': peer}, device_id_type=MESH)

    mine = core * 4 + p1 * 2
    other = core * 4 + (1 - p1) * 2

    def half_rows(u):
        return pl.ds(pl.multiple_of(u * HALF, HALF), HALF)

    def y_part(u, piece, count):
        return y_v.at[half_rows(u), pl.ds(pl.multiple_of(piece * 256, 256), count * 256)]

    def copy_of(kind, u):
        if kind == D2D_FIRST or kind == D2D_SECOND:
            return remote(kind, u, d2d_src.at[u, kind], d2d_dst.at[u, kind], sibling)
        if kind == RED_ONE:
            return remote(kind, u, h_send.at[u], r1_dst.at[u], n1)
        if kind == RED_TWO:
            return remote(kind, u, p_send.at[u], r2_dst.at[u], n2)
        if kind == GAT_ONE:
            part = y_part(u, mine + p2, 1)
            return remote(kind, u, part, part, n2)
        if kind == GAT_TWO:
            part = y_part(u, mine, 2)
            return remote(kind, u, part, part, n1)
        part = y_part(u, mine if kind == OUT_FIRST else other, 2)
        return remote(kind, u, part, part, sibling)

    def norm_rows(b, r):
        x_f = x_v[pl.ds(pl.multiple_of(b * ROWS + r * 16, 16), 16), :].astype(F32)
        inv = lax.rsqrt(jnp.mean(x_f * x_f, axis=-1, keepdims=True) + NORM_EPS)
        gain = jnp.concatenate([gf_v[...], gf_v[...]], axis=0)
        a_v[b % 2, pl.ds(r * 16, 16), :] = (x_f * inv * gain).astype(BF16)

    def project(b):
        @pl.when(b == 0)
        def _():
            load_g.wait()
            gf_v[...] = jnp.broadcast_to(g_v[...].astype(F32)[None, :], (8, WIDTH))
            for n in range(4):
                load_first(n).wait()
                if n < 3:
                    for copy in load_gu[n]:
                        copy.start()
                for r in range(n * 4, n * 4 + 4):
                    norm_rows(0, r)
            load_x(1).start()
            for copy in load_qkv:
                copy.wait()
            pl.semaphore_wait(barrier, 3)

        @pl.when(b == 1)
        def _():
            load_tab.wait()

        tab = tab_v[rows_of(b), :]
        swapped = pltpu.roll(tab, HEAD_DIM // 2, 1)
        low = lax.broadcasted_iota(jnp.int32, tab.shape, 1) < HEAD_DIM // 2
        cos = jnp.where(low, tab, swapped)
        sin = jnp.where(low, -swapped, tab)
        qkv = jnp.dot(a_v[lax.rem(b, 2)], wqkv_v[...], preferred_element_type=F32)

        def rope(h):
            return (h * cos + pltpu.roll(h, HEAD_DIM // 2, 1) * sin).astype(BF16)

        q_v[pl.ds(0, ROWS), :] = rope(qkv[:, 0:128])
        q_v[pl.ds(ROWS, ROWS), :] = rope(qkv[:, 128:256])
        k_v[rows_of(b), :] = rope(qkv[:, 256:384])
        v_v[rows_of(b), :] = qkv[:, 384:512].astype(BF16)

    def attention(b):
        def tile(j):
            return pl.ds(j * ROWS, ROWS)

        heads = range(2)
        peak, total, shift = [None] * 2, [None] * 2, [None] * 2
        for j in range(b + 1):
            for h in heads:
                q = q_v[pl.ds(h * ROWS, ROWS), :]
                s = lax.dot_general(q, k_v[tile(j), :], (((1,), (1,)), ((), ())), preferred_element_type=F32) * SCORE_SCALE
                if j == b:
                    qpos = lax.broadcasted_iota(jnp.int32, (ROWS, ROWS), 0)
                    kpos = lax.broadcasted_iota(jnp.int32, (ROWS, ROWS), 1)
                    s = jnp.where(kpos <= qpos, s, -1e30)
                s_v[h, :, tile(j)] = s
                pair = jnp.maximum(s[:, :128], s[:, 128:])
                peak[h] = pair if j == 0 else jnp.maximum(peak[h], pair)
                yield
        for h in heads:
            peak[h] = jnp.max(peak[h], axis=1, keepdims=True)
        for j in range(b + 1):
            for h in heads:
                e = jnp.exp2(s_v[h, :, tile(j)] - peak[h])
                pair = e[:, :128] + e[:, 128:]
                total[h] = pair if j == 0 else total[h] + pair
                yield
        for h in heads:
            shift[h] = peak[h] + jnp.log2(jnp.sum(total[h], axis=1, keepdims=True))
        for j in range(b + 1):
            for h in heads:
                p_v[h, :, tile(j)] = jnp.exp2(s_v[h, :, tile(j)] - shift[h]).astype(BF16)
                yield
        keys = pl.ds(0, (b + 1) * ROWS)
        for h in heads:
            o = jnp.dot(p_v[h, :, keys], v_v[keys, :], preferred_element_type=F32)
            om_v[:, pl.ds(h * HEAD_DIM, HEAD_DIM)] = o.astype(BF16)
            yield

    def gate_up(b):
        normed = a_v.at[b % 2]
        for n in range(FFCOLS // 256):
            if b == 0:
                for copy in load_gu[n]:
                    copy.wait()
            cols = pl.ds(n * 256, 256)
            gate = jnp.dot(normed[...], wg_v[:, cols], preferred_element_type=F32)
            yield
            up = jnp.dot(normed[...], wu_v[:, cols], preferred_element_type=F32)
            om_v[:, pl.ds(QCOLS + n * 256, 256)] = (gate * (1.0 / (1.0 + jnp.exp(-gate))) * up).astype(BF16)
            yield

    def next_norm(b):
        if b == 0:
            load_x(1).wait()
        for r in range(ROWS // 16):
            norm_rows(b + 1, r)
            yield

    def mix_block(b):
        works = [(gate_up(b), [k / 6 for k in range(6)])]
        count = 6 * (b + 1) + 2
        works.append((attention(b), [k / count for k in range(count)]))
        if b == 0:
            for copy in load_od:
                copy.start()
        if b < BLOCKS - 1:
            count = ROWS // 16
            if b > 0:
                load_x(b + 1).wait()
            works.append((next_norm(b), [k / count if b else 0.6 + 0.4 * k / count for k in range(count)]))
        turns = sorted((turn, index) for index, (_, turns) in enumerate(works) for turn in turns)
        for _, index in turns:
            next(works[index][0])
        for work, _ in works:
            for _ in work:
                pass

    def mix(i):
        for b in range(BLOCKS):
            @pl.when(i == b)
            def _():
                mix_block(b)

    def down(half, quarter):
        cols = pl.ds(pl.multiple_of(half * 1024 + quarter * 512, 512), 512)
        return jnp.dot(om_v[...], wod_v[:, cols], preferred_element_type=F32)

    def down_other(b):
        @pl.when(b == 0)
        def _():
            load_tab.start()
            for n in range(2, BLOCKS):
                load_x(n).start()
            for copy in load_od:
                copy.wait()

        for kind, quarter in ((D2D_FIRST, 1 - p2), (D2D_SECOND, p2)):
            part = down(1 - core, quarter).astype(BF16)
            for s in range(2):
                d2d_src[2 * b + s, kind] = part[s * HALF:(s + 1) * HALF]
            for s in range(2):
                copy_of(kind, 2 * b + s).start()

    def down_mine(b):
        part = down(core, 1 - p1)
        for s in range(2):
            u = 2 * b + s
            with jax.named_scope("recv"):
                copy_of(D2D_FIRST, u).wait_recv()
            h_send[u] = (part[s * HALF:(s + 1) * HALF] + d2d_dst[u, 0].astype(F32)).astype(BF16)
            copy_of(RED_ONE, u).start()
        part = down(core, p1)
        for s in range(2):
            u = 2 * b + s
            with jax.named_scope("recv"):
                copy_of(D2D_SECOND, u).wait_recv()
            h_keep[u] = part[s * HALF:(s + 1) * HALF] + d2d_dst[u, 1].astype(F32)

    def stage_b(u):
        with jax.named_scope("recv"):
            copy_of(RED_ONE, u).wait_recv()
        send = pl.ds(pl.multiple_of((1 - p2) * 256, 256), 256)
        keep = pl.ds(pl.multiple_of(p2 * 256, 256), 256)
        p_send[u] = (h_keep[u, :, send] + r1_dst[u, :, send].astype(F32)).astype(BF16)
        copy_of(RED_TWO, u).start()
        p_keep[u] = h_keep[u, :, keep] + r1_dst[u, :, keep].astype(F32)

    def stage_c(u):
        with jax.named_scope("recv"):
            copy_of(RED_TWO, u).wait_recv()
        cols = pl.ds(pl.multiple_of((mine + p2) * 256, 256), 256)
        x_f = x_v[half_rows(u), cols].astype(F32)
        y_v[half_rows(u), cols] = (x_f + (p_keep[u] + r2_dst[u].astype(F32))).astype(BF16)
        copy_of(GAT_ONE, u).start()

    def stage_d(u):
        with jax.named_scope("recv"):
            copy_of(GAT_ONE, u).wait_recv()
        copy_of(GAT_TWO, u).start()
        copy_of(OUT_FIRST, u).start()

    def stage_e(u):
        with jax.named_scope("recv"):
            copy_of(GAT_TWO, u).wait_recv()
        copy_of(OUT_SECOND, u).start()

    def stage_f(u):
        with jax.named_scope("recv"):
            copy_of(OUT_FIRST, u).wait_recv()
            copy_of(OUT_SECOND, u).wait_recv()

    stages = {"b": stage_b, "c": stage_c, "d": stage_d, "e": stage_e, "f": stage_f}

    def communicate(i, point):
        for name, ats in STAGE_AT:
            for s, at in enumerate(ats):
                if (at + 4 - point) % 5 == 0:
                    b = i - (at + 4 - point) // 5

                    @pl.when((b >= 0) & (b < BLOCKS))
                    def _():
                        with jax.named_scope("stage_" + name):
                            stages[name](2 * b + s)

    def step(i, carry):
        for point, part in enumerate((project, None, mix, down_other, down_mine)):
            if part is not None:
                @pl.when(i < BLOCKS)
                def _():
                    with jax.named_scope(part.__name__):
                        part(i)

            communicate(i, point)
        return carry

    lax.fori_loop(0, BLOCKS + DRAIN, step, 0)

    def finish(u, carry):
        for kind in range(8):
            copy_of(kind, u).wait_send()
        return carry

    with jax.named_scope("finish"):
        lax.fori_loop(0, UNITS, finish, 0)


def store_kernel(y_v, k_v, v_v, y_out, k_out, v_out, sem):
    copies = [pltpu.make_async_copy(k_v, k_out, sem.at[0]), pltpu.make_async_copy(v_v, v_out, sem.at[1])]
    for b in range(BLOCKS):
        rows = pl.ds(b * ROWS, ROWS)
        copies.append(pltpu.make_async_copy(y_v.at[rows, :], y_out.at[rows, :], sem.at[2 + b]))
    for copy in copies:
        copy.start()
    for copy in copies:
        copy.wait()


def solution(mesh):
    table = rope_table()

    def local_layer(x_in, g_norm, w_q, w_k, w_v, w_o, w_gate, w_up, w_down):
        any_spec = pl.BlockSpec(memory_space=pl.ANY)
        y, k, v = pl.pallas_call(
            layer_kernel,
            out_shape=(pltpu.VMEM((TOKENS, WIDTH), BF16), pltpu.VMEM((TOKENS, HEAD_DIM), BF16), pltpu.VMEM((TOKENS, HEAD_DIM), BF16)),
            in_specs=[any_spec] * 10,
            out_specs=(pl.BlockSpec(memory_space=pltpu.VMEM),) * 3,
            scratch_shapes=[
                pltpu.VMEM((TOKENS, WIDTH), BF16),
                pltpu.VMEM((WIDTH,), BF16),
                pltpu.VMEM((8, WIDTH), F32),
                pltpu.VMEM((WIDTH, QCOLS + 2 * HEAD_DIM), BF16),
                pltpu.VMEM((WIDTH, FFCOLS), BF16),
                pltpu.VMEM((WIDTH, FFCOLS), BF16),
                pltpu.VMEM((KDOWN, WIDTH), BF16),
                pltpu.VMEM((TOKENS, HEAD_DIM), F32),
                pltpu.VMEM((2, ROWS, WIDTH), BF16),
                pltpu.VMEM((2 * ROWS, HEAD_DIM), BF16),
                pltpu.VMEM((2, ROWS, TOKENS), F32),
                pltpu.VMEM((2, ROWS, TOKENS), BF16),
                pltpu.VMEM((ROWS, KDOWN), BF16),
                pltpu.VMEM((UNITS, 2, HALF, 512), BF16),
                pltpu.VMEM((UNITS, 2, HALF, 512), BF16),
                pltpu.VMEM((UNITS, HALF, 512), BF16),
                pltpu.VMEM((UNITS, HALF, 512), F32),
                pltpu.VMEM((UNITS, HALF, 512), BF16),
                pltpu.VMEM((UNITS, HALF, 256), BF16),
                pltpu.VMEM((UNITS, HALF, 256), F32),
                pltpu.VMEM((UNITS, HALF, 256), BF16),
                pltpu.SemaphoreType.DMA((BLOCKS + 3,)),
                pltpu.SemaphoreType.DMA((14,)),
                pltpu.SemaphoreType.DMA((8, UNITS)),
                pltpu.SemaphoreType.DMA((8, UNITS)),
            ],
            compiler_params=pltpu.CompilerParams(collective_id=0, has_side_effects=True, vmem_limit_bytes=67043328 - 8 * 1024 * 1024),
        )(x_in, g_norm, w_q, w_k, w_v, w_o, w_gate, w_up, w_down, jnp.asarray(table))
        y, k, v = pl.pallas_call(
            store_kernel,
            out_shape=(jax.ShapeDtypeStruct((TOKENS, WIDTH), BF16), jax.ShapeDtypeStruct((TOKENS, HEAD_DIM), BF16),
                       jax.ShapeDtypeStruct((TOKENS, HEAD_DIM), BF16)),
            in_specs=[any_spec] * 3,
            out_specs=(any_spec,) * 3,
            scratch_shapes=[pltpu.SemaphoreType.DMA((2 + BLOCKS,))],
            compiler_params=pltpu.CompilerParams(vmem_limit_bytes=1024 * 1024),
        )(*(pltpu.with_memory_space_constraint(part, pltpu.VMEM) for part in (y, k, v)))
        return y, k.reshape(TOKENS, 1, HEAD_DIM), v.reshape(TOKENS, 1, HEAD_DIM)

    return jax.shard_map(local_layer, mesh=mesh, in_specs=(P('dp', None), P(None), P(None, 'tp'), P(None, None), P(None, None), P('tp', None), P(None, 'tp'), P(None, 'tp'), P('tp', None)), out_specs=(P('dp', None), P('dp', 'tp', None), P('dp', 'tp', None)), check_vma=False)
```

```python
import math
import numpy as np
import jax
import jax.numpy as jnp
from jax import lax
from jax.experimental import pallas as pl
from jax.experimental.pallas import tpu as pltpu
from jax.sharding import PartitionSpec as P

HEAD_DIM = 128
ROPE_BASE = 500000.0
NORM_EPS = 1e-5
TOKENS = 1536
WIDTH = 2048
QCOLS = 256
FFCOLS = 768
ROWS = 256
BLOCKS = TOKENS // ROWS
KDOWN = QCOLS + FFCOLS
HALF = ROWS // 2
UNITS = TOKENS // HALF
STAGE_SLOTS = {
    "b": (7, 8, 12, 14, 19, 20, 24, 28, 32, 49, 50, 61),
    "c": (10, 12, 16, 21, 23, 30, 44, 57, 57, 64, 66, 74),
    "d": (13, 17, 18, 26, 27, 42, 58, 70, 75, 75, 79, 79),
    "e": (22, 27, 31, 46, 49, 62, 76, 77, 82, 85, 90, 105),
    "f": (41, 51, 61, 61, 85, 87, 88, 94, 107, 110, 118, 125),
}
SCORE_SCALE = math.log2(math.e) / math.sqrt(HEAD_DIM)
F32 = jnp.float32
BF16 = jnp.bfloat16
MESH = pl.DeviceIdType.MESH

D2D_FIRST, D2D_SECOND, RED_ONE, RED_TWO, GAT_ONE, GAT_TWO, OUT_FIRST, OUT_SECOND = range(8)


def rope_table():
    inv_freq = np.float32(ROPE_BASE) ** (-np.arange(0, HEAD_DIM, 2, dtype=np.float32) / np.float32(HEAD_DIM))
    angles = np.arange(TOKENS, dtype=np.float32)[:, None] * inv_freq.astype(np.float32)[None, :]
    angles = angles.astype(np.float64)
    return np.concatenate([np.cos(angles), np.sin(angles)], axis=1).astype(np.float32)


def layer_kernel(x_hbm, g_hbm, wq_hbm, wk_hbm, wv_hbm, wo_hbm, wg_hbm, wu_hbm, wd_hbm, tab_hbm,
                 y_v, k_v, v_v,
                 x_v, g_v, gf_v, wqkv_v, wg_v, wu_v, wod_v, tab_v,
                 a_v, q_v, s_v, p_v, om_v,
                 d2d_src, d2d_dst, h_send, h_keep, r1_dst, p_send, p_keep, r2_dst,
                 x_sem, w_sem, ssem, rsem):
    me = lax.axis_index('tp')
    core = lax.rem(me, 2)
    xpos = lax.rem(me // 2, 2)
    ypos = me // 4
    sibling = me + 1 - 2 * core
    xpeer = me + 2 - 4 * xpos
    ypeer = me + 4 - 8 * ypos
    p1 = xpos + core * (ypos - xpos)
    p2 = ypos + core * (xpos - ypos)
    n1 = xpeer + core * (ypeer - xpeer)
    n2 = ypeer + core * (xpeer - ypeer)

    def rows_of(b):
        return pl.ds(pl.multiple_of(b * ROWS, ROWS), ROWS)

    def load(src, dst, index):
        return pltpu.make_async_copy(src, dst, w_sem.at[index])

    def load_x(b):
        return pltpu.make_async_copy(x_hbm.at[rows_of(b), :], x_v.at[rows_of(b), :], x_sem.at[b])

    def load_first(n):
        rows = pl.ds(n * 64, 64)
        return pltpu.make_async_copy(x_hbm.at[rows, :], x_v.at[rows, :], x_sem.at[0 if n == 0 else BLOCKS - 1 + n])

    kv_cols = pl.ds(pl.multiple_of(me * HEAD_DIM, HEAD_DIM), HEAD_DIM)
    early, late = pl.ds(0, ROWS), pl.ds(ROWS, TOKENS - ROWS)
    load_g = load(g_hbm, g_v, 0)
    load_qkv = [
        load(wk_hbm.at[:, kv_cols], wqkv_v.at[:, pl.ds(QCOLS, HEAD_DIM)], 1),
        load(wv_hbm.at[:, kv_cols], wqkv_v.at[:, pl.ds(QCOLS + HEAD_DIM, HEAD_DIM)], 2),
        load(wq_hbm, wqkv_v.at[:, pl.ds(0, QCOLS)], 3),
        load(tab_hbm.at[early, :], tab_v.at[early, :], 4),
    ]
    load_gu = []
    for n in range(FFCOLS // 256):
        tile = pl.ds(n * 256, 256)
        load_gu.append((load(wg_hbm.at[:, tile], wg_v.at[:, tile], 6 + 2 * n), load(wu_hbm.at[:, tile], wu_v.at[:, tile], 7 + 2 * n)))
    load_od = []
    for n, half in enumerate((1 - core, core)):
        cols = pl.ds(pl.multiple_of(half * 1024, 1024), 1024)
        load_od.append((load(wo_hbm.at[:, cols], wod_v.at[pl.ds(0, QCOLS), cols], 12 + 2 * n),
                        load(wd_hbm.at[:, cols], wod_v.at[pl.ds(QCOLS, FFCOLS), cols], 13 + 2 * n)))
    load_tab = load(tab_hbm.at[late, :], tab_v.at[late, :], 5)

    load_g.start()
    for n in range(4):
        load_first(n).start()
    for copy in load_qkv:
        copy.start()

    barrier = pltpu.get_barrier_semaphore()
    for peer in (sibling, xpeer, ypeer):
        pl.semaphore_signal(barrier, inc=1, device_id={'tp': peer}, device_id_type=MESH)

    def remote(kind, u, src, dst, peer):
        return pltpu.make_async_remote_copy(src_ref=src, dst_ref=dst, send_sem=ssem.at[kind, u], recv_sem=rsem.at[kind, u],
                                            device_id={'tp': peer}, device_id_type=MESH)

    mine = core * 4 + p1 * 2
    other = core * 4 + (1 - p1) * 2

    def half_rows(u):
        return pl.ds(pl.multiple_of(u * HALF, HALF), HALF)

    def y_part(u, piece, count):
        return y_v.at[half_rows(u), pl.ds(pl.multiple_of(piece * 256, 256), count * 256)]

    def copy_of(kind, u):
        if kind == D2D_FIRST or kind == D2D_SECOND:
            return remote(kind, u, d2d_src.at[u, kind], d2d_dst.at[u, kind], sibling)
        if kind == RED_ONE:
            return remote(kind, u, h_send.at[u], r1_dst.at[u], n1)
        if kind == RED_TWO:
            return remote(kind, u, p_send.at[u], r2_dst.at[u], n2)
        if kind == GAT_ONE:
            part = y_part(u, mine + p2, 1)
            return remote(kind, u, part, part, n2)
        if kind == GAT_TWO:
            part = y_part(u, mine, 2)
            return remote(kind, u, part, part, n1)
        part = y_part(u, mine if kind == OUT_FIRST else other, 2)
        return remote(kind, u, part, part, sibling)

    def norm_rows(b, r):
        x_f = x_v[pl.ds(pl.multiple_of(b * ROWS + r * 16, 16), 16), :].astype(F32)
        inv = lax.rsqrt(jnp.mean(x_f * x_f, axis=-1, keepdims=True) + NORM_EPS)
        gain = jnp.concatenate([gf_v[...], gf_v[...]], axis=0)
        a_v[b % 2, pl.ds(r * 16, 16), :] = (x_f * inv * gain).astype(BF16)

    def project(b):
        @pl.when(b == 0)
        def _():
            load_g.wait()
            gf_v[...] = jnp.broadcast_to(g_v[...].astype(F32)[None, :], (8, WIDTH))
            for n in range(4):
                load_first(n).wait()
                if n < 3:
                    for copy in load_gu[n]:
                        copy.start()
                for r in range(n * 4, n * 4 + 4):
                    norm_rows(0, r)
            for copy in load_qkv:
                copy.wait()
            pl.semaphore_wait(barrier, 3)

        @pl.when(b == 1)
        def _():
            load_tab.wait()

        tab = tab_v[rows_of(b), :]
        swapped = pltpu.roll(tab, HEAD_DIM // 2, 1)
        low = lax.broadcasted_iota(jnp.int32, tab.shape, 1) < HEAD_DIM // 2
        cos = jnp.where(low, tab, swapped)
        sin = jnp.where(low, -swapped, tab)
        qkv = jnp.dot(a_v[lax.rem(b, 2)], wqkv_v[...], preferred_element_type=F32)

        def rope(h):
            return (h * cos + pltpu.roll(h, HEAD_DIM // 2, 1) * sin).astype(BF16)

        q_v[pl.ds(0, ROWS), :] = rope(qkv[:, 0:128])
        q_v[pl.ds(ROWS, ROWS), :] = rope(qkv[:, 128:256])
        k_v[rows_of(b), :] = rope(qkv[:, 256:384])
        v_v[rows_of(b), :] = qkv[:, 384:512].astype(BF16)

    def attention(b):
        def tile(j):
            return pl.ds(j * ROWS, ROWS)

        heads = range(2)
        peak, total, shift = [None] * 2, [None] * 2, [None] * 2
        for j in range(b + 1):
            for h in heads:
                q = q_v[pl.ds(h * ROWS, ROWS), :]
                s = lax.dot_general(q, k_v[tile(j), :], (((1,), (1,)), ((), ())), preferred_element_type=F32) * SCORE_SCALE
                if j == b:
                    qpos = lax.broadcasted_iota(jnp.int32, (ROWS, ROWS), 0)
                    kpos = lax.broadcasted_iota(jnp.int32, (ROWS, ROWS), 1)
                    s = jnp.where(kpos <= qpos, s, -1e30)
                s_v[h, :, tile(j)] = s
                pair = jnp.maximum(s[:, :128], s[:, 128:])
                peak[h] = pair if j == 0 else jnp.maximum(peak[h], pair)
                yield
        for h in heads:
            peak[h] = jnp.max(peak[h], axis=1, keepdims=True)
        for j in range(b + 1):
            for h in heads:
                e = jnp.exp2(s_v[h, :, tile(j)] - peak[h])
                pair = e[:, :128] + e[:, 128:]
                total[h] = pair if j == 0 else total[h] + pair
                yield
        for h in heads:
            shift[h] = peak[h] + jnp.log2(jnp.sum(total[h], axis=1, keepdims=True))
        for j in range(b + 1):
            for h in heads:
                p_v[h, :, tile(j)] = jnp.exp2(s_v[h, :, tile(j)] - shift[h]).astype(BF16)
                yield
        keys = pl.ds(0, (b + 1) * ROWS)
        for h in heads:
            o = jnp.dot(p_v[h, :, keys], v_v[keys, :], preferred_element_type=F32)
            om_v[:, pl.ds(h * HEAD_DIM, HEAD_DIM)] = o.astype(BF16)
            yield

    def gate_up(b):
        normed = a_v.at[b % 2]
        for n in range(FFCOLS // 256):
            if b == 0:
                for copy in load_gu[n]:
                    copy.wait()
            cols = pl.ds(n * 256, 256)
            gate = jnp.dot(normed[...], wg_v[:, cols], preferred_element_type=F32)
            yield
            up = jnp.dot(normed[...], wu_v[:, cols], preferred_element_type=F32)
            om_v[:, pl.ds(QCOLS + n * 256, 256)] = (gate * (1.0 / (1.0 + jnp.exp(-gate))) * up).astype(BF16)
            yield

    def next_norm(b):
        for r in range(ROWS // 16):
            norm_rows(b + 1, r)
            yield

    def mix_block(b):
        works = [(gate_up(b), [k / 6 for k in range(6)])]
        count = 6 * (b + 1) + 2
        works.append((attention(b), [k / count for k in range(count)]))
        if b == 0:
            for copy in load_od[0]:
                copy.start()
            load_x(1).start()
            for copy in load_od[1]:
                copy.start()
        elif b < BLOCKS - 1:
            count = ROWS // 16
            load_x(b + 1).wait()
            works.append((next_norm(b), [k / count for k in range(count)]))
        turns = sorted((turn, index) for index, (_, turns) in enumerate(works) for turn in turns)
        for _, index in turns:
            next(works[index][0])
        for work, _ in works:
            for _ in work:
                pass

    def mix(i):
        for b in range(BLOCKS):
            @pl.when(i == b)
            def _():
                mix_block(b)

    def down(half, quarter):
        cols = pl.ds(pl.multiple_of(half * 1024 + quarter * 512, 512), 512)
        return jnp.dot(om_v[...], wod_v[:, cols], preferred_element_type=F32)

    def down_other(b):
        def halves(u, after):
            for kind, quarter in ((D2D_FIRST, 1 - p2), (D2D_SECOND, p2)):
                part = down(1 - core, quarter).astype(BF16)
                for s in range(2):
                    d2d_src[u + s, kind] = part[s * HALF:(s + 1) * HALF]
                for s in range(2):
                    copy_of(kind, u + s).start()
                for r in range(8 * kind, 8 * kind + 8) if after else ():
                    norm_rows(1, r)

        @pl.when(b == 0)
        def _():
            for copy in load_od[0]:
                copy.wait()
            load_x(1).wait()
            load_tab.start()
            for n in range(2, BLOCKS):
                load_x(n).start()
            halves(0, True)

        @pl.when(b > 0)
        def _():
            halves(2 * b, False)

    def down_mine(b):
        @pl.when(b == 0)
        def _():
            for copy in load_od[1]:
                copy.wait()

        part = down(core, 1 - p1)
        for s in range(2):
            u = 2 * b + s
            with jax.named_scope("recv"):
                copy_of(D2D_FIRST, u).wait_recv()
            h_send[u] = (part[s * HALF:(s + 1) * HALF] + d2d_dst[u, 0].astype(F32)).astype(BF16)
            copy_of(RED_ONE, u).start()
        part = down(core, p1)
        for s in range(2):
            u = 2 * b + s
            with jax.named_scope("recv"):
                copy_of(D2D_SECOND, u).wait_recv()
            h_keep[u] = part[s * HALF:(s + 1) * HALF] + d2d_dst[u, 1].astype(F32)

    def stage_b(u):
        with jax.named_scope("recv"):
            copy_of(RED_ONE, u).wait_recv()
        send = pl.ds(pl.multiple_of((1 - p2) * 256, 256), 256)
        keep = pl.ds(pl.multiple_of(p2 * 256, 256), 256)
        p_send[u] = (h_keep[u, :, send] + r1_dst[u, :, send].astype(F32)).astype(BF16)
        copy_of(RED_TWO, u).start()
        p_keep[u] = h_keep[u, :, keep] + r1_dst[u, :, keep].astype(F32)

    def stage_c(u):
        with jax.named_scope("recv"):
            copy_of(RED_TWO, u).wait_recv()
        cols = pl.ds(pl.multiple_of((mine + p2) * 256, 256), 256)
        x_f = x_v[half_rows(u), cols].astype(F32)
        y_v[half_rows(u), cols] = (x_f + (p_keep[u] + r2_dst[u].astype(F32))).astype(BF16)
        copy_of(GAT_ONE, u).start()

    def stage_d(u):
        with jax.named_scope("recv"):
            copy_of(GAT_ONE, u).wait_recv()
        copy_of(GAT_TWO, u).start()
        copy_of(OUT_FIRST, u).start()

    def stage_e(u):
        with jax.named_scope("recv"):
            copy_of(GAT_TWO, u).wait_recv()
        copy_of(OUT_SECOND, u).start()

    def stage_f(u):
        with jax.named_scope("recv"):
            copy_of(OUT_FIRST, u).wait_recv()
            copy_of(OUT_SECOND, u).wait_recv()

    stages = {"b": stage_b, "c": stage_c, "d": stage_d, "e": stage_e, "f": stage_f}

    slots = {}
    for name in "bcdef":
        for u in range(UNITS):
            slots.setdefault(STAGE_SLOTS[name][u], []).append((name, u))

    def communicate(slot):
        for name, u in slots.get(slot, ()):
            with jax.named_scope("stage_" + name):
                stages[name](u)

    def step(i, carry):
        for point, part in enumerate((project, None, mix, down_other, down_mine)):
            if part is not None:
                with jax.named_scope(part.__name__):
                    part(i)
            for b in range(BLOCKS):
                if 5 * b + point in slots:
                    @pl.when(i == b)
                    def _():
                        communicate(5 * b + point)

        return carry

    lax.fori_loop(0, BLOCKS, step, 0)
    for slot in range(5 * BLOCKS, max(slots) + 1):
        communicate(slot)

    def finish(u, carry):
        for kind in range(8):
            copy_of(kind, u).wait_send()
        return carry

    with jax.named_scope("finish"):
        lax.fori_loop(0, UNITS, finish, 0)


def store_kernel(y_v, k_v, v_v, y_out, k_out, v_out, sem):
    copies = [pltpu.make_async_copy(k_v, k_out, sem.at[0]), pltpu.make_async_copy(v_v, v_out, sem.at[1])]
    for b in range(BLOCKS):
        rows = pl.ds(b * ROWS, ROWS)
        copies.append(pltpu.make_async_copy(y_v.at[rows, :], y_out.at[rows, :], sem.at[2 + b]))
    for copy in copies:
        copy.start()
    for copy in copies:
        copy.wait()


def solution(mesh):
    table = rope_table()

    def local_layer(x_in, g_norm, w_q, w_k, w_v, w_o, w_gate, w_up, w_down):
        any_spec = pl.BlockSpec(memory_space=pl.ANY)
        y, k, v = pl.pallas_call(
            layer_kernel,
            out_shape=(pltpu.VMEM((TOKENS, WIDTH), BF16), pltpu.VMEM((TOKENS, HEAD_DIM), BF16), pltpu.VMEM((TOKENS, HEAD_DIM), BF16)),
            in_specs=[any_spec] * 10,
            out_specs=(pl.BlockSpec(memory_space=pltpu.VMEM),) * 3,
            scratch_shapes=[
                pltpu.VMEM((TOKENS, WIDTH), BF16),
                pltpu.VMEM((WIDTH,), BF16),
                pltpu.VMEM((8, WIDTH), F32),
                pltpu.VMEM((WIDTH, QCOLS + 2 * HEAD_DIM), BF16),
                pltpu.VMEM((WIDTH, FFCOLS), BF16),
                pltpu.VMEM((WIDTH, FFCOLS), BF16),
                pltpu.VMEM((KDOWN, WIDTH), BF16),
                pltpu.VMEM((TOKENS, HEAD_DIM), F32),
                pltpu.VMEM((2, ROWS, WIDTH), BF16),
                pltpu.VMEM((2 * ROWS, HEAD_DIM), BF16),
                pltpu.VMEM((2, ROWS, TOKENS), F32),
                pltpu.VMEM((2, ROWS, TOKENS), BF16),
                pltpu.VMEM((ROWS, KDOWN), BF16),
                pltpu.VMEM((UNITS, 2, HALF, 512), BF16),
                pltpu.VMEM((UNITS, 2, HALF, 512), BF16),
                pltpu.VMEM((UNITS, HALF, 512), BF16),
                pltpu.VMEM((UNITS, HALF, 512), F32),
                pltpu.VMEM((UNITS, HALF, 512), BF16),
                pltpu.VMEM((UNITS, HALF, 256), BF16),
                pltpu.VMEM((UNITS, HALF, 256), F32),
                pltpu.VMEM((UNITS, HALF, 256), BF16),
                pltpu.SemaphoreType.DMA((BLOCKS + 3,)),
                pltpu.SemaphoreType.DMA((16,)),
                pltpu.SemaphoreType.DMA((8, UNITS)),
                pltpu.SemaphoreType.DMA((8, UNITS)),
            ],
            compiler_params=pltpu.CompilerParams(collective_id=0, has_side_effects=True, vmem_limit_bytes=67043328 - 8 * 1024 * 1024),
        )(x_in, g_norm, w_q, w_k, w_v, w_o, w_gate, w_up, w_down, jnp.asarray(table))
        y, k, v = pl.pallas_call(
            store_kernel,
            out_shape=(jax.ShapeDtypeStruct((TOKENS, WIDTH), BF16), jax.ShapeDtypeStruct((TOKENS, HEAD_DIM), BF16),
                       jax.ShapeDtypeStruct((TOKENS, HEAD_DIM), BF16)),
            in_specs=[any_spec] * 3,
            out_specs=(any_spec,) * 3,
            scratch_shapes=[pltpu.SemaphoreType.DMA((2 + BLOCKS,))],
            compiler_params=pltpu.CompilerParams(vmem_limit_bytes=1024 * 1024),
        )(*(pltpu.with_memory_space_constraint(part, pltpu.VMEM) for part in (y, k, v)))
        return y, k.reshape(TOKENS, 1, HEAD_DIM), v.reshape(TOKENS, 1, HEAD_DIM)

    return jax.shard_map(local_layer, mesh=mesh, in_specs=(P('dp', None), P(None), P(None, 'tp'), P(None, None), P(None, None), P('tp', None), P(None, 'tp'), P(None, 'tp'), P('tp', None)), out_specs=(P('dp', None), P('dp', 'tp', None), P('dp', 'tp', None)), check_vma=False)
```

```python
import math
import numpy as np
import jax
import jax.numpy as jnp
from jax import lax
from jax.experimental import pallas as pl
from jax.experimental.pallas import tpu as pltpu
from jax.sharding import PartitionSpec as P

HEAD_DIM = 128
ROPE_BASE = 500000.0
NORM_EPS = 1e-5
TOKENS = 1536
WIDTH = 2048
QCOLS = 256
FFCOLS = 768
ROWS = 256
BLOCKS = TOKENS // ROWS
KDOWN = QCOLS + FFCOLS
HALF = ROWS // 2
UNITS = TOKENS // HALF
STAGE_SLOTS = {
    "b": (7, 8, 12, 14, 19, 20, 24, 28, 32, 49, 50, 61),
    "c": (10, 12, 16, 21, 23, 30, 44, 57, 57, 64, 66, 74),
    "d": (13, 17, 18, 26, 27, 42, 58, 70, 75, 75, 79, 79),
    "e": (22, 27, 31, 46, 49, 62, 76, 77, 82, 85, 90, 105),
}
SCORE_SCALE = math.log2(math.e) / math.sqrt(HEAD_DIM)
F32 = jnp.float32
BF16 = jnp.bfloat16
MESH = pl.DeviceIdType.MESH

D2D_FIRST, D2D_SECOND, RED_ONE, RED_TWO, GAT_ONE, GAT_TWO, OUT_FIRST, OUT_SECOND = range(8)


def rope_table():
    inv_freq = np.float32(ROPE_BASE) ** (-np.arange(0, HEAD_DIM, 2, dtype=np.float32) / np.float32(HEAD_DIM))
    angles = np.arange(TOKENS, dtype=np.float32)[:, None] * inv_freq.astype(np.float32)[None, :]
    angles = angles.astype(np.float64)
    return np.concatenate([np.cos(angles), np.sin(angles)], axis=1).astype(np.float32)


def layer_kernel(x_hbm, g_hbm, wq_hbm, wk_hbm, wv_hbm, wo_hbm, wg_hbm, wu_hbm, wd_hbm, tab_hbm,
                 y_v, k_v, v_v,
                 x_v, g_v, gf_v, wqkv_v, wg_v, wu_v, wod_v, tab_v,
                 a_v, q_v, s_v, p_v, om_v,
                 d2d_src, d2d_dst, h_send, h_keep, r1_dst, p_send, p_keep, r2_dst,
                 x_sem, w_sem, ssem, pair_sem, link_sem, out_sem):
    me = lax.axis_index('tp')
    core = lax.rem(me, 2)
    xpos = lax.rem(me // 2, 2)
    ypos = me // 4
    sibling = me + 1 - 2 * core
    xpeer = me + 2 - 4 * xpos
    ypeer = me + 4 - 8 * ypos
    p1 = xpos + core * (ypos - xpos)
    p2 = ypos + core * (xpos - ypos)
    n1 = xpeer + core * (ypeer - xpeer)
    n2 = ypeer + core * (xpeer - ypeer)

    def rows_of(b):
        return pl.ds(pl.multiple_of(b * ROWS, ROWS), ROWS)

    def load(src, dst, index):
        return pltpu.make_async_copy(src, dst, w_sem.at[index])

    def load_x(b):
        return pltpu.make_async_copy(x_hbm.at[rows_of(b), :], x_v.at[rows_of(b), :], x_sem.at[b])

    def load_first(n):
        rows = pl.ds(n * 64, 64)
        return pltpu.make_async_copy(x_hbm.at[rows, :], x_v.at[rows, :], x_sem.at[0 if n == 0 else BLOCKS - 1 + n])

    kv_cols = pl.ds(pl.multiple_of(me * HEAD_DIM, HEAD_DIM), HEAD_DIM)
    early, late = pl.ds(0, ROWS), pl.ds(ROWS, TOKENS - ROWS)
    load_g = load(g_hbm, g_v, 0)
    load_qkv = [
        load(wk_hbm.at[:, kv_cols], wqkv_v.at[:, pl.ds(QCOLS, HEAD_DIM)], 1),
        load(wv_hbm.at[:, kv_cols], wqkv_v.at[:, pl.ds(QCOLS + HEAD_DIM, HEAD_DIM)], 1),
        load(wq_hbm, wqkv_v.at[:, pl.ds(0, QCOLS)], 1),
    ]
    wait_qkv = load(wqkv_v, wqkv_v, 1)
    load_early = load(tab_hbm.at[early, :], tab_v.at[early, :], 2)
    load_gu, wait_gu = [], []
    for n in range(FFCOLS // 256):
        tile = pl.ds(n * 256, 256)
        load_gu.append((load(wg_hbm.at[:, tile], wg_v.at[:, tile], 3 + n), load(wu_hbm.at[:, tile], wu_v.at[:, tile], 3 + n)))
        both = wg_v.at[:, pl.ds(0, 512)]
        wait_gu.append(load(both, both, 3 + n))
    load_od, wait_od = [], []
    for n, half in enumerate((1 - core, core)):
        cols = pl.ds(pl.multiple_of(half * 1024, 1024), 1024)
        load_od.append((load(wo_hbm.at[:, cols], wod_v.at[pl.ds(0, QCOLS), cols], 6 + n),
                        load(wd_hbm.at[:, cols], wod_v.at[pl.ds(QCOLS, FFCOLS), cols], 6 + n)))
        wait_od.append(load(wod_v.at[:, cols], wod_v.at[:, cols], 6 + n))
    load_tab = load(tab_hbm.at[late, :], tab_v.at[late, :], 8)

    load_g.start()
    for n in range(4):
        load_first(n).start()
    for copy in load_qkv:
        copy.start()
    load_early.start()

    barrier = pltpu.get_barrier_semaphore()
    for peer in (sibling, xpeer, ypeer):
        pl.semaphore_signal(barrier, inc=1, device_id={'tp': peer}, device_id_type=MESH)

    def remote(kind, src, dst, recv, peer):
        return pltpu.make_async_remote_copy(src_ref=src, dst_ref=dst, send_sem=ssem.at[kind], recv_sem=recv,
                                            device_id={'tp': peer}, device_id_type=MESH)

    mine = core * 4 + p1 * 2
    other = core * 4 + (1 - p1) * 2

    def half_rows(u):
        return pl.ds(pl.multiple_of(u * HALF, HALF), HALF)

    def y_part(u, piece, count):
        return y_v.at[half_rows(u), pl.ds(pl.multiple_of(piece * 256, 256), count * 256)]

    def pair_copy(kind, b):
        units = pl.ds(2 * b, 2)
        return remote(kind, d2d_src.at[kind, units], d2d_dst.at[kind, units], pair_sem.at[kind, b], sibling)

    def copy_of(kind, u):
        if kind == RED_ONE:
            return remote(kind, h_send.at[u], r1_dst.at[u], link_sem.at[0, u], n1)
        if kind == RED_TWO:
            return remote(kind, p_send.at[u], r2_dst.at[u], link_sem.at[1, u], n2)
        if kind == GAT_ONE:
            part = y_part(u, mine + p2, 1)
            return remote(kind, part, part, link_sem.at[2, u], n2)
        if kind == GAT_TWO:
            part = y_part(u, mine, 2)
            return remote(kind, part, part, link_sem.at[3, u], n1)
        part = y_part(u, mine if kind == OUT_FIRST else other, 2)
        return remote(kind, part, part, out_sem.at[kind - OUT_FIRST], sibling)

    def all_of(kind):
        src, dst = (p_send, r2_dst) if kind in (RED_TWO, GAT_ONE) else (h_send, r1_dst)
        return remote(kind, src, dst, out_sem.at[1 if kind == OUT_SECOND else 0], sibling)

    def norm_rows(b, r):
        x_f = x_v[pl.ds(pl.multiple_of(b * ROWS + r * 16, 16), 16), :].astype(F32)
        inv = lax.rsqrt(jnp.mean(x_f * x_f, axis=-1, keepdims=True) + NORM_EPS)
        gain = jnp.concatenate([gf_v[...], gf_v[...]], axis=0)
        a_v[b % 2, pl.ds(r * 16, 16), :] = (x_f * inv * gain).astype(BF16)

    def project(b):
        @pl.when(b == 0)
        def _():
            load_g.wait()
            gf_v[...] = jnp.broadcast_to(g_v[...].astype(F32)[None, :], (8, WIDTH))
            for n in range(4):
                load_first(n).wait()
                if n < 3:
                    for copy in load_gu[n]:
                        copy.start()
                for r in range(n * 4, n * 4 + 4):
                    norm_rows(0, r)
            wait_qkv.wait()
            load_early.wait()
            pl.semaphore_wait(barrier, 3)

        @pl.when(b == 1)
        def _():
            load_tab.wait()

        tab = tab_v[rows_of(b), :]
        swapped = pltpu.roll(tab, HEAD_DIM // 2, 1)
        low = lax.broadcasted_iota(jnp.int32, tab.shape, 1) < HEAD_DIM // 2
        cos = jnp.where(low, tab, swapped)
        sin = jnp.where(low, -swapped, tab)
        qkv = jnp.dot(a_v[lax.rem(b, 2)], wqkv_v[...], preferred_element_type=F32)

        def rope(h):
            return (h * cos + pltpu.roll(h, HEAD_DIM // 2, 1) * sin).astype(BF16)

        q_v[pl.ds(0, ROWS), :] = rope(qkv[:, 0:128])
        q_v[pl.ds(ROWS, ROWS), :] = rope(qkv[:, 128:256])
        k_v[rows_of(b), :] = rope(qkv[:, 256:384])
        v_v[rows_of(b), :] = qkv[:, 384:512].astype(BF16)

    def attention(b):
        def tile(j):
            return pl.ds(j * ROWS, ROWS)

        heads = range(2)
        peak, total, shift = [None] * 2, [None] * 2, [None] * 2
        for j in range(b + 1):
            for h in heads:
                q = q_v[pl.ds(h * ROWS, ROWS), :]
                s = lax.dot_general(q, k_v[tile(j), :], (((1,), (1,)), ((), ())), preferred_element_type=F32) * SCORE_SCALE
                if j == b:
                    qpos = lax.broadcasted_iota(jnp.int32, (ROWS, ROWS), 0)
                    kpos = lax.broadcasted_iota(jnp.int32, (ROWS, ROWS), 1)
                    s = jnp.where(kpos <= qpos, s, -1e30)
                s_v[h, :, tile(j)] = s
                pair = jnp.maximum(s[:, :128], s[:, 128:])
                peak[h] = pair if j == 0 else jnp.maximum(peak[h], pair)
                yield
        for h in heads:
            peak[h] = jnp.max(peak[h], axis=1, keepdims=True)
        for j in range(b + 1):
            for h in heads:
                e = jnp.exp2(s_v[h, :, tile(j)] - peak[h])
                pair = e[:, :128] + e[:, 128:]
                total[h] = pair if j == 0 else total[h] + pair
                yield
        for h in heads:
            shift[h] = peak[h] + jnp.log2(jnp.sum(total[h], axis=1, keepdims=True))
        for j in range(b + 1):
            for h in heads:
                p_v[h, :, tile(j)] = jnp.exp2(s_v[h, :, tile(j)] - shift[h]).astype(BF16)
                yield
        keys = pl.ds(0, (b + 1) * ROWS)
        for h in heads:
            o = jnp.dot(p_v[h, :, keys], v_v[keys, :], preferred_element_type=F32)
            om_v[:, pl.ds(h * HEAD_DIM, HEAD_DIM)] = o.astype(BF16)
            yield

    def gate_up(b):
        normed = a_v.at[b % 2]
        for n in range(FFCOLS // 256):
            if b == 0:
                wait_gu[n].wait()
                if n == 2:
                    load_x(1).start()
                    for copy in load_od[1]:
                        copy.start()
            cols = pl.ds(n * 256, 256)
            gate = jnp.dot(normed[...], wg_v[:, cols], preferred_element_type=F32)
            yield
            up = jnp.dot(normed[...], wu_v[:, cols], preferred_element_type=F32)
            om_v[:, pl.ds(QCOLS + n * 256, 256)] = (gate * (1.0 / (1.0 + jnp.exp(-gate))) * up).astype(BF16)
            yield

    def next_norm(b):
        for r in range(ROWS // 16):
            norm_rows(b + 1, r)
            yield

    def mix_block(b):
        works = [(gate_up(b), [k / 6 for k in range(6)])]
        count = 6 * (b + 1) + 2
        works.append((attention(b), [k / count for k in range(count)]))
        if b == 0:
            for copy in load_od[0]:
                copy.start()
        elif b < BLOCKS - 1:
            count = ROWS // 16
            load_x(b + 1).wait()
            works.append((next_norm(b), [k / count for k in range(count)]))
        turns = sorted((turn, index) for index, (_, turns) in enumerate(works) for turn in turns)
        for _, index in turns:
            next(works[index][0])
        for work, _ in works:
            for _ in work:
                pass

    def mix(i):
        for b in range(BLOCKS):
            @pl.when(i == b)
            def _():
                mix_block(b)

    def down(half, quarter):
        cols = pl.ds(pl.multiple_of(half * 1024 + quarter * 512, 512), 512)
        return jnp.dot(om_v[...], wod_v[:, cols], preferred_element_type=F32)

    def down_other(b):
        @pl.when(b == 0)
        def _():
            wait_od[0].wait()
            load_tab.start()
            for n in range(2, BLOCKS):
                load_x(n).start()

        for kind, quarter in ((D2D_FIRST, 1 - p2), (D2D_SECOND, p2)):
            part = down(1 - core, quarter).astype(BF16)
            for s in range(2):
                d2d_src[kind, 2 * b + s] = part[s * HALF:(s + 1) * HALF]
            pair_copy(kind, b).start()

    def down_mine(b):
        @pl.when(b == 0)
        def _():
            wait_od[1].wait()

        part = down(core, 1 - p1)
        with jax.named_scope("recv"):
            pair_copy(D2D_FIRST, b).wait_recv()
        for s in range(2):
            u = 2 * b + s
            h_send[u] = (part[s * HALF:(s + 1) * HALF] + d2d_dst[0, u].astype(F32)).astype(BF16)
            copy_of(RED_ONE, u).start()

        def keep_part(after):
            part = down(core, p1)
            for r in range(ROWS // 16) if after else ():
                norm_rows(1, r)
            with jax.named_scope("recv"):
                pair_copy(D2D_SECOND, b).wait_recv()
            for s in range(2):
                u = 2 * b + s
                h_keep[u] = part[s * HALF:(s + 1) * HALF] + d2d_dst[1, u].astype(F32)

        @pl.when(b == 0)
        def _():
            load_x(1).wait()
            keep_part(True)

        @pl.when(b > 0)
        def _():
            keep_part(False)

    def stage_b(u):
        with jax.named_scope("recv"):
            copy_of(RED_ONE, u).wait_recv()
        send = pl.ds(pl.multiple_of((1 - p2) * 256, 256), 256)
        keep = pl.ds(pl.multiple_of(p2 * 256, 256), 256)
        p_send[u] = (h_keep[u, :, send] + r1_dst[u, :, send].astype(F32)).astype(BF16)
        copy_of(RED_TWO, u).start()
        p_keep[u] = h_keep[u, :, keep] + r1_dst[u, :, keep].astype(F32)

    def stage_c(u):
        with jax.named_scope("recv"):
            copy_of(RED_TWO, u).wait_recv()
        cols = pl.ds(pl.multiple_of((mine + p2) * 256, 256), 256)
        x_f = x_v[half_rows(u), cols].astype(F32)
        y_v[half_rows(u), cols] = (x_f + (p_keep[u] + r2_dst[u].astype(F32))).astype(BF16)
        copy_of(GAT_ONE, u).start()

    def stage_d(u):
        with jax.named_scope("recv"):
            copy_of(GAT_ONE, u).wait_recv()
        copy_of(GAT_TWO, u).start()
        copy_of(OUT_FIRST, u).start()

    def stage_e(u):
        with jax.named_scope("recv"):
            copy_of(GAT_TWO, u).wait_recv()
        copy_of(OUT_SECOND, u).start()

    stages = {"b": stage_b, "c": stage_c, "d": stage_d, "e": stage_e}

    slots = {}
    for name in "bcde":
        for u in range(UNITS):
            slots.setdefault(STAGE_SLOTS[name][u], []).append((name, u))

    def communicate(slot):
        for name, u in slots.get(slot, ()):
            with jax.named_scope("stage_" + name):
                stages[name](u)

    def step(i, carry):
        for point, part in enumerate((project, None, mix, down_other, down_mine)):
            if part is not None:
                with jax.named_scope(part.__name__):
                    part(i)
            for b in range(BLOCKS):
                if 5 * b + point in slots:
                    @pl.when(i == b)
                    def _():
                        communicate(5 * b + point)

        return carry

    lax.fori_loop(0, BLOCKS, step, 0)
    for slot in range(5 * BLOCKS, max(slots) + 1):
        communicate(slot)

    with jax.named_scope("finish"):
        for kind in (OUT_FIRST, OUT_SECOND):
            all_of(kind).wait_recv()
        for kind in range(8):
            all_of(kind).wait_send()


def store_kernel(y_v, k_v, v_v, y_out, k_out, v_out, sem):
    copies = [pltpu.make_async_copy(k_v, k_out, sem.at[0]), pltpu.make_async_copy(v_v, v_out, sem.at[1])]
    for b in range(BLOCKS):
        rows = pl.ds(b * ROWS, ROWS)
        copies.append(pltpu.make_async_copy(y_v.at[rows, :], y_out.at[rows, :], sem.at[2 + b]))
    for copy in copies:
        copy.start()
    for copy in copies:
        copy.wait()


def solution(mesh):
    table = rope_table()

    def local_layer(x_in, g_norm, w_q, w_k, w_v, w_o, w_gate, w_up, w_down):
        any_spec = pl.BlockSpec(memory_space=pl.ANY)
        y, k, v = pl.pallas_call(
            layer_kernel,
            out_shape=(pltpu.VMEM((TOKENS, WIDTH), BF16), pltpu.VMEM((TOKENS, HEAD_DIM), BF16), pltpu.VMEM((TOKENS, HEAD_DIM), BF16)),
            in_specs=[any_spec] * 10,
            out_specs=(pl.BlockSpec(memory_space=pltpu.VMEM),) * 3,
            scratch_shapes=[
                pltpu.VMEM((TOKENS, WIDTH), BF16),
                pltpu.VMEM((WIDTH,), BF16),
                pltpu.VMEM((8, WIDTH), F32),
                pltpu.VMEM((WIDTH, QCOLS + 2 * HEAD_DIM), BF16),
                pltpu.VMEM((WIDTH, FFCOLS), BF16),
                pltpu.VMEM((WIDTH, FFCOLS), BF16),
                pltpu.VMEM((KDOWN, WIDTH), BF16),
                pltpu.VMEM((TOKENS, HEAD_DIM), F32),
                pltpu.VMEM((2, ROWS, WIDTH), BF16),
                pltpu.VMEM((2 * ROWS, HEAD_DIM), BF16),
                pltpu.VMEM((2, ROWS, TOKENS), F32),
                pltpu.VMEM((2, ROWS, TOKENS), BF16),
                pltpu.VMEM((ROWS, KDOWN), BF16),
                pltpu.VMEM((2, UNITS, HALF, 512), BF16),
                pltpu.VMEM((2, UNITS, HALF, 512), BF16),
                pltpu.VMEM((UNITS, HALF, 512), BF16),
                pltpu.VMEM((UNITS, HALF, 512), F32),
                pltpu.VMEM((UNITS, HALF, 512), BF16),
                pltpu.VMEM((UNITS, HALF, 256), BF16),
                pltpu.VMEM((UNITS, HALF, 256), F32),
                pltpu.VMEM((UNITS, HALF, 256), BF16),
                pltpu.SemaphoreType.DMA((BLOCKS + 3,)),
                pltpu.SemaphoreType.DMA((9,)),
                pltpu.SemaphoreType.DMA((8,)),
                pltpu.SemaphoreType.DMA((2, BLOCKS)),
                pltpu.SemaphoreType.DMA((4, UNITS)),
                pltpu.SemaphoreType.DMA((2,)),
            ],
            compiler_params=pltpu.CompilerParams(collective_id=0, has_side_effects=True, vmem_limit_bytes=67043328 - 8 * 1024 * 1024),
        )(x_in, g_norm, w_q, w_k, w_v, w_o, w_gate, w_up, w_down, jnp.asarray(table))
        y, k, v = pl.pallas_call(
            store_kernel,
            out_shape=(jax.ShapeDtypeStruct((TOKENS, WIDTH), BF16), jax.ShapeDtypeStruct((TOKENS, HEAD_DIM), BF16),
                       jax.ShapeDtypeStruct((TOKENS, HEAD_DIM), BF16)),
            in_specs=[any_spec] * 3,
            out_specs=(any_spec,) * 3,
            scratch_shapes=[pltpu.SemaphoreType.DMA((2 + BLOCKS,))],
            compiler_params=pltpu.CompilerParams(vmem_limit_bytes=1024 * 1024),
        )(*(pltpu.with_memory_space_constraint(part, pltpu.VMEM) for part in (y, k, v)))
        return y, k.reshape(TOKENS, 1, HEAD_DIM), v.reshape(TOKENS, 1, HEAD_DIM)

    return jax.shard_map(local_layer, mesh=mesh, in_specs=(P('dp', None), P(None), P(None, 'tp'), P(None, None), P(None, None), P('tp', None), P(None, 'tp'), P(None, 'tp'), P('tp', None)), out_specs=(P('dp', None), P('dp', 'tp', None), P('dp', 'tp', None)), check_vma=False)
```

```python
import math
import numpy as np
import jax
import jax.numpy as jnp
from jax import lax
from jax.experimental import pallas as pl
from jax.experimental.pallas import tpu as pltpu
from jax.sharding import PartitionSpec as P

HEAD_DIM = 128
ROPE_BASE = 500000.0
NORM_EPS = 1e-5
TOKENS = 1536
WIDTH = 2048
QCOLS = 256
FFCOLS = 768
ROWS = 256
BLOCKS = TOKENS // ROWS
KDOWN = QCOLS + FFCOLS
HALF = ROWS // 2
UNITS = TOKENS // HALF
STAGE_SLOTS = {
    "b": (3, 5, 6, 8, 9, 12, 12, 15, 24, 27, 32, 32),
    "c": (5, 6, 8, 9, 12, 19, 23, 27, 31, 47, 56, 57),
    "d": (6, 8, 11, 13, 22, 24, 36, 41, 74, 85, 90, 106),
    "e": (25, 54, 57, 62, 64, 67, 78, 110, 132, 144, 147, 164),
}
SCORE_SCALE = math.log2(math.e) / math.sqrt(HEAD_DIM)
F32 = jnp.float32
BF16 = jnp.bfloat16
MESH = pl.DeviceIdType.MESH

D2D_FIRST, D2D_SECOND, RED_ONE, RED_TWO, GAT_ONE, GAT_TWO, OUT_FIRST, OUT_SECOND = range(8)


def rope_table():
    inv_freq = np.float32(ROPE_BASE) ** (-np.arange(0, HEAD_DIM, 2, dtype=np.float32) / np.float32(HEAD_DIM))
    angles = np.arange(TOKENS, dtype=np.float32)[:, None] * inv_freq.astype(np.float32)[None, :]
    angles = angles.astype(np.float64)
    return np.concatenate([np.cos(angles), np.sin(angles)], axis=1).astype(np.float32)


def layer_kernel(x_hbm, g_hbm, wq_hbm, wk_hbm, wv_hbm, wo_hbm, wg_hbm, wu_hbm, wd_hbm, tab_hbm,
                 y_v, k_v, v_v,
                 x_v, g_v, gf_v, wqkv_v, wg_v, wu_v, wod_v, tab_v,
                 a_v, q_v, s_v, p_v, om_v,
                 d2d_src, d2d_dst, h_send, h_keep, r1_dst, p_send, p_keep, r2_dst,
                 x_sem, w_sem, ssem, pair_sem, link_sem, out_sem):
    me = lax.axis_index('tp')
    core = lax.rem(me, 2)
    xpos = lax.rem(me // 2, 2)
    ypos = me // 4
    sibling = me + 1 - 2 * core
    xpeer = me + 2 - 4 * xpos
    ypeer = me + 4 - 8 * ypos
    p1 = xpos + core * (ypos - xpos)
    p2 = ypos + core * (xpos - ypos)
    n1 = xpeer + core * (ypeer - xpeer)
    n2 = ypeer + core * (xpeer - ypeer)

    def rows_of(b):
        return pl.ds(pl.multiple_of(b * ROWS, ROWS), ROWS)

    def load(src, dst, index):
        return pltpu.make_async_copy(src, dst, w_sem.at[index])

    def load_x(b):
        return pltpu.make_async_copy(x_hbm.at[rows_of(b), :], x_v.at[rows_of(b), :], x_sem.at[b])

    def load_first(n):
        rows = pl.ds(n * 64, 64)
        return pltpu.make_async_copy(x_hbm.at[rows, :], x_v.at[rows, :], x_sem.at[0 if n == 0 else BLOCKS - 1 + n])

    kv_cols = pl.ds(pl.multiple_of(me * HEAD_DIM, HEAD_DIM), HEAD_DIM)
    early, late = pl.ds(0, ROWS), pl.ds(ROWS, TOKENS - ROWS)
    load_g = load(g_hbm, g_v, 0)
    load_qkv = [
        load(wk_hbm.at[:, kv_cols], wqkv_v.at[:, pl.ds(QCOLS, HEAD_DIM)], 1),
        load(wv_hbm.at[:, kv_cols], wqkv_v.at[:, pl.ds(QCOLS + HEAD_DIM, HEAD_DIM)], 1),
        load(wq_hbm, wqkv_v.at[:, pl.ds(0, QCOLS)], 1),
    ]
    wait_qkv = load(wqkv_v, wqkv_v, 1)
    load_early = load(tab_hbm.at[early, :], tab_v.at[early, :], 2)
    load_gu, wait_gu = [], []
    for n in range(FFCOLS // 256):
        tile = pl.ds(n * 256, 256)
        load_gu.append((load(wg_hbm.at[:, tile], wg_v.at[:, tile], 3 + n), load(wu_hbm.at[:, tile], wu_v.at[:, tile], 3 + n)))
        both = wg_v.at[:, pl.ds(0, 512)]
        wait_gu.append(load(both, both, 3 + n))
    load_od, wait_od = [], []
    for n, half in enumerate((1 - core, core)):
        cols = pl.ds(pl.multiple_of(half * 1024, 1024), 1024)
        load_od.append((load(wo_hbm.at[:, cols], wod_v.at[pl.ds(0, QCOLS), cols], 6 + n),
                        load(wd_hbm.at[:, cols], wod_v.at[pl.ds(QCOLS, FFCOLS), cols], 6 + n)))
        wait_od.append(load(wod_v.at[:, cols], wod_v.at[:, cols], 6 + n))
    load_tab = load(tab_hbm.at[late, :], tab_v.at[late, :], 8)

    load_g.start()
    for n in range(4):
        load_first(n).start()
    for copy in load_qkv:
        copy.start()
    load_early.start()

    barrier = pltpu.get_barrier_semaphore()
    for peer in (sibling, xpeer, ypeer):
        pl.semaphore_signal(barrier, inc=1, device_id={'tp': peer}, device_id_type=MESH)

    def remote(kind, src, dst, recv, peer):
        return pltpu.make_async_remote_copy(src_ref=src, dst_ref=dst, send_sem=ssem.at[kind], recv_sem=recv,
                                            device_id={'tp': peer}, device_id_type=MESH)

    mine = core * 4 + p1 * 2
    other = core * 4 + (1 - p1) * 2

    def half_rows(u):
        return pl.ds(pl.multiple_of(u * HALF, HALF), HALF)

    def y_part(u, piece, count):
        return y_v.at[half_rows(u), pl.ds(pl.multiple_of(piece * 256, 256), count * 256)]

    def pair_copy(kind, b):
        units = pl.ds(2 * b, 2)
        return remote(kind, d2d_src.at[kind, units], d2d_dst.at[kind, units], pair_sem.at[kind, b], sibling)

    def copy_of(kind, u):
        if kind == RED_ONE:
            return remote(kind, h_send.at[u], r1_dst.at[u], link_sem.at[0, u], n1)
        if kind == RED_TWO:
            return remote(kind, p_send.at[u], r2_dst.at[u], link_sem.at[1, u], n2)
        if kind == GAT_ONE:
            part = y_part(u, mine + p2, 1)
            return remote(kind, part, part, link_sem.at[2, u], n2)
        if kind == GAT_TWO:
            part = y_part(u, mine, 2)
            return remote(kind, part, part, link_sem.at[3, u], n1)
        part = y_part(u, mine if kind == OUT_FIRST else other, 2)
        return remote(kind, part, part, out_sem.at[kind - OUT_FIRST], sibling)

    def all_of(kind):
        src, dst = (p_send, r2_dst) if kind in (RED_TWO, GAT_ONE) else (h_send, r1_dst)
        return remote(kind, src, dst, out_sem.at[1 if kind == OUT_SECOND else 0], sibling)

    def norm_rows(b, r):
        x_f = x_v[pl.ds(pl.multiple_of(b * ROWS + r * 16, 16), 16), :].astype(F32)
        inv = lax.rsqrt(jnp.mean(x_f * x_f, axis=-1, keepdims=True) + NORM_EPS)
        gain = jnp.concatenate([gf_v[...], gf_v[...]], axis=0)
        a_v[b % 2, pl.ds(r * 16, 16), :] = (x_f * inv * gain).astype(BF16)

    def first_norm():
        load_g.wait()
        gf_v[...] = jnp.broadcast_to(g_v[...].astype(F32)[None, :], (8, WIDTH))
        for n in range(4):
            load_first(n).wait()
            if n < 3:
                for copy in load_gu[n]:
                    copy.start()
            for r in range(n * 4, n * 4 + 4):
                norm_rows(0, r)
        wait_qkv.wait()
        load_early.wait()
        pl.semaphore_wait(barrier, 3)

    def project(b):
        @pl.when(b == 1)
        def _():
            load_tab.wait()

        tab = tab_v[rows_of(b), :]
        swapped = pltpu.roll(tab, HEAD_DIM // 2, 1)
        low = lax.broadcasted_iota(jnp.int32, tab.shape, 1) < HEAD_DIM // 2
        cos = jnp.where(low, tab, swapped)
        sin = jnp.where(low, -swapped, tab)
        qkv = jnp.dot(a_v[lax.rem(b, 2)], wqkv_v[...], preferred_element_type=F32)

        def rope(h):
            return (h * cos + pltpu.roll(h, HEAD_DIM // 2, 1) * sin).astype(BF16)

        q_v[pl.ds(0, ROWS), :] = rope(qkv[:, 0:128])
        q_v[pl.ds(ROWS, ROWS), :] = rope(qkv[:, 128:256])
        k_v[rows_of(b), :] = rope(qkv[:, 256:384])
        v_v[rows_of(b), :] = qkv[:, 384:512].astype(BF16)

    def attention(b):
        def tile(j):
            return pl.ds(j * ROWS, ROWS)

        heads = range(2)
        peak, total, shift = [None] * 2, [None] * 2, [None] * 2
        for j in range(b + 1):
            for h in heads:
                q = q_v[pl.ds(h * ROWS, ROWS), :]
                s = lax.dot_general(q, k_v[tile(j), :], (((1,), (1,)), ((), ())), preferred_element_type=F32) * SCORE_SCALE
                if j == b:
                    qpos = lax.broadcasted_iota(jnp.int32, (ROWS, ROWS), 0)
                    kpos = lax.broadcasted_iota(jnp.int32, (ROWS, ROWS), 1)
                    s = jnp.where(kpos <= qpos, s, -1e30)
                s_v[h, :, tile(j)] = s
                pair = jnp.maximum(s[:, :128], s[:, 128:])
                peak[h] = pair if j == 0 else jnp.maximum(peak[h], pair)
                yield
        for h in heads:
            peak[h] = jnp.max(peak[h], axis=1, keepdims=True)
        for j in range(b + 1):
            for h in heads:
                e = jnp.exp2(s_v[h, :, tile(j)] - peak[h])
                pair = e[:, :128] + e[:, 128:]
                total[h] = pair if j == 0 else total[h] + pair
                yield
        for h in heads:
            shift[h] = peak[h] + jnp.log2(jnp.sum(total[h], axis=1, keepdims=True))
        for j in range(b + 1):
            for h in heads:
                p_v[h, :, tile(j)] = jnp.exp2(s_v[h, :, tile(j)] - shift[h]).astype(BF16)
                yield
        keys = pl.ds(0, (b + 1) * ROWS)
        for h in heads:
            o = jnp.dot(p_v[h, :, keys], v_v[keys, :], preferred_element_type=F32)
            om_v[:, pl.ds(h * HEAD_DIM, HEAD_DIM)] = o.astype(BF16)
            yield

    def gate_up(b):
        normed = a_v.at[b % 2]
        for n in range(FFCOLS // 256):
            if b == 0:
                wait_gu[n].wait()
                if n == 2:
                    load_x(1).start()
                    for copy in load_od[1]:
                        copy.start()
            cols = pl.ds(n * 256, 256)
            gate = jnp.dot(normed[...], wg_v[:, cols], preferred_element_type=F32)
            yield
            up = jnp.dot(normed[...], wu_v[:, cols], preferred_element_type=F32)
            om_v[:, pl.ds(QCOLS + n * 256, 256)] = (gate * (1.0 / (1.0 + jnp.exp(-gate))) * up).astype(BF16)
            yield

    def next_norm(b):
        for r in range(ROWS // 16):
            norm_rows(b + 1, r)
            yield

    def mix_block(b):
        works = [(gate_up(b), [k / 6 for k in range(6)])]
        count = 6 * (b + 1) + 2
        works.append((attention(b), [k / count for k in range(count)]))
        if b == 0:
            for copy in load_od[0]:
                copy.start()
        elif b < BLOCKS - 1:
            count = ROWS // 16
            load_x(b + 1).wait()
            works.append((next_norm(b), [k / count for k in range(count)]))
        turns = sorted((turn, index) for index, (_, turns) in enumerate(works) for turn in turns)
        for _, index in turns:
            next(works[index][0])
        for work, _ in works:
            for _ in work:
                pass
        if b == 0:
            wait_od[0].wait()
        pair_product(D2D_FIRST, 1 - p2, b)
        pair_copy(D2D_FIRST, b).start()

    def mix(i):
        for b in range(BLOCKS):
            @pl.when(i == b)
            def _():
                mix_block(b)

    def down(half, quarter):
        cols = pl.ds(pl.multiple_of(half * 1024 + quarter * 512, 512), 512)
        return jnp.dot(om_v[...], wod_v[:, cols], preferred_element_type=F32)

    def pair_product(kind, quarter, b):
        part = down(1 - core, quarter).astype(BF16)
        for s in range(2):
            d2d_src[kind, 2 * b + s] = part[s * HALF:(s + 1) * HALF]

    def down_rest(i):
        def rest(b, first):
            norms = iter(range(ROWS // 16) if first else ())

            def some_norms():
                for _ in range(6):
                    for r in norms:
                        norm_rows(1, r)
                        break

            pair_product(D2D_SECOND, p2, b)
            some_norms()
            send = down(core, 1 - p1)
            some_norms()
            keep = down(core, p1)
            some_norms()
            for s in range(2):
                h_keep[2 * b + s] = keep[s * HALF:(s + 1) * HALF]
            pair_copy(D2D_SECOND, b).start()
            with jax.named_scope("recv"):
                pair_copy(D2D_FIRST, b).wait_recv()
            for s in range(2):
                u = 2 * b + s
                h_send[u] = (send[s * HALF:(s + 1) * HALF] + d2d_dst[0, u].astype(F32)).astype(BF16)
                copy_of(RED_ONE, u).start()

        @pl.when(i == 0)
        def _():
            load_tab.start()
            for n in range(2, BLOCKS):
                load_x(n).start()
            wait_od[1].wait()
            load_x(1).wait()
            rest(0, True)

        @pl.when(i > 0)
        def _():
            rest(i, False)

    def stage_b(u):
        with jax.named_scope("recv"):
            copy_of(RED_ONE, u).wait_recv()
            if u % 2 == 0:
                pair_copy(D2D_SECOND, u // 2).wait_recv()
        send = pl.ds(pl.multiple_of((1 - p2) * 256, 256), 256)
        keep = pl.ds(pl.multiple_of(p2 * 256, 256), 256)

        def summed(cols):
            return h_keep[u, :, cols] + d2d_dst[1, u, :, cols].astype(F32) + r1_dst[u, :, cols].astype(F32)

        p_send[u] = summed(send).astype(BF16)
        copy_of(RED_TWO, u).start()
        p_keep[u] = summed(keep)

    def stage_c(u):
        with jax.named_scope("recv"):
            copy_of(RED_TWO, u).wait_recv()
        cols = pl.ds(pl.multiple_of((mine + p2) * 256, 256), 256)
        x_f = x_v[half_rows(u), cols].astype(F32)
        y_v[half_rows(u), cols] = (x_f + (p_keep[u] + r2_dst[u].astype(F32))).astype(BF16)
        copy_of(GAT_ONE, u).start()

    def stage_d(u):
        with jax.named_scope("recv"):
            copy_of(GAT_ONE, u).wait_recv()
        copy_of(GAT_TWO, u).start()
        copy_of(OUT_FIRST, u).start()

    def stage_e(u):
        with jax.named_scope("recv"):
            copy_of(GAT_TWO, u).wait_recv()
        copy_of(OUT_SECOND, u).start()

    stages = {"b": stage_b, "c": stage_c, "d": stage_d, "e": stage_e}

    slots = {}
    for name in "bcde":
        for u in range(UNITS):
            slots.setdefault(STAGE_SLOTS[name][u], []).append((name, u))

    def communicate(slot):
        for name, u in slots.get(slot, ()):
            with jax.named_scope("stage_" + name):
                stages[name](u)

    def next_project(i):
        @pl.when(i < BLOCKS - 1)
        def _():
            project(i + 1)

    def step(i, carry):
        for point, part in enumerate((mix, down_rest, next_project)):
            with jax.named_scope(part.__name__):
                part(i)
            for b in range(BLOCKS):
                if 3 * b + point in slots:
                    @pl.when(i == b)
                    def _():
                        communicate(3 * b + point)

        return carry

    with jax.named_scope("first"):
        first_norm()
        project(0)
    lax.fori_loop(0, BLOCKS, step, 0)
    for slot in range(3 * BLOCKS, max(slots) + 1):
        communicate(slot)

    with jax.named_scope("finish"):
        for kind in (OUT_FIRST, OUT_SECOND):
            all_of(kind).wait_recv()
        for kind in range(8):
            all_of(kind).wait_send()


def store_kernel(y_v, k_v, v_v, y_out, k_out, v_out, sem):
    copies = [pltpu.make_async_copy(k_v, k_out, sem.at[0]), pltpu.make_async_copy(v_v, v_out, sem.at[1])]
    for b in range(BLOCKS):
        rows = pl.ds(b * ROWS, ROWS)
        copies.append(pltpu.make_async_copy(y_v.at[rows, :], y_out.at[rows, :], sem.at[2 + b]))
    for copy in copies:
        copy.start()
    for copy in copies:
        copy.wait()


def solution(mesh):
    table = rope_table()

    def local_layer(x_in, g_norm, w_q, w_k, w_v, w_o, w_gate, w_up, w_down):
        any_spec = pl.BlockSpec(memory_space=pl.ANY)
        y, k, v = pl.pallas_call(
            layer_kernel,
            out_shape=(pltpu.VMEM((TOKENS, WIDTH), BF16), pltpu.VMEM((TOKENS, HEAD_DIM), BF16), pltpu.VMEM((TOKENS, HEAD_DIM), BF16)),
            in_specs=[any_spec] * 10,
            out_specs=(pl.BlockSpec(memory_space=pltpu.VMEM),) * 3,
            scratch_shapes=[
                pltpu.VMEM((TOKENS, WIDTH), BF16),
                pltpu.VMEM((WIDTH,), BF16),
                pltpu.VMEM((8, WIDTH), F32),
                pltpu.VMEM((WIDTH, QCOLS + 2 * HEAD_DIM), BF16),
                pltpu.VMEM((WIDTH, FFCOLS), BF16),
                pltpu.VMEM((WIDTH, FFCOLS), BF16),
                pltpu.VMEM((KDOWN, WIDTH), BF16),
                pltpu.VMEM((TOKENS, HEAD_DIM), F32),
                pltpu.VMEM((2, ROWS, WIDTH), BF16),
                pltpu.VMEM((2 * ROWS, HEAD_DIM), BF16),
                pltpu.VMEM((2, ROWS, TOKENS), F32),
                pltpu.VMEM((2, ROWS, TOKENS), BF16),
                pltpu.VMEM((ROWS, KDOWN), BF16),
                pltpu.VMEM((2, UNITS, HALF, 512), BF16),
                pltpu.VMEM((2, UNITS, HALF, 512), BF16),
                pltpu.VMEM((UNITS, HALF, 512), BF16),
                pltpu.VMEM((UNITS, HALF, 512), F32),
                pltpu.VMEM((UNITS, HALF, 512), BF16),
                pltpu.VMEM((UNITS, HALF, 256), BF16),
                pltpu.VMEM((UNITS, HALF, 256), F32),
                pltpu.VMEM((UNITS, HALF, 256), BF16),
                pltpu.SemaphoreType.DMA((BLOCKS + 3,)),
                pltpu.SemaphoreType.DMA((9,)),
                pltpu.SemaphoreType.DMA((8,)),
                pltpu.SemaphoreType.DMA((2, BLOCKS)),
                pltpu.SemaphoreType.DMA((4, UNITS)),
                pltpu.SemaphoreType.DMA((2,)),
            ],
            compiler_params=pltpu.CompilerParams(collective_id=0, has_side_effects=True, vmem_limit_bytes=67043328 - 8 * 1024 * 1024),
        )(x_in, g_norm, w_q, w_k, w_v, w_o, w_gate, w_up, w_down, jnp.asarray(table))
        y, k, v = pl.pallas_call(
            store_kernel,
            out_shape=(jax.ShapeDtypeStruct((TOKENS, WIDTH), BF16), jax.ShapeDtypeStruct((TOKENS, HEAD_DIM), BF16),
                       jax.ShapeDtypeStruct((TOKENS, HEAD_DIM), BF16)),
            in_specs=[any_spec] * 3,
            out_specs=(any_spec,) * 3,
            scratch_shapes=[pltpu.SemaphoreType.DMA((2 + BLOCKS,))],
            compiler_params=pltpu.CompilerParams(vmem_limit_bytes=1024 * 1024),
        )(*(pltpu.with_memory_space_constraint(part, pltpu.VMEM) for part in (y, k, v)))
        return y, k.reshape(TOKENS, 1, HEAD_DIM), v.reshape(TOKENS, 1, HEAD_DIM)

    return jax.shard_map(local_layer, mesh=mesh, in_specs=(P('dp', None), P(None), P(None, 'tp'), P(None, None), P(None, None), P('tp', None), P(None, 'tp'), P(None, 'tp'), P('tp', None)), out_specs=(P('dp', None), P('dp', 'tp', None), P('dp', 'tp', None)), check_vma=False)
```

```python
import math
import numpy as np
import jax
import jax.numpy as jnp
from jax import lax
from jax.experimental import pallas as pl
from jax.experimental.pallas import tpu as pltpu
from jax.sharding import PartitionSpec as P

HEAD_DIM = 128
ROPE_BASE = 500000.0
NORM_EPS = 1e-5
TOKENS = 1536
WIDTH = 2048
QCOLS = 256
FFCOLS = 768
ROWS = 256
BLOCKS = TOKENS // ROWS
KDOWN = QCOLS + FFCOLS
HALF = ROWS // 2
UNITS = TOKENS // HALF
STAGE_SLOTS = {
    "b": (3, 5, 6, 7, 11, 11, 15, 15, 15, 26, 29, 29),
    "c": (5, 6, 8, 11, 13, 14, 18, 28, 28, 30, 41, 56),
    "d": (6, 9, 11, 14, 17, 20, 28, 39, 51, 60, 61, 67),
    "e": (15, 35, 42, 51, 61, 73, 74, 94, 96, 110, 110, 120),
}
SCORE_SCALE = math.log2(math.e) / math.sqrt(HEAD_DIM)
F32 = jnp.float32
BF16 = jnp.bfloat16
MESH = pl.DeviceIdType.MESH

D2D_FIRST, D2D_SECOND, RED_ONE, RED_TWO, GAT_ONE, GAT_TWO, OUT_FIRST, OUT_SECOND = range(8)


def rope_table():
    inv_freq = np.float32(ROPE_BASE) ** (-np.arange(0, HEAD_DIM, 2, dtype=np.float32) / np.float32(HEAD_DIM))
    angles = np.arange(TOKENS, dtype=np.float32)[:, None] * inv_freq.astype(np.float32)[None, :]
    angles = angles.astype(np.float64)
    return np.concatenate([np.cos(angles), np.sin(angles)], axis=1).astype(np.float32)


def layer_kernel(x_hbm, g_hbm, wq_hbm, wk_hbm, wv_hbm, wo_hbm, wg_hbm, wu_hbm, wd_hbm, tab_hbm,
                 y_v, k_v, v_v,
                 x_v, g_v, gf_v, wqkv_v, wg_v, wu_v, wod_v, tab_v,
                 a_v, q_v, s_v, p_v, om_v,
                 d2d_src, d2d_dst, h_send, h_keep, r1_dst, p_send, p_keep, r2_dst,
                 x_sem, w_sem, ssem, pair_sem, link_sem, out_sem):
    me = lax.axis_index('tp')
    core = lax.rem(me, 2)
    xpos = lax.rem(me // 2, 2)
    ypos = me // 4
    sibling = me + 1 - 2 * core
    xpeer = me + 2 - 4 * xpos
    ypeer = me + 4 - 8 * ypos
    p1 = xpos + core * (ypos - xpos)
    p2 = ypos + core * (xpos - ypos)
    n1 = xpeer + core * (ypeer - xpeer)
    n2 = ypeer + core * (xpeer - ypeer)

    def rows_of(b):
        return pl.ds(pl.multiple_of(b * ROWS, ROWS), ROWS)

    def load(src, dst, index):
        return pltpu.make_async_copy(src, dst, w_sem.at[index])

    def load_x(b):
        return pltpu.make_async_copy(x_hbm.at[rows_of(b), :], x_v.at[rows_of(b), :], x_sem.at[b])

    def load_first(n):
        rows = pl.ds(n * 64, 64)
        return pltpu.make_async_copy(x_hbm.at[rows, :], x_v.at[rows, :], x_sem.at[0 if n == 0 else BLOCKS - 1 + n])

    kv_cols = pl.ds(pl.multiple_of(me * HEAD_DIM, HEAD_DIM), HEAD_DIM)
    early, late = pl.ds(0, 2 * ROWS), pl.ds(2 * ROWS, TOKENS - 2 * ROWS)
    load_g = load(g_hbm, g_v, 0)
    load_qkv = [
        load(wk_hbm.at[:, kv_cols], wqkv_v.at[:, pl.ds(QCOLS, HEAD_DIM)], 1),
        load(wv_hbm.at[:, kv_cols], wqkv_v.at[:, pl.ds(QCOLS + HEAD_DIM, HEAD_DIM)], 1),
        load(wq_hbm, wqkv_v.at[:, pl.ds(0, QCOLS)], 1),
    ]
    wait_qkv = load(wqkv_v, wqkv_v, 1)
    load_early = load(tab_hbm.at[early, :], tab_v.at[early, :], 2)
    load_gu, wait_gu = [], []
    for n in range(FFCOLS // 256):
        tile = pl.ds(n * 256, 256)
        load_gu.append((load(wg_hbm.at[:, tile], wg_v.at[:, tile], 3 + n), load(wu_hbm.at[:, tile], wu_v.at[:, tile], 3 + n)))
        both = wg_v.at[:, pl.ds(0, 512)]
        wait_gu.append(load(both, both, 3 + n))
    load_od, wait_od = [], []
    for n, half in enumerate((1 - core, core)):
        cols = pl.ds(pl.multiple_of(half * 1024, 1024), 1024)
        load_od.append((load(wo_hbm.at[:, cols], wod_v.at[pl.ds(0, QCOLS), cols], 6 + n),
                        load(wd_hbm.at[:, cols], wod_v.at[pl.ds(QCOLS, FFCOLS), cols], 6 + n)))
        wait_od.append(load(wod_v.at[:, cols], wod_v.at[:, cols], 6 + n))
    load_tab = load(tab_hbm.at[late, :], tab_v.at[late, :], 8)

    load_g.start()
    for n in range(4):
        load_first(n).start()
    for copy in load_qkv:
        copy.start()
    load_early.start()

    barrier = pltpu.get_barrier_semaphore()
    for peer in (sibling, xpeer, ypeer):
        pl.semaphore_signal(barrier, inc=1, device_id={'tp': peer}, device_id_type=MESH)

    def remote(kind, src, dst, recv, peer):
        return pltpu.make_async_remote_copy(src_ref=src, dst_ref=dst, send_sem=ssem.at[kind], recv_sem=recv,
                                            device_id={'tp': peer}, device_id_type=MESH)

    mine = core * 4 + p1 * 2
    other = core * 4 + (1 - p1) * 2

    def half_rows(u):
        return pl.ds(pl.multiple_of(u * HALF, HALF), HALF)

    def y_part(u, piece, count):
        return y_v.at[half_rows(u), pl.ds(pl.multiple_of(piece * 256, 256), count * 256)]

    def pair_copy(kind, b):
        units = pl.ds(2 * b, 2)
        return remote(kind, d2d_src.at[kind, units], d2d_dst.at[kind, units], pair_sem.at[kind, b], sibling)

    def copy_of(kind, u):
        if kind == RED_ONE:
            return remote(kind, h_send.at[u], r1_dst.at[u], link_sem.at[0, u], n1)
        if kind == RED_TWO:
            return remote(kind, p_send.at[u], r2_dst.at[u], link_sem.at[1, u], n2)
        if kind == GAT_ONE:
            part = y_part(u, mine + p2, 1)
            return remote(kind, part, part, link_sem.at[2, u], n2)
        if kind == GAT_TWO:
            part = y_part(u, mine, 2)
            return remote(kind, part, part, link_sem.at[3, u], n1)
        part = y_part(u, mine if kind == OUT_FIRST else other, 2)
        return remote(kind, part, part, out_sem.at[kind - OUT_FIRST], sibling)

    def all_of(kind):
        src, dst = (p_send, r2_dst) if kind in (RED_TWO, GAT_ONE) else (h_send, r1_dst)
        return remote(kind, src, dst, out_sem.at[1 if kind == OUT_SECOND else 0], sibling)

    def norm_rows(b, r):
        x_f = x_v[pl.ds(pl.multiple_of(b * ROWS + r * 16, 16), 16), :].astype(F32)
        inv = lax.rsqrt(jnp.mean(x_f * x_f, axis=-1, keepdims=True) + NORM_EPS)
        gain = jnp.concatenate([gf_v[...], gf_v[...]], axis=0)
        a_v[b % 2, pl.ds(r * 16, 16), :] = (x_f * inv * gain).astype(BF16)

    def first_norm():
        load_g.wait()
        gf_v[...] = jnp.broadcast_to(g_v[...].astype(F32)[None, :], (8, WIDTH))
        for n in range(4):
            load_first(n).wait()
            if n < 3:
                for copy in load_gu[n]:
                    copy.start()
            for r in range(n * 4, n * 4 + 4):
                norm_rows(0, r)
        wait_qkv.wait()
        load_early.wait()
        pl.semaphore_wait(barrier, 3)

    def project(b):
        @pl.when(b == 2)
        def _():
            load_tab.wait()

        tab = tab_v[rows_of(b), :]
        swapped = pltpu.roll(tab, HEAD_DIM // 2, 1)
        low = lax.broadcasted_iota(jnp.int32, tab.shape, 1) < HEAD_DIM // 2
        cos = jnp.where(low, tab, swapped)
        sin = jnp.where(low, -swapped, tab)
        qkv = jnp.dot(a_v[lax.rem(b, 2)], wqkv_v[...], preferred_element_type=F32)

        def rope(h):
            return (h * cos + pltpu.roll(h, HEAD_DIM // 2, 1) * sin).astype(BF16)

        q_v[pl.ds(0, ROWS), :] = rope(qkv[:, 0:128])
        q_v[pl.ds(ROWS, ROWS), :] = rope(qkv[:, 128:256])
        k_v[rows_of(b), :] = rope(qkv[:, 256:384])
        v_v[rows_of(b), :] = qkv[:, 384:512].astype(BF16)

    def attention(b):
        def tile(j):
            return pl.ds(j * ROWS, ROWS)

        heads = range(2)
        peak, total, shift = [None] * 2, [None] * 2, [None] * 2
        for j in range(b + 1):
            for h in heads:
                q = q_v[pl.ds(h * ROWS, ROWS), :]
                s = lax.dot_general(q, k_v[tile(j), :], (((1,), (1,)), ((), ())), preferred_element_type=F32) * SCORE_SCALE
                if j == b:
                    qpos = lax.broadcasted_iota(jnp.int32, (ROWS, ROWS), 0)
                    kpos = lax.broadcasted_iota(jnp.int32, (ROWS, ROWS), 1)
                    s = jnp.where(kpos <= qpos, s, -1e30)
                s_v[h, :, tile(j)] = s
                pair = jnp.maximum(s[:, :128], s[:, 128:])
                peak[h] = pair if j == 0 else jnp.maximum(peak[h], pair)
                yield
        for h in heads:
            peak[h] = jnp.max(peak[h], axis=1, keepdims=True)
        for j in range(b + 1):
            for h in heads:
                e = jnp.exp2(s_v[h, :, tile(j)] - peak[h])
                pair = e[:, :128] + e[:, 128:]
                total[h] = pair if j == 0 else total[h] + pair
                yield
        for h in heads:
            shift[h] = peak[h] + jnp.log2(jnp.sum(total[h], axis=1, keepdims=True))
        for j in range(b + 1):
            for h in heads:
                p_v[h, :, tile(j)] = jnp.exp2(s_v[h, :, tile(j)] - shift[h]).astype(BF16)
                yield
        keys = pl.ds(0, (b + 1) * ROWS)
        for h in heads:
            o = jnp.dot(p_v[h, :, keys], v_v[keys, :], preferred_element_type=F32)
            om_v[:, pl.ds(h * HEAD_DIM, HEAD_DIM)] = o.astype(BF16)
            yield

    def gate_up(b):
        normed = a_v.at[b % 2]
        for n in range(FFCOLS // 256):
            if b == 0:
                wait_gu[n].wait()
            cols = pl.ds(n * 256, 256)
            gate = jnp.dot(normed[...], wg_v[:, cols], preferred_element_type=F32)
            yield
            up = jnp.dot(normed[...], wu_v[:, cols], preferred_element_type=F32)
            om_v[:, pl.ds(QCOLS + n * 256, 256)] = (gate * (1.0 / (1.0 + jnp.exp(-gate))) * up).astype(BF16)
            yield

    def next_norm(b):
        for r in range(ROWS // 16):
            norm_rows(b + 1, r)
            yield

    def mix_block(b):
        works = [(gate_up(b), [k / 6 for k in range(6)])]
        count = 6 * (b + 1) + 2
        works.append((attention(b), [k / count for k in range(count)]))
        if b == 0:
            for copy in load_od[0]:
                copy.start()
            load_x(1).start()
            for copy in load_od[1]:
                copy.start()
        elif b < BLOCKS - 1:
            count = ROWS // 16
            load_x(b + 1).wait()
            works.append((next_norm(b), [k / count for k in range(count)]))
        turns = sorted((turn, index) for index, (_, turns) in enumerate(works) for turn in turns)
        for _, index in turns:
            next(works[index][0])
        for work, _ in works:
            for _ in work:
                pass
        if b == 0:
            wait_od[0].wait()
        pair_product(D2D_FIRST, 1 - p2, b)
        pair_copy(D2D_FIRST, b).start()

    def mix(i):
        for b in range(BLOCKS):
            @pl.when(i == b)
            def _():
                mix_block(b)

    def down(half, quarter):
        cols = pl.ds(pl.multiple_of(half * 1024 + quarter * 512, 512), 512)
        return jnp.dot(om_v[...], wod_v[:, cols], preferred_element_type=F32)

    def pair_product(kind, quarter, b):
        part = down(1 - core, quarter).astype(BF16)
        for s in range(2):
            d2d_src[kind, 2 * b + s] = part[s * HALF:(s + 1) * HALF]

    def down_rest(i):
        def rest(b, first):
            norms = iter(range(ROWS // 16) if first else ())

            def some_norms():
                for _ in range(6):
                    for r in norms:
                        norm_rows(1, r)
                        break

            pair_product(D2D_SECOND, p2, b)
            some_norms()
            send = down(core, 1 - p1)
            some_norms()
            keep = down(core, p1)
            some_norms()
            for s in range(2):
                h_keep[2 * b + s] = keep[s * HALF:(s + 1) * HALF]
            pair_copy(D2D_SECOND, b).start()
            with jax.named_scope("recv"):
                pair_copy(D2D_FIRST, b).wait_recv()
            for s in range(2):
                u = 2 * b + s
                h_send[u] = (send[s * HALF:(s + 1) * HALF] + d2d_dst[0, u].astype(F32)).astype(BF16)
                copy_of(RED_ONE, u).start()

        @pl.when(i == 0)
        def _():
            wait_od[1].wait()
            load_x(1).wait()
            rest(0, True)
            load_tab.start()
            for n in range(2, BLOCKS):
                load_x(n).start()

        @pl.when(i > 0)
        def _():
            rest(i, False)

    def stage_b(u):
        with jax.named_scope("recv"):
            copy_of(RED_ONE, u).wait_recv()
            if u % 2 == 0:
                pair_copy(D2D_SECOND, u // 2).wait_recv()
        send = pl.ds(pl.multiple_of((1 - p2) * 256, 256), 256)
        keep = pl.ds(pl.multiple_of(p2 * 256, 256), 256)

        def summed(cols):
            return h_keep[u, :, cols] + d2d_dst[1, u, :, cols].astype(F32) + r1_dst[u, :, cols].astype(F32)

        p_send[u] = summed(send).astype(BF16)
        copy_of(RED_TWO, u).start()
        p_keep[u] = summed(keep)

    def stage_c(u):
        with jax.named_scope("recv"):
            copy_of(RED_TWO, u).wait_recv()
        cols = pl.ds(pl.multiple_of((mine + p2) * 256, 256), 256)
        x_f = x_v[half_rows(u), cols].astype(F32)
        y_v[half_rows(u), cols] = (x_f + (p_keep[u] + r2_dst[u].astype(F32))).astype(BF16)
        copy_of(GAT_ONE, u).start()

    def stage_d(u):
        with jax.named_scope("recv"):
            copy_of(GAT_ONE, u).wait_recv()
        copy_of(GAT_TWO, u).start()
        copy_of(OUT_FIRST, u).start()

    def stage_e(u):
        with jax.named_scope("recv"):
            copy_of(GAT_TWO, u).wait_recv()
        copy_of(OUT_SECOND, u).start()

    stages = {"b": stage_b, "c": stage_c, "d": stage_d, "e": stage_e}

    slots = {}
    for name in "bcde":
        for u in range(UNITS):
            slots.setdefault(STAGE_SLOTS[name][u], []).append((name, u))

    def communicate(slot):
        for name, u in slots.get(slot, ()):
            with jax.named_scope("stage_" + name):
                stages[name](u)

    def next_project(i):
        @pl.when(i < BLOCKS - 1)
        def _():
            project(i + 1)

    def step(i, carry):
        for point, part in enumerate((mix, down_rest, next_project)):
            with jax.named_scope(part.__name__):
                part(i)
            for b in range(BLOCKS):
                if 3 * b + point in slots:
                    @pl.when(i == b)
                    def _():
                        communicate(3 * b + point)

        return carry

    with jax.named_scope("first"):
        first_norm()
        project(0)
    lax.fori_loop(0, BLOCKS, step, 0)
    for slot in range(3 * BLOCKS, max(slots) + 1):
        communicate(slot)

    with jax.named_scope("finish"):
        for kind in (OUT_FIRST, OUT_SECOND):
            all_of(kind).wait_recv()
        for kind in range(8):
            all_of(kind).wait_send()


def store_kernel(y_v, k_v, v_v, y_out, k_out, v_out, sem):
    copies = [pltpu.make_async_copy(k_v, k_out, sem.at[0]), pltpu.make_async_copy(v_v, v_out, sem.at[1])]
    for b in range(BLOCKS):
        rows = pl.ds(b * ROWS, ROWS)
        copies.append(pltpu.make_async_copy(y_v.at[rows, :], y_out.at[rows, :], sem.at[2 + b]))
    for copy in copies:
        copy.start()
    for copy in copies:
        copy.wait()


def solution(mesh):
    table = rope_table()

    def local_layer(x_in, g_norm, w_q, w_k, w_v, w_o, w_gate, w_up, w_down):
        any_spec = pl.BlockSpec(memory_space=pl.ANY)
        y, k, v = pl.pallas_call(
            layer_kernel,
            out_shape=(pltpu.VMEM((TOKENS, WIDTH), BF16), pltpu.VMEM((TOKENS, HEAD_DIM), BF16), pltpu.VMEM((TOKENS, HEAD_DIM), BF16)),
            in_specs=[any_spec] * 10,
            out_specs=(pl.BlockSpec(memory_space=pltpu.VMEM),) * 3,
            scratch_shapes=[
                pltpu.VMEM((TOKENS, WIDTH), BF16),
                pltpu.VMEM((WIDTH,), BF16),
                pltpu.VMEM((8, WIDTH), F32),
                pltpu.VMEM((WIDTH, QCOLS + 2 * HEAD_DIM), BF16),
                pltpu.VMEM((WIDTH, FFCOLS), BF16),
                pltpu.VMEM((WIDTH, FFCOLS), BF16),
                pltpu.VMEM((KDOWN, WIDTH), BF16),
                pltpu.VMEM((TOKENS, HEAD_DIM), F32),
                pltpu.VMEM((2, ROWS, WIDTH), BF16),
                pltpu.VMEM((2 * ROWS, HEAD_DIM), BF16),
                pltpu.VMEM((2, ROWS, TOKENS), F32),
                pltpu.VMEM((2, ROWS, TOKENS), BF16),
                pltpu.VMEM((ROWS, KDOWN), BF16),
                pltpu.VMEM((2, UNITS, HALF, 512), BF16),
                pltpu.VMEM((2, UNITS, HALF, 512), BF16),
                pltpu.VMEM((UNITS, HALF, 512), BF16),
                pltpu.VMEM((UNITS, HALF, 512), F32),
                pltpu.VMEM((UNITS, HALF, 512), BF16),
                pltpu.VMEM((UNITS, HALF, 256), BF16),
                pltpu.VMEM((UNITS, HALF, 256), F32),
                pltpu.VMEM((UNITS, HALF, 256), BF16),
                pltpu.SemaphoreType.DMA((BLOCKS + 3,)),
                pltpu.SemaphoreType.DMA((9,)),
                pltpu.SemaphoreType.DMA((8,)),
                pltpu.SemaphoreType.DMA((2, BLOCKS)),
                pltpu.SemaphoreType.DMA((4, UNITS)),
                pltpu.SemaphoreType.DMA((2,)),
            ],
            compiler_params=pltpu.CompilerParams(collective_id=0, has_side_effects=True, vmem_limit_bytes=67043328 - 8 * 1024 * 1024),
        )(x_in, g_norm, w_q, w_k, w_v, w_o, w_gate, w_up, w_down, jnp.asarray(table))
        y, k, v = pl.pallas_call(
            store_kernel,
            out_shape=(jax.ShapeDtypeStruct((TOKENS, WIDTH), BF16), jax.ShapeDtypeStruct((TOKENS, HEAD_DIM), BF16),
                       jax.ShapeDtypeStruct((TOKENS, HEAD_DIM), BF16)),
            in_specs=[any_spec] * 3,
            out_specs=(any_spec,) * 3,
            scratch_shapes=[pltpu.SemaphoreType.DMA((2 + BLOCKS,))],
            compiler_params=pltpu.CompilerParams(vmem_limit_bytes=1024 * 1024),
        )(*(pltpu.with_memory_space_constraint(part, pltpu.VMEM) for part in (y, k, v)))
        return y, k.reshape(TOKENS, 1, HEAD_DIM), v.reshape(TOKENS, 1, HEAD_DIM)

    return jax.shard_map(local_layer, mesh=mesh, in_specs=(P('dp', None), P(None), P(None, 'tp'), P(None, None), P(None, None), P('tp', None), P(None, 'tp'), P(None, 'tp'), P('tp', None)), out_specs=(P('dp', None), P('dp', 'tp', None), P('dp', 'tp', None)), check_vma=False)
```

```python
import math
import numpy as np
import jax
import jax.numpy as jnp
from jax import lax
from jax.experimental import pallas as pl
from jax.experimental.pallas import tpu as pltpu
from jax.sharding import PartitionSpec as P

HEAD_DIM = 128
ROPE_BASE = 500000.0
NORM_EPS = 1e-5
TOKENS = 1536
WIDTH = 2048
QCOLS = 256
FFCOLS = 768
ROWS = 256
BLOCKS = TOKENS // ROWS
KDOWN = QCOLS + FFCOLS
HALF = ROWS // 2
UNITS = TOKENS // HALF
STAGE_SLOTS = {
    "b": (3, 3, 6, 7, 9, 11, 12, 15, 17, 22, 22, 29),
    "c": (5, 6, 10, 10, 12, 17, 17, 17, 25, 35, 35, 48),
    "d": (7, 9, 21, 21, 21, 26, 31, 32, 35, 38, 41, 59),
    "e": (24, 26, 35, 51, 51, 56, 59, 61, 62, 66, 71, 73),
}
SCORE_SCALE = math.log2(math.e) / math.sqrt(HEAD_DIM)
F32 = jnp.float32
BF16 = jnp.bfloat16
MESH = pl.DeviceIdType.MESH

D2D_FIRST, D2D_SECOND, RED_PASS, RED_STAY, RED_TWO, GAT_ONE, GAT_OWN, GAT_PASS, OUT_FIRST, OUT_SECOND = range(10)


def rope_table():
    inv_freq = np.float32(ROPE_BASE) ** (-np.arange(0, HEAD_DIM, 2, dtype=np.float32) / np.float32(HEAD_DIM))
    angles = np.arange(TOKENS, dtype=np.float32)[:, None] * inv_freq.astype(np.float32)[None, :]
    angles = angles.astype(np.float64)
    return np.concatenate([np.cos(angles), np.sin(angles)], axis=1).astype(np.float32)


def layer_kernel(x_hbm, g_hbm, wq_hbm, wk_hbm, wv_hbm, wo_hbm, wg_hbm, wu_hbm, wd_hbm, tab_hbm,
                 y_v, k_v, v_v,
                 x_v, g_v, gf_v, wqkv_v, wg_v, wu_v, wod_v, tab_v,
                 a_v, q_v, s_v, p_v, om_v,
                 d2d_src, d2d_dst, h_send, h_keep, r1_dst, p_send, r2_dst,
                 x_sem, w_sem, ssem, pair_sem, link_sem, out_sem):
    me = lax.axis_index('tp')
    core = lax.rem(me, 2)
    xpos = lax.rem(me // 2, 2)
    ypos = me // 4
    sibling = me + 1 - 2 * core
    xpeer = me + 2 - 4 * xpos
    ypeer = me + 4 - 8 * ypos
    p1 = xpos + core * (ypos - xpos)
    p2 = ypos + core * (xpos - ypos)
    n1 = xpeer + core * (ypeer - xpeer)
    n2 = ypeer + core * (xpeer - ypeer)

    def rows_of(b):
        return pl.ds(pl.multiple_of(b * ROWS, ROWS), ROWS)

    def load(src, dst, index):
        return pltpu.make_async_copy(src, dst, w_sem.at[index])

    def load_x(b):
        return pltpu.make_async_copy(x_hbm.at[rows_of(b), :], x_v.at[rows_of(b), :], x_sem.at[b])

    def load_first(n):
        rows = pl.ds(n * 64, 64)
        return pltpu.make_async_copy(x_hbm.at[rows, :], x_v.at[rows, :], x_sem.at[0 if n == 0 else BLOCKS - 1 + n])

    kv_cols = pl.ds(pl.multiple_of(me * HEAD_DIM, HEAD_DIM), HEAD_DIM)
    early, late = pl.ds(0, 2 * ROWS), pl.ds(2 * ROWS, TOKENS - 2 * ROWS)
    load_g = load(g_hbm, g_v, 0)
    load_qkv = [
        load(wk_hbm.at[:, kv_cols], wqkv_v.at[:, pl.ds(QCOLS, HEAD_DIM)], 1),
        load(wv_hbm.at[:, kv_cols], wqkv_v.at[:, pl.ds(QCOLS + HEAD_DIM, HEAD_DIM)], 1),
        load(wq_hbm, wqkv_v.at[:, pl.ds(0, QCOLS)], 1),
    ]
    wait_qkv = load(wqkv_v, wqkv_v, 1)
    load_early = load(tab_hbm.at[early, :], tab_v.at[early, :], 2)
    load_gu, wait_gu = [], []
    for n in range(FFCOLS // 256):
        tile = pl.ds(n * 256, 256)
        load_gu.append((load(wg_hbm.at[:, tile], wg_v.at[:, tile], 3 + n), load(wu_hbm.at[:, tile], wu_v.at[:, tile], 3 + n)))
        both = wg_v.at[:, pl.ds(0, 512)]
        wait_gu.append(load(both, both, 3 + n))
    load_od, wait_od = [], []
    for n, half in enumerate((1 - core, core)):
        cols = pl.ds(pl.multiple_of(half * 1024, 1024), 1024)
        load_od.append((load(wo_hbm.at[:, cols], wod_v.at[pl.ds(0, QCOLS), cols], 6 + n),
                        load(wd_hbm.at[:, cols], wod_v.at[pl.ds(QCOLS, FFCOLS), cols], 6 + n)))
        wait_od.append(load(wod_v.at[:, cols], wod_v.at[:, cols], 6 + n))
    load_tab = load(tab_hbm.at[late, :], tab_v.at[late, :], 8)

    load_g.start()
    for n in range(4):
        load_first(n).start()
    for copy in load_qkv:
        copy.start()
    load_early.start()

    barrier = pltpu.get_barrier_semaphore()
    for peer in (sibling, xpeer, ypeer):
        pl.semaphore_signal(barrier, inc=1, device_id={'tp': peer}, device_id_type=MESH)

    def remote(kind, src, dst, recv, peer):
        return pltpu.make_async_remote_copy(src_ref=src, dst_ref=dst, send_sem=ssem.at[kind], recv_sem=recv,
                                            device_id={'tp': peer}, device_id_type=MESH)

    mine = core * 4 + p1 * 2
    other = core * 4 + (1 - p1) * 2

    def half_rows(u):
        return pl.ds(pl.multiple_of(u * HALF, HALF), HALF)

    def y_part(u, piece, count):
        return y_v.at[half_rows(u), pl.ds(pl.multiple_of(piece * 256, 256), count * 256)]

    def pair_copy(kind, b):
        units = pl.ds(2 * b, 2)
        return remote(kind, d2d_src.at[kind, units], d2d_dst.at[kind, units], pair_sem.at[kind, b], sibling)

    def quarter_cols(index):
        return pl.ds(pl.multiple_of(index * 256, 256), 256)

    def copy_of(kind, u):
        if kind in (OUT_FIRST, OUT_SECOND):
            part = y_part(u, mine if kind == OUT_FIRST else other, 2)
            return remote(kind, part, part, out_sem.at[kind - OUT_FIRST], sibling)
        sem = link_sem.at[kind - RED_PASS, u]
        if kind in (RED_PASS, RED_STAY):
            cols = quarter_cols(1 - p2 if kind == RED_PASS else p2)
            return remote(kind, h_send.at[u, :, cols], r1_dst.at[u, :, cols], sem, n1)
        if kind == RED_TWO:
            return remote(kind, p_send.at[u], r2_dst.at[u], sem, n2)
        part = y_part(u, mine + (1 - p2 if kind == GAT_PASS else p2), 1)
        return remote(kind, part, part, sem, n2 if kind == GAT_ONE else n1)

    def all_of(kind):
        small = RED_PASS <= kind <= GAT_PASS
        src, dst = (p_send, r2_dst) if small else (h_send, r1_dst)
        return remote(kind, src, dst, out_sem.at[1 if kind == OUT_SECOND else 0], sibling)

    def norm_rows(b, r):
        x_f = x_v[pl.ds(pl.multiple_of(b * ROWS + r * 16, 16), 16), :].astype(F32)
        inv = lax.rsqrt(jnp.mean(x_f * x_f, axis=-1, keepdims=True) + NORM_EPS)
        gain = jnp.concatenate([gf_v[...], gf_v[...]], axis=0)
        a_v[b % 2, pl.ds(r * 16, 16), :] = (x_f * inv * gain).astype(BF16)

    def first_norm():
        load_g.wait()
        gf_v[...] = jnp.broadcast_to(g_v[...].astype(F32)[None, :], (8, WIDTH))
        for n in range(4):
            load_first(n).wait()
            if n < 3:
                for copy in load_gu[n]:
                    copy.start()
            for r in range(n * 4, n * 4 + 4):
                norm_rows(0, r)
        wait_qkv.wait()
        load_early.wait()
        pl.semaphore_wait(barrier, 3)

    def project(b):
        @pl.when(b == 2)
        def _():
            load_tab.wait()

        tab = tab_v[rows_of(b), :]
        swapped = pltpu.roll(tab, HEAD_DIM // 2, 1)
        low = lax.broadcasted_iota(jnp.int32, tab.shape, 1) < HEAD_DIM // 2
        cos = jnp.where(low, tab, swapped)
        sin = jnp.where(low, -swapped, tab)
        qkv = jnp.dot(a_v[lax.rem(b, 2)], wqkv_v[...], preferred_element_type=F32)

        def rope(h):
            return (h * cos + pltpu.roll(h, HEAD_DIM // 2, 1) * sin).astype(BF16)

        q_v[pl.ds(0, ROWS), :] = rope(qkv[:, 0:128])
        q_v[pl.ds(ROWS, ROWS), :] = rope(qkv[:, 128:256])
        k_v[rows_of(b), :] = rope(qkv[:, 256:384])
        v_v[rows_of(b), :] = qkv[:, 384:512].astype(BF16)

    def attention(b):
        def tile(j):
            return pl.ds(j * ROWS, ROWS)

        heads = range(2)
        peak, total, shift = [None] * 2, [None] * 2, [None] * 2
        for j in range(b + 1):
            for h in heads:
                q = q_v[pl.ds(h * ROWS, ROWS), :]
                s = lax.dot_general(q, k_v[tile(j), :], (((1,), (1,)), ((), ())), preferred_element_type=F32) * SCORE_SCALE
                if j == b:
                    qpos = lax.broadcasted_iota(jnp.int32, (ROWS, ROWS), 0)
                    kpos = lax.broadcasted_iota(jnp.int32, (ROWS, ROWS), 1)
                    s = jnp.where(kpos <= qpos, s, -1e30)
                s_v[h, :, tile(j)] = s
                pair = jnp.maximum(s[:, :128], s[:, 128:])
                peak[h] = pair if j == 0 else jnp.maximum(peak[h], pair)
                yield
        for h in heads:
            peak[h] = jnp.max(peak[h], axis=1, keepdims=True)
        for j in range(b + 1):
            for h in heads:
                e = jnp.exp2(s_v[h, :, tile(j)] - peak[h])
                pair = e[:, :128] + e[:, 128:]
                total[h] = pair if j == 0 else total[h] + pair
                yield
        for h in heads:
            shift[h] = peak[h] + jnp.log2(jnp.sum(total[h], axis=1, keepdims=True))
        for j in range(b + 1):
            for h in heads:
                p_v[h, :, tile(j)] = jnp.exp2(s_v[h, :, tile(j)] - shift[h]).astype(BF16)
                yield
        keys = pl.ds(0, (b + 1) * ROWS)
        for h in heads:
            o = jnp.dot(p_v[h, :, keys], v_v[keys, :], preferred_element_type=F32)
            om_v[:, pl.ds(h * HEAD_DIM, HEAD_DIM)] = o.astype(BF16)
            yield

    def gate_up(b):
        normed = a_v.at[b % 2]
        for n in range(FFCOLS // 256):
            if b == 0:
                wait_gu[n].wait()
            cols = pl.ds(n * 256, 256)
            gate = jnp.dot(normed[...], wg_v[:, cols], preferred_element_type=F32)
            yield
            up = jnp.dot(normed[...], wu_v[:, cols], preferred_element_type=F32)
            om_v[:, pl.ds(QCOLS + n * 256, 256)] = (gate * (1.0 / (1.0 + jnp.exp(-gate))) * up).astype(BF16)
            yield

    def next_norm(b):
        for r in range(ROWS // 16):
            norm_rows(b + 1, r)
            yield

    def mix_block(b):
        works = [(gate_up(b), [k / 6 for k in range(6)])]
        count = 6 * (b + 1) + 2
        works.append((attention(b), [k / count for k in range(count)]))
        if b == 0:
            for copy in load_od[0]:
                copy.start()
            load_x(1).start()
            for copy in load_od[1]:
                copy.start()
        elif b < BLOCKS - 1:
            count = ROWS // 16
            load_x(b + 1).wait()
            works.append((next_norm(b), [k / count for k in range(count)]))
        turns = sorted((turn, index) for index, (_, turns) in enumerate(works) for turn in turns)
        for _, index in turns:
            next(works[index][0])
        for work, _ in works:
            for _ in work:
                pass
        if b == 0:
            wait_od[0].wait()
        pair_product(D2D_FIRST, 1 - p2, b)
        pair_copy(D2D_FIRST, b).start()

    def mix(i):
        for b in range(BLOCKS):
            @pl.when(i == b)
            def _():
                mix_block(b)

    def down(half, quarter):
        cols = pl.ds(pl.multiple_of(half * 1024 + quarter * 512, 512), 512)
        return jnp.dot(om_v[...], wod_v[:, cols], preferred_element_type=F32)

    def pair_product(kind, quarter, b):
        part = down(1 - core, quarter).astype(BF16)
        for s in range(2):
            d2d_src[kind, 2 * b + s] = part[s * HALF:(s + 1) * HALF]

    def down_rest(i):
        def rest(b, first):
            norms = iter(range(ROWS // 16) if first else ())

            def some_norms():
                for _ in range(6):
                    for r in norms:
                        norm_rows(1, r)
                        break

            pair_product(D2D_SECOND, p2, b)
            some_norms()
            send = down(core, 1 - p1)
            some_norms()
            keep = down(core, p1)
            some_norms()
            for s in range(2):
                h_keep[2 * b + s] = keep[s * HALF:(s + 1) * HALF]
            pair_copy(D2D_SECOND, b).start()
            with jax.named_scope("recv"):
                pair_copy(D2D_FIRST, b).wait_recv()
            for s in range(2):
                u = 2 * b + s
                h_send[u] = (send[s * HALF:(s + 1) * HALF] + d2d_dst[0, u].astype(F32)).astype(BF16)
                copy_of(RED_PASS, u).start()
                copy_of(RED_STAY, u).start()

        @pl.when(i == 0)
        def _():
            wait_od[1].wait()
            load_x(1).wait()
            rest(0, True)
            load_tab.start()
            for n in range(2, BLOCKS):
                load_x(n).start()

        @pl.when(i > 0)
        def _():
            rest(i, False)

    def stage_b(u):
        with jax.named_scope("recv"):
            copy_of(RED_PASS, u).wait_recv()
            if u % 2 == 0:
                pair_copy(D2D_SECOND, u // 2).wait_recv()
        p_send[u] = partial(u, quarter_cols(1 - p2)).astype(BF16)
        copy_of(RED_TWO, u).start()

    def partial(u, cols):
        return h_keep[u, :, cols] + d2d_dst[1, u, :, cols].astype(F32) + r1_dst[u, :, cols].astype(F32)

    def stage_c(u):
        with jax.named_scope("recv"):
            copy_of(RED_STAY, u).wait_recv()
            copy_of(RED_TWO, u).wait_recv()
        cols = quarter_cols(mine + p2)
        x_f = x_v[half_rows(u), cols].astype(F32)
        y_v[half_rows(u), cols] = (x_f + (partial(u, quarter_cols(p2)) + r2_dst[u].astype(F32))).astype(BF16)
        copy_of(GAT_ONE, u).start()
        copy_of(GAT_OWN, u).start()

    def stage_d(u):
        with jax.named_scope("recv"):
            copy_of(GAT_ONE, u).wait_recv()
        copy_of(GAT_PASS, u).start()
        copy_of(OUT_FIRST, u).start()

    def stage_e(u):
        with jax.named_scope("recv"):
            copy_of(GAT_OWN, u).wait_recv()
            copy_of(GAT_PASS, u).wait_recv()
        copy_of(OUT_SECOND, u).start()

    stages = {"b": stage_b, "c": stage_c, "d": stage_d, "e": stage_e}

    slots = {}
    for name in "bcde":
        for u in range(UNITS):
            slots.setdefault(STAGE_SLOTS[name][u], []).append((name, u))

    def communicate(slot):
        for name, u in slots.get(slot, ()):
            with jax.named_scope("stage_" + name):
                stages[name](u)

    def next_project(i):
        @pl.when(i < BLOCKS - 1)
        def _():
            project(i + 1)

    def step(i, carry):
        for point, part in enumerate((mix, down_rest, next_project)):
            with jax.named_scope(part.__name__):
                part(i)
            for b in range(BLOCKS):
                if 3 * b + point in slots:
                    @pl.when(i == b)
                    def _():
                        communicate(3 * b + point)

        return carry

    with jax.named_scope("first"):
        first_norm()
        project(0)
    lax.fori_loop(0, BLOCKS, step, 0)
    for slot in range(3 * BLOCKS, max(slots) + 1):
        communicate(slot)

    with jax.named_scope("finish"):
        for kind in (OUT_FIRST, OUT_SECOND):
            all_of(kind).wait_recv()
        for kind in range(10):
            all_of(kind).wait_send()


def store_kernel(y_v, k_v, v_v, y_out, k_out, v_out, sem):
    copies = [pltpu.make_async_copy(k_v, k_out, sem.at[0]), pltpu.make_async_copy(v_v, v_out, sem.at[1])]
    for b in range(BLOCKS):
        rows = pl.ds(b * ROWS, ROWS)
        copies.append(pltpu.make_async_copy(y_v.at[rows, :], y_out.at[rows, :], sem.at[2 + b]))
    for copy in copies:
        copy.start()
    for copy in copies:
        copy.wait()


def solution(mesh):
    table = rope_table()

    def local_layer(x_in, g_norm, w_q, w_k, w_v, w_o, w_gate, w_up, w_down):
        any_spec = pl.BlockSpec(memory_space=pl.ANY)
        y, k, v = pl.pallas_call(
            layer_kernel,
            out_shape=(pltpu.VMEM((TOKENS, WIDTH), BF16), pltpu.VMEM((TOKENS, HEAD_DIM), BF16), pltpu.VMEM((TOKENS, HEAD_DIM), BF16)),
            in_specs=[any_spec] * 10,
            out_specs=(pl.BlockSpec(memory_space=pltpu.VMEM),) * 3,
            scratch_shapes=[
                pltpu.VMEM((TOKENS, WIDTH), BF16),
                pltpu.VMEM((WIDTH,), BF16),
                pltpu.VMEM((8, WIDTH), F32),
                pltpu.VMEM((WIDTH, QCOLS + 2 * HEAD_DIM), BF16),
                pltpu.VMEM((WIDTH, FFCOLS), BF16),
                pltpu.VMEM((WIDTH, FFCOLS), BF16),
                pltpu.VMEM((KDOWN, WIDTH), BF16),
                pltpu.VMEM((TOKENS, HEAD_DIM), F32),
                pltpu.VMEM((2, ROWS, WIDTH), BF16),
                pltpu.VMEM((2 * ROWS, HEAD_DIM), BF16),
                pltpu.VMEM((2, ROWS, TOKENS), F32),
                pltpu.VMEM((2, ROWS, TOKENS), BF16),
                pltpu.VMEM((ROWS, KDOWN), BF16),
                pltpu.VMEM((2, UNITS, HALF, 512), BF16),
                pltpu.VMEM((2, UNITS, HALF, 512), BF16),
                pltpu.VMEM((UNITS, HALF, 512), BF16),
                pltpu.VMEM((UNITS, HALF, 512), F32),
                pltpu.VMEM((UNITS, HALF, 512), BF16),
                pltpu.VMEM((UNITS, HALF, 256), BF16),
                pltpu.VMEM((UNITS, HALF, 256), BF16),
                pltpu.SemaphoreType.DMA((BLOCKS + 3,)),
                pltpu.SemaphoreType.DMA((9,)),
                pltpu.SemaphoreType.DMA((10,)),
                pltpu.SemaphoreType.DMA((2, BLOCKS)),
                pltpu.SemaphoreType.DMA((6, UNITS)),
                pltpu.SemaphoreType.DMA((2,)),
            ],
            compiler_params=pltpu.CompilerParams(collective_id=0, has_side_effects=True, vmem_limit_bytes=67043328 - 8 * 1024 * 1024),
        )(x_in, g_norm, w_q, w_k, w_v, w_o, w_gate, w_up, w_down, jnp.asarray(table))
        y, k, v = pl.pallas_call(
            store_kernel,
            out_shape=(jax.ShapeDtypeStruct((TOKENS, WIDTH), BF16), jax.ShapeDtypeStruct((TOKENS, HEAD_DIM), BF16),
                       jax.ShapeDtypeStruct((TOKENS, HEAD_DIM), BF16)),
            in_specs=[any_spec] * 3,
            out_specs=(any_spec,) * 3,
            scratch_shapes=[pltpu.SemaphoreType.DMA((2 + BLOCKS,))],
            compiler_params=pltpu.CompilerParams(vmem_limit_bytes=1024 * 1024),
        )(*(pltpu.with_memory_space_constraint(part, pltpu.VMEM) for part in (y, k, v)))
        return y, k.reshape(TOKENS, 1, HEAD_DIM), v.reshape(TOKENS, 1, HEAD_DIM)

    return jax.shard_map(local_layer, mesh=mesh, in_specs=(P('dp', None), P(None), P(None, 'tp'), P(None, None), P(None, None), P('tp', None), P(None, 'tp'), P(None, 'tp'), P('tp', None)), out_specs=(P('dp', None), P('dp', 'tp', None), P('dp', 'tp', None)), check_vma=False)
```

```python
import math
import numpy as np
import jax
import jax.numpy as jnp
from jax import lax
from jax.experimental import pallas as pl
from jax.experimental.pallas import tpu as pltpu
from jax.sharding import PartitionSpec as P

HEAD_DIM = 128
ROPE_BASE = 500000.0
NORM_EPS = 1e-5
TOKENS = 1536
WIDTH = 2048
QCOLS = 256
FFCOLS = 768
ROWS = 256
BLOCKS = TOKENS // ROWS
KDOWN = QCOLS + FFCOLS
HALF = ROWS // 2
UNITS = TOKENS // HALF
STAGE_SLOTS = {
    "b": (3, 3, 6, 6, 9, 9, 12, 17, 23, 27, 27, 32),
    "c": (5, 5, 9, 11, 13, 17, 20, 23, 39, 39, 40, 46),
    "d": (6, 8, 13, 14, 17, 38, 43, 44, 45, 56, 57, 60),
    "e": (9, 25, 27, 34, 42, 56, 63, 64, 83, 88, 90, 94),
}
SCORE_SCALE = math.log2(math.e) / math.sqrt(HEAD_DIM)
F32 = jnp.float32
BF16 = jnp.bfloat16
MESH = pl.DeviceIdType.MESH

PAIR_PASS, PAIR_STAY, PAIR_KEEP, RED_PASS, RED_STAY, RED_TWO, GAT_ONE, GAT_OWN, GAT_PASS, OUT_FIRST, OUT_SECOND = range(11)


def rope_table():
    inv_freq = np.float32(ROPE_BASE) ** (-np.arange(0, HEAD_DIM, 2, dtype=np.float32) / np.float32(HEAD_DIM))
    angles = np.arange(TOKENS, dtype=np.float32)[:, None] * inv_freq.astype(np.float32)[None, :]
    angles = angles.astype(np.float64)
    return np.concatenate([np.cos(angles), np.sin(angles)], axis=1).astype(np.float32)


def layer_kernel(x_hbm, g_hbm, wq_hbm, wk_hbm, wv_hbm, wo_hbm, wg_hbm, wu_hbm, wd_hbm, tab_hbm,
                 y_v, k_v, v_v,
                 x_v, g_v, gf_v, wqkv_v, wg_v, wu_v, wod_v, tab_v,
                 a_v, q_v, s_v, p_v, om_v,
                 d2d_src, d2d_dst, h_send, h_keep, r1_dst, p_send, r2_dst, send_v,
                 x_sem, w_sem, ssem, pair_sem, link_sem, out_sem):
    me = lax.axis_index('tp')
    core = lax.rem(me, 2)
    xpos = lax.rem(me // 2, 2)
    ypos = me // 4
    sibling = me + 1 - 2 * core
    xpeer = me + 2 - 4 * xpos
    ypeer = me + 4 - 8 * ypos
    p1 = xpos + core * (ypos - xpos)
    p2 = ypos + core * (xpos - ypos)
    n1 = xpeer + core * (ypeer - xpeer)
    n2 = ypeer + core * (xpeer - ypeer)

    def rows_of(b):
        return pl.ds(pl.multiple_of(b * ROWS, ROWS), ROWS)

    def load(src, dst, index):
        return pltpu.make_async_copy(src, dst, w_sem.at[index])

    def load_x(b):
        return pltpu.make_async_copy(x_hbm.at[rows_of(b), :], x_v.at[rows_of(b), :], x_sem.at[b])

    def load_first(n):
        rows = pl.ds(n * 64, 64)
        return pltpu.make_async_copy(x_hbm.at[rows, :], x_v.at[rows, :], x_sem.at[0 if n == 0 else BLOCKS - 1 + n])

    kv_cols = pl.ds(pl.multiple_of(me * HEAD_DIM, HEAD_DIM), HEAD_DIM)
    early, late = pl.ds(0, 2 * ROWS), pl.ds(2 * ROWS, TOKENS - 2 * ROWS)
    load_g = load(g_hbm, g_v, 0)
    load_qkv = [
        load(wk_hbm.at[:, kv_cols], wqkv_v.at[:, pl.ds(QCOLS, HEAD_DIM)], 1),
        load(wv_hbm.at[:, kv_cols], wqkv_v.at[:, pl.ds(QCOLS + HEAD_DIM, HEAD_DIM)], 1),
        load(wq_hbm, wqkv_v.at[:, pl.ds(0, QCOLS)], 1),
    ]
    wait_qkv = load(wqkv_v, wqkv_v, 1)
    load_early = load(tab_hbm.at[early, :], tab_v.at[early, :], 2)
    load_gu, wait_gu = [], []
    for n in range(FFCOLS // 256):
        tile = pl.ds(n * 256, 256)
        load_gu.append((load(wg_hbm.at[:, tile], wg_v.at[:, tile], 3 + n), load(wu_hbm.at[:, tile], wu_v.at[:, tile], 3 + n)))
        both = wg_v.at[:, pl.ds(0, 512)]
        wait_gu.append(load(both, both, 3 + n))
    load_od, wait_od = [], []
    for n, half in enumerate((1 - core, core)):
        cols = pl.ds(pl.multiple_of(half * 1024, 1024), 1024)
        load_od.append((load(wo_hbm.at[:, cols], wod_v.at[pl.ds(0, QCOLS), cols], 6 + n),
                        load(wd_hbm.at[:, cols], wod_v.at[pl.ds(QCOLS, FFCOLS), cols], 6 + n)))
        wait_od.append(load(wod_v.at[:, cols], wod_v.at[:, cols], 6 + n))
    load_tab = load(tab_hbm.at[late, :], tab_v.at[late, :], 8)

    load_g.start()
    for n in range(4):
        load_first(n).start()
    for copy in load_qkv:
        copy.start()
    load_early.start()

    barrier = pltpu.get_barrier_semaphore()
    for peer in (sibling, xpeer, ypeer):
        pl.semaphore_signal(barrier, inc=1, device_id={'tp': peer}, device_id_type=MESH)

    def remote(kind, src, dst, recv, peer):
        return pltpu.make_async_remote_copy(src_ref=src, dst_ref=dst, send_sem=ssem.at[kind], recv_sem=recv,
                                            device_id={'tp': peer}, device_id_type=MESH)

    mine = core * 4 + p1 * 2
    other = core * 4 + (1 - p1) * 2

    def half_rows(u):
        return pl.ds(pl.multiple_of(u * HALF, HALF), HALF)

    def y_part(u, piece, count):
        return y_v.at[half_rows(u), pl.ds(pl.multiple_of(piece * 256, 256), count * 256)]

    def quarter_cols(index):
        return pl.ds(pl.multiple_of(index * 256, 256), 256)

    def pair_copy(kind, b):
        units = pl.ds(2 * b, 2)
        if kind == PAIR_KEEP:
            src, dst = d2d_src.at[1, units], d2d_dst.at[1, units]
        else:
            cols = quarter_cols(1 - p1 if kind == PAIR_PASS else p1)
            src, dst = d2d_src.at[0, units, :, cols], d2d_dst.at[0, units, :, cols]
        return remote(kind, src, dst, pair_sem.at[kind, b], sibling)

    def copy_of(kind, u):
        if kind in (OUT_FIRST, OUT_SECOND):
            part = y_part(u, mine if kind == OUT_FIRST else other, 2)
            return remote(kind, part, part, out_sem.at[kind - OUT_FIRST], sibling)
        sem = link_sem.at[kind - RED_PASS, u]
        if kind in (RED_PASS, RED_STAY):
            cols = quarter_cols(1 - p2 if kind == RED_PASS else p2)
            return remote(kind, h_send.at[u, :, cols], r1_dst.at[u, :, cols], sem, n1)
        if kind == RED_TWO:
            return remote(kind, p_send.at[u], r2_dst.at[u], sem, n2)
        part = y_part(u, mine + (1 - p2 if kind == GAT_PASS else p2), 1)
        return remote(kind, part, part, sem, n2 if kind == GAT_ONE else n1)

    def all_of(kind):
        small = kind not in (PAIR_KEEP, OUT_FIRST, OUT_SECOND)
        src, dst = (p_send, r2_dst) if small else (h_send, r1_dst)
        return remote(kind, src, dst, out_sem.at[1 if kind == OUT_SECOND else 0], sibling)

    def norm_rows(b, r):
        x_f = x_v[pl.ds(pl.multiple_of(b * ROWS + r * 16, 16), 16), :].astype(F32)
        inv = lax.rsqrt(jnp.mean(x_f * x_f, axis=-1, keepdims=True) + NORM_EPS)
        gain = jnp.concatenate([gf_v[...], gf_v[...]], axis=0)
        a_v[b % 2, pl.ds(r * 16, 16), :] = (x_f * inv * gain).astype(BF16)

    def first_norm():
        load_g.wait()
        gf_v[...] = jnp.broadcast_to(g_v[...].astype(F32)[None, :], (8, WIDTH))
        for n in range(4):
            load_first(n).wait()
            if n < 3:
                for copy in load_gu[n]:
                    copy.start()
            for r in range(n * 4, n * 4 + 4):
                norm_rows(0, r)
        wait_qkv.wait()
        load_early.wait()
        pl.semaphore_wait(barrier, 3)

    def project(b):
        @pl.when(b == 2)
        def _():
            load_tab.wait()

        tab = tab_v[rows_of(b), :]
        swapped = pltpu.roll(tab, HEAD_DIM // 2, 1)
        low = lax.broadcasted_iota(jnp.int32, tab.shape, 1) < HEAD_DIM // 2
        cos = jnp.where(low, tab, swapped)
        sin = jnp.where(low, -swapped, tab)
        qkv = jnp.dot(a_v[lax.rem(b, 2)], wqkv_v[...], preferred_element_type=F32)

        def rope(h):
            return (h * cos + pltpu.roll(h, HEAD_DIM // 2, 1) * sin).astype(BF16)

        q_v[pl.ds(0, ROWS), :] = rope(qkv[:, 0:128])
        q_v[pl.ds(ROWS, ROWS), :] = rope(qkv[:, 128:256])
        k_v[rows_of(b), :] = rope(qkv[:, 256:384])
        v_v[rows_of(b), :] = qkv[:, 384:512].astype(BF16)

    def attention(b):
        def tile(j):
            return pl.ds(j * ROWS, ROWS)

        heads = range(2)
        peak, total, shift = [None] * 2, [None] * 2, [None] * 2
        for j in range(b + 1):
            for h in heads:
                q = q_v[pl.ds(h * ROWS, ROWS), :]
                s = lax.dot_general(q, k_v[tile(j), :], (((1,), (1,)), ((), ())), preferred_element_type=F32) * SCORE_SCALE
                if j == b:
                    qpos = lax.broadcasted_iota(jnp.int32, (ROWS, ROWS), 0)
                    kpos = lax.broadcasted_iota(jnp.int32, (ROWS, ROWS), 1)
                    s = jnp.where(kpos <= qpos, s, -1e30)
                s_v[h, :, tile(j)] = s
                pair = jnp.maximum(s[:, :128], s[:, 128:])
                peak[h] = pair if j == 0 else jnp.maximum(peak[h], pair)
                yield
        for h in heads:
            peak[h] = jnp.max(peak[h], axis=1, keepdims=True)
        for j in range(b + 1):
            for h in heads:
                e = jnp.exp2(s_v[h, :, tile(j)] - peak[h])
                pair = e[:, :128] + e[:, 128:]
                total[h] = pair if j == 0 else total[h] + pair
                yield
        for h in heads:
            shift[h] = peak[h] + jnp.log2(jnp.sum(total[h], axis=1, keepdims=True))
        for j in range(b + 1):
            for h in heads:
                p_v[h, :, tile(j)] = jnp.exp2(s_v[h, :, tile(j)] - shift[h]).astype(BF16)
                yield
        keys = pl.ds(0, (b + 1) * ROWS)
        for h in heads:
            o = jnp.dot(p_v[h, :, keys], v_v[keys, :], preferred_element_type=F32)
            om_v[:, pl.ds(h * HEAD_DIM, HEAD_DIM)] = o.astype(BF16)
            yield

    def gate_up(b):
        normed = a_v.at[b % 2]
        for n in range(FFCOLS // 256):
            if b == 0:
                wait_gu[n].wait()
            cols = pl.ds(n * 256, 256)
            gate = jnp.dot(normed[...], wg_v[:, cols], preferred_element_type=F32)
            yield
            up = jnp.dot(normed[...], wu_v[:, cols], preferred_element_type=F32)
            om_v[:, pl.ds(QCOLS + n * 256, 256)] = (gate * (1.0 / (1.0 + jnp.exp(-gate))) * up).astype(BF16)
            yield

    def next_norm(b):
        for r in range(ROWS // 16):
            norm_rows(b + 1, r)
            yield

    def mix_block(b):
        works = [(gate_up(b), [k / 6 for k in range(6)])]
        count = 6 * (b + 1) + 2
        works.append((attention(b), [k / count for k in range(count)]))
        if b == 0:
            for copy in load_od[0]:
                copy.start()
            load_x(1).start()
            for copy in load_od[1]:
                copy.start()
        elif b < BLOCKS - 1:
            count = ROWS // 16
            load_x(b + 1).wait()
            works.append((next_norm(b), [k / count for k in range(count)]))
        turns = sorted((turn, index) for index, (_, turns) in enumerate(works) for turn in turns)
        for _, index in turns:
            next(works[index][0])
        for work, _ in works:
            for _ in work:
                pass
        if b == 0:
            wait_od[0].wait()
        pair_product(0, 1 - p2, b)
        pair_copy(PAIR_PASS, b).start()
        pair_copy(PAIR_STAY, b).start()

    def mix(i):
        for b in range(BLOCKS):
            @pl.when(i == b)
            def _():
                mix_block(b)

    def down(half, quarter):
        cols = pl.ds(pl.multiple_of(half * 1024 + quarter * 512, 512), 512)
        return jnp.dot(om_v[...], wod_v[:, cols], preferred_element_type=F32)

    def pair_product(slot, quarter, b):
        part = down(1 - core, quarter).astype(BF16)
        for s in range(2):
            d2d_src[slot, 2 * b + s] = part[s * HALF:(s + 1) * HALF]

    def down_rest(i):
        def rest(b, first):
            norms = iter(range(ROWS // 16) if first else ())

            def some_norms():
                for _ in range(6):
                    for r in norms:
                        norm_rows(1, r)
                        break

            pair_product(1, p2, b)
            some_norms()
            send_v[...] = down(core, 1 - p1)
            some_norms()
            keep = down(core, p1)
            some_norms()
            for s in range(2):
                h_keep[2 * b + s] = keep[s * HALF:(s + 1) * HALF]
            pair_copy(PAIR_KEEP, b).start()
            for kind, pair, index in ((RED_PASS, PAIR_PASS, 1 - p2), (RED_STAY, PAIR_STAY, p2)):
                with jax.named_scope("recv"):
                    pair_copy(pair, b).wait_recv()
                cols = quarter_cols(index)
                for s in range(2):
                    u = 2 * b + s
                    h_send[u, :, cols] = (send_v[pl.ds(s * HALF, HALF), cols] + d2d_dst[0, u, :, cols].astype(F32)).astype(BF16)
                for s in range(2):
                    copy_of(kind, 2 * b + s).start()

        @pl.when(i == 0)
        def _():
            wait_od[1].wait()
            load_x(1).wait()
            rest(0, True)
            load_tab.start()
            for n in range(2, BLOCKS):
                load_x(n).start()

        @pl.when(i > 0)
        def _():
            rest(i, False)

    def stage_b(u):
        with jax.named_scope("recv"):
            copy_of(RED_PASS, u).wait_recv()
            if u % 2 == 0:
                pair_copy(PAIR_KEEP, u // 2).wait_recv()
        p_send[u] = partial(u, quarter_cols(1 - p2)).astype(BF16)
        copy_of(RED_TWO, u).start()

    def partial(u, cols):
        return h_keep[u, :, cols] + d2d_dst[1, u, :, cols].astype(F32) + r1_dst[u, :, cols].astype(F32)

    def stage_c(u):
        with jax.named_scope("recv"):
            copy_of(RED_STAY, u).wait_recv()
            copy_of(RED_TWO, u).wait_recv()
        cols = quarter_cols(mine + p2)
        x_f = x_v[half_rows(u), cols].astype(F32)
        y_v[half_rows(u), cols] = (x_f + (partial(u, quarter_cols(p2)) + r2_dst[u].astype(F32))).astype(BF16)
        copy_of(GAT_ONE, u).start()
        copy_of(GAT_OWN, u).start()

    def stage_d(u):
        with jax.named_scope("recv"):
            copy_of(GAT_ONE, u).wait_recv()
        copy_of(GAT_PASS, u).start()
        copy_of(OUT_FIRST, u).start()

    def stage_e(u):
        with jax.named_scope("recv"):
            copy_of(GAT_OWN, u).wait_recv()
            copy_of(GAT_PASS, u).wait_recv()
        copy_of(OUT_SECOND, u).start()

    stages = {"b": stage_b, "c": stage_c, "d": stage_d, "e": stage_e}

    slots = {}
    for name in "bcde":
        for u in range(UNITS):
            slots.setdefault(STAGE_SLOTS[name][u], []).append((name, u))

    def communicate(slot):
        for name, u in slots.get(slot, ()):
            with jax.named_scope("stage_" + name):
                stages[name](u)

    def next_project(i):
        @pl.when(i < BLOCKS - 1)
        def _():
            project(i + 1)

    def step(i, carry):
        for point, part in enumerate((mix, down_rest, next_project)):
            with jax.named_scope(part.__name__):
                part(i)
            for b in range(BLOCKS):
                if 3 * b + point in slots:
                    @pl.when(i == b)
                    def _():
                        communicate(3 * b + point)

        return carry

    with jax.named_scope("first"):
        first_norm()
        project(0)
    lax.fori_loop(0, BLOCKS, step, 0)
    for slot in range(3 * BLOCKS, max(slots) + 1):
        communicate(slot)

    with jax.named_scope("finish"):
        for kind in (OUT_FIRST, OUT_SECOND):
            all_of(kind).wait_recv()
        for kind in range(11):
            all_of(kind).wait_send()


def store_kernel(y_v, k_v, v_v, y_out, k_out, v_out, sem):
    copies = [pltpu.make_async_copy(k_v, k_out, sem.at[0]), pltpu.make_async_copy(v_v, v_out, sem.at[1])]
    for b in range(BLOCKS):
        rows = pl.ds(b * ROWS, ROWS)
        copies.append(pltpu.make_async_copy(y_v.at[rows, :], y_out.at[rows, :], sem.at[2 + b]))
    for copy in copies:
        copy.start()
    for copy in copies:
        copy.wait()


def solution(mesh):
    table = rope_table()

    def local_layer(x_in, g_norm, w_q, w_k, w_v, w_o, w_gate, w_up, w_down):
        any_spec = pl.BlockSpec(memory_space=pl.ANY)
        y, k, v = pl.pallas_call(
            layer_kernel,
            out_shape=(pltpu.VMEM((TOKENS, WIDTH), BF16), pltpu.VMEM((TOKENS, HEAD_DIM), BF16), pltpu.VMEM((TOKENS, HEAD_DIM), BF16)),
            in_specs=[any_spec] * 10,
            out_specs=(pl.BlockSpec(memory_space=pltpu.VMEM),) * 3,
            scratch_shapes=[
                pltpu.VMEM((TOKENS, WIDTH), BF16),
                pltpu.VMEM((WIDTH,), BF16),
                pltpu.VMEM((8, WIDTH), F32),
                pltpu.VMEM((WIDTH, QCOLS + 2 * HEAD_DIM), BF16),
                pltpu.VMEM((WIDTH, FFCOLS), BF16),
                pltpu.VMEM((WIDTH, FFCOLS), BF16),
                pltpu.VMEM((KDOWN, WIDTH), BF16),
                pltpu.VMEM((TOKENS, HEAD_DIM), F32),
                pltpu.VMEM((2, ROWS, WIDTH), BF16),
                pltpu.VMEM((2 * ROWS, HEAD_DIM), BF16),
                pltpu.VMEM((2, ROWS, TOKENS), F32),
                pltpu.VMEM((2, ROWS, TOKENS), BF16),
                pltpu.VMEM((ROWS, KDOWN), BF16),
                pltpu.VMEM((2, UNITS, HALF, 512), BF16),
                pltpu.VMEM((2, UNITS, HALF, 512), BF16),
                pltpu.VMEM((UNITS, HALF, 512), BF16),
                pltpu.VMEM((UNITS, HALF, 512), F32),
                pltpu.VMEM((UNITS, HALF, 512), BF16),
                pltpu.VMEM((UNITS, HALF, 256), BF16),
                pltpu.VMEM((UNITS, HALF, 256), BF16),
                pltpu.VMEM((ROWS, 512), F32),
                pltpu.SemaphoreType.DMA((BLOCKS + 3,)),
                pltpu.SemaphoreType.DMA((9,)),
                pltpu.SemaphoreType.DMA((11,)),
                pltpu.SemaphoreType.DMA((3, BLOCKS)),
                pltpu.SemaphoreType.DMA((6, UNITS)),
                pltpu.SemaphoreType.DMA((2,)),
            ],
            compiler_params=pltpu.CompilerParams(collective_id=0, has_side_effects=True, vmem_limit_bytes=67043328 - 8 * 1024 * 1024),
        )(x_in, g_norm, w_q, w_k, w_v, w_o, w_gate, w_up, w_down, jnp.asarray(table))
        y, k, v = pl.pallas_call(
            store_kernel,
            out_shape=(jax.ShapeDtypeStruct((TOKENS, WIDTH), BF16), jax.ShapeDtypeStruct((TOKENS, HEAD_DIM), BF16),
                       jax.ShapeDtypeStruct((TOKENS, HEAD_DIM), BF16)),
            in_specs=[any_spec] * 3,
            out_specs=(any_spec,) * 3,
            scratch_shapes=[pltpu.SemaphoreType.DMA((2 + BLOCKS,))],
            compiler_params=pltpu.CompilerParams(vmem_limit_bytes=1024 * 1024),
        )(*(pltpu.with_memory_space_constraint(part, pltpu.VMEM) for part in (y, k, v)))
        return y, k.reshape(TOKENS, 1, HEAD_DIM), v.reshape(TOKENS, 1, HEAD_DIM)

    return jax.shard_map(local_layer, mesh=mesh, in_specs=(P('dp', None), P(None), P(None, 'tp'), P(None, None), P(None, None), P('tp', None), P(None, 'tp'), P(None, 'tp'), P('tp', None)), out_specs=(P('dp', None), P('dp', 'tp', None), P('dp', 'tp', None)), check_vma=False)
```

```python
import math
import numpy as np
import jax
import jax.numpy as jnp
from jax import lax
from jax.experimental import pallas as pl
from jax.experimental.pallas import tpu as pltpu
from jax.sharding import PartitionSpec as P

HEAD_DIM = 128
ROPE_BASE = 500000.0
NORM_EPS = 1e-5
TOKENS = 1536
WIDTH = 2048
QCOLS = 256
FFCOLS = 768
ROWS = 256
BLOCKS = TOKENS // ROWS
KDOWN = QCOLS + FFCOLS
HALF = ROWS // 2
UNITS = TOKENS // HALF
STAGE_SLOTS = {
    "b": (3, 3, 6, 7, 9, 11, 12, 15, 17, 22, 22, 29),
    "c": (5, 6, 10, 10, 12, 17, 17, 17, 25, 35, 35, 48),
    "d": (7, 9, 21, 21, 21, 26, 31, 32, 35, 38, 41, 59),
    "e": (24, 26, 35, 51, 51, 56, 59, 61, 62, 66, 71, 73),
}
SCORE_SCALE = math.log2(math.e) / math.sqrt(HEAD_DIM)
F32 = jnp.float32
BF16 = jnp.bfloat16
MESH = pl.DeviceIdType.MESH

PAIR_PASS, PAIR_STAY, PAIR_KEEP, RED_PASS, RED_STAY, RED_TWO, GAT_ONE, GAT_OWN, GAT_PASS, OUT_FIRST, OUT_SECOND = range(11)


def rope_table():
    inv_freq = np.float32(ROPE_BASE) ** (-np.arange(0, HEAD_DIM, 2, dtype=np.float32) / np.float32(HEAD_DIM))
    angles = np.arange(TOKENS, dtype=np.float32)[:, None] * inv_freq.astype(np.float32)[None, :]
    angles = angles.astype(np.float64)
    return np.concatenate([np.cos(angles), np.sin(angles)], axis=1).astype(np.float32)


def layer_kernel(x_hbm, g_hbm, wq_hbm, wk_hbm, wv_hbm, wo_hbm, wg_hbm, wu_hbm, wd_hbm, tab_hbm,
                 y_v, k_v, v_v,
                 x_v, g_v, gf_v, wqkv_v, wg_v, wu_v, wod_v, tab_v,
                 a_v, q_v, s_v, p_v, om_v,
                 d2d_src, d2d_dst, h_send, h_keep, r1_dst, p_send, r2_dst, send_v,
                 x_sem, w_sem, ssem, pair_sem, link_sem, out_sem):
    me = lax.axis_index('tp')
    core = lax.rem(me, 2)
    xpos = lax.rem(me // 2, 2)
    ypos = me // 4
    sibling = me + 1 - 2 * core
    xpeer = me + 2 - 4 * xpos
    ypeer = me + 4 - 8 * ypos
    p1 = xpos + core * (ypos - xpos)
    p2 = ypos + core * (xpos - ypos)
    n1 = xpeer + core * (ypeer - xpeer)
    n2 = ypeer + core * (xpeer - ypeer)

    def rows_of(b):
        return pl.ds(pl.multiple_of(b * ROWS, ROWS), ROWS)

    def load(src, dst, index):
        return pltpu.make_async_copy(src, dst, w_sem.at[index])

    def load_x(b):
        return pltpu.make_async_copy(x_hbm.at[rows_of(b), :], x_v.at[rows_of(b), :], x_sem.at[b])

    def load_first(n):
        rows = pl.ds(n * 64, 64)
        return pltpu.make_async_copy(x_hbm.at[rows, :], x_v.at[rows, :], x_sem.at[0 if n == 0 else BLOCKS - 1 + n])

    kv_cols = pl.ds(pl.multiple_of(me * HEAD_DIM, HEAD_DIM), HEAD_DIM)
    early, late = pl.ds(0, 2 * ROWS), pl.ds(2 * ROWS, TOKENS - 2 * ROWS)
    load_g = load(g_hbm, g_v, 0)
    load_qkv = [
        load(wk_hbm.at[:, kv_cols], wqkv_v.at[:, pl.ds(QCOLS, HEAD_DIM)], 1),
        load(wv_hbm.at[:, kv_cols], wqkv_v.at[:, pl.ds(QCOLS + HEAD_DIM, HEAD_DIM)], 1),
        load(wq_hbm, wqkv_v.at[:, pl.ds(0, QCOLS)], 1),
    ]
    wait_qkv = load(wqkv_v, wqkv_v, 1)
    load_early = load(tab_hbm.at[early, :], tab_v.at[early, :], 2)
    load_gu, wait_gu = [], []
    for n in range(FFCOLS // 256):
        tile = pl.ds(n * 256, 256)
        load_gu.append((load(wg_hbm.at[:, tile], wg_v.at[:, tile], 3 + n), load(wu_hbm.at[:, tile], wu_v.at[:, tile], 3 + n)))
        both = wg_v.at[:, pl.ds(0, 512)]
        wait_gu.append(load(both, both, 3 + n))
    load_od, wait_od = [], []
    for n, half in enumerate((1 - core, core)):
        cols = pl.ds(pl.multiple_of(half * 1024, 1024), 1024)
        load_od.append((load(wo_hbm.at[:, cols], wod_v.at[pl.ds(0, QCOLS), cols], 6 + n),
                        load(wd_hbm.at[:, cols], wod_v.at[pl.ds(QCOLS, FFCOLS), cols], 6 + n)))
        wait_od.append(load(wod_v.at[:, cols], wod_v.at[:, cols], 6 + n))
    load_tab = load(tab_hbm.at[late, :], tab_v.at[late, :], 8)

    load_g.start()
    for n in range(4):
        load_first(n).start()
    for copy in load_qkv:
        copy.start()
    load_early.start()

    barrier = pltpu.get_barrier_semaphore()
    for peer in (sibling, xpeer, ypeer):
        pl.semaphore_signal(barrier, inc=1, device_id={'tp': peer}, device_id_type=MESH)

    def remote(kind, src, dst, recv, peer):
        return pltpu.make_async_remote_copy(src_ref=src, dst_ref=dst, send_sem=ssem.at[kind], recv_sem=recv,
                                            device_id={'tp': peer}, device_id_type=MESH)

    mine = core * 4 + p1 * 2
    other = core * 4 + (1 - p1) * 2

    def half_rows(u):
        return pl.ds(pl.multiple_of(u * HALF, HALF), HALF)

    def y_part(u, piece, count):
        return y_v.at[half_rows(u), pl.ds(pl.multiple_of(piece * 256, 256), count * 256)]

    def quarter_cols(index):
        return pl.ds(pl.multiple_of(index * 256, 256), 256)

    def pair_copy(kind, b):
        units = pl.ds(2 * b, 2)
        if kind == PAIR_KEEP:
            src, dst = d2d_src.at[1, units], d2d_dst.at[1, units]
        else:
            cols = quarter_cols(1 - p1 if kind == PAIR_PASS else p1)
            src, dst = d2d_src.at[0, units, :, cols], d2d_dst.at[0, units, :, cols]
        return remote(kind, src, dst, pair_sem.at[kind, b], sibling)

    def copy_of(kind, u):
        if kind in (OUT_FIRST, OUT_SECOND):
            part = y_part(u, mine if kind == OUT_FIRST else other, 2)
            return remote(kind, part, part, out_sem.at[kind - OUT_FIRST], sibling)
        sem = link_sem.at[kind - RED_PASS, u]
        if kind in (RED_PASS, RED_STAY):
            cols = quarter_cols(1 - p2 if kind == RED_PASS else p2)
            return remote(kind, h_send.at[u, :, cols], r1_dst.at[u, :, cols], sem, n1)
        if kind == RED_TWO:
            return remote(kind, p_send.at[u], r2_dst.at[u], sem, n2)
        part = y_part(u, mine + (1 - p2 if kind == GAT_PASS else p2), 1)
        return remote(kind, part, part, sem, n2 if kind == GAT_ONE else n1)

    def all_of(kind):
        small = kind not in (PAIR_KEEP, OUT_FIRST, OUT_SECOND)
        src, dst = (p_send, r2_dst) if small else (h_send, r1_dst)
        return remote(kind, src, dst, out_sem.at[1 if kind == OUT_SECOND else 0], sibling)

    def norm_rows(b, r):
        x_f = x_v[pl.ds(pl.multiple_of(b * ROWS + r * 16, 16), 16), :].astype(F32)
        inv = lax.rsqrt(jnp.mean(x_f * x_f, axis=-1, keepdims=True) + NORM_EPS)
        gain = jnp.concatenate([gf_v[...], gf_v[...]], axis=0)
        a_v[b % 2, pl.ds(r * 16, 16), :] = (x_f * inv * gain).astype(BF16)

    def first_norm():
        load_g.wait()
        gf_v[...] = jnp.broadcast_to(g_v[...].astype(F32)[None, :], (8, WIDTH))
        for n in range(4):
            load_first(n).wait()
            if n < 3:
                for copy in load_gu[n]:
                    copy.start()
            for r in range(n * 4, n * 4 + 4):
                norm_rows(0, r)
        wait_qkv.wait()
        load_early.wait()
        pl.semaphore_wait(barrier, 3)

    def project(b):
        @pl.when(b == 2)
        def _():
            load_tab.wait()

        tab = tab_v[rows_of(b), :]
        swapped = pltpu.roll(tab, HEAD_DIM // 2, 1)
        low = lax.broadcasted_iota(jnp.int32, tab.shape, 1) < HEAD_DIM // 2
        cos = jnp.where(low, tab, swapped)
        sin = jnp.where(low, -swapped, tab)
        qkv = jnp.dot(a_v[lax.rem(b, 2)], wqkv_v[...], preferred_element_type=F32)

        def rope(h):
            return (h * cos + pltpu.roll(h, HEAD_DIM // 2, 1) * sin).astype(BF16)

        q_v[pl.ds(0, ROWS), :] = rope(qkv[:, 0:128])
        q_v[pl.ds(ROWS, ROWS), :] = rope(qkv[:, 128:256])
        k_v[rows_of(b), :] = rope(qkv[:, 256:384])
        v_v[rows_of(b), :] = qkv[:, 384:512].astype(BF16)

    def attention(b):
        def tile(j):
            return pl.ds(j * ROWS, ROWS)

        heads = range(2)
        peak, total, shift = [None] * 2, [None] * 2, [None] * 2
        for j in range(b + 1):
            for h in heads:
                q = q_v[pl.ds(h * ROWS, ROWS), :]
                s = lax.dot_general(q, k_v[tile(j), :], (((1,), (1,)), ((), ())), preferred_element_type=F32) * SCORE_SCALE
                if j == b:
                    qpos = lax.broadcasted_iota(jnp.int32, (ROWS, ROWS), 0)
                    kpos = lax.broadcasted_iota(jnp.int32, (ROWS, ROWS), 1)
                    s = jnp.where(kpos <= qpos, s, -1e30)
                s_v[h, :, tile(j)] = s
                pair = jnp.maximum(s[:, :128], s[:, 128:])
                peak[h] = pair if j == 0 else jnp.maximum(peak[h], pair)
                yield
        for h in heads:
            peak[h] = jnp.max(peak[h], axis=1, keepdims=True)
        for j in range(b + 1):
            for h in heads:
                e = jnp.exp2(s_v[h, :, tile(j)] - peak[h])
                pair = e[:, :128] + e[:, 128:]
                total[h] = pair if j == 0 else total[h] + pair
                yield
        for h in heads:
            shift[h] = peak[h] + jnp.log2(jnp.sum(total[h], axis=1, keepdims=True))
        for j in range(b + 1):
            for h in heads:
                p_v[h, :, tile(j)] = jnp.exp2(s_v[h, :, tile(j)] - shift[h]).astype(BF16)
                yield
        keys = pl.ds(0, (b + 1) * ROWS)
        for h in heads:
            o = jnp.dot(p_v[h, :, keys], v_v[keys, :], preferred_element_type=F32)
            om_v[:, pl.ds(h * HEAD_DIM, HEAD_DIM)] = o.astype(BF16)
            yield

    def gate_up(b):
        normed = a_v.at[b % 2]
        for n in range(FFCOLS // 256):
            if b == 0:
                wait_gu[n].wait()
            cols = pl.ds(n * 256, 256)
            gate = jnp.dot(normed[...], wg_v[:, cols], preferred_element_type=F32)
            yield
            up = jnp.dot(normed[...], wu_v[:, cols], preferred_element_type=F32)
            om_v[:, pl.ds(QCOLS + n * 256, 256)] = (gate * (1.0 / (1.0 + jnp.exp(-gate))) * up).astype(BF16)
            yield

    def next_norm(b):
        for r in range(ROWS // 16):
            norm_rows(b + 1, r)
            yield

    def mix_block(b):
        works = [(gate_up(b), [k / 6 for k in range(6)])]
        count = 6 * (b + 1) + 2
        works.append((attention(b), [k / count for k in range(count)]))
        if b == 0:
            for copy in load_od[0]:
                copy.start()
            load_x(1).start()
            for copy in load_od[1]:
                copy.start()
        elif b < BLOCKS - 1:
            count = ROWS // 16
            load_x(b + 1).wait()
            works.append((next_norm(b), [k / count for k in range(count)]))
        turns = sorted((turn, index) for index, (_, turns) in enumerate(works) for turn in turns)
        for _, index in turns:
            next(works[index][0])
        for work, _ in works:
            for _ in work:
                pass
        if b == 0:
            wait_od[0].wait()
        pair_product(0, 1 - p2, b)
        pair_copy(PAIR_PASS, b).start()
        pair_copy(PAIR_STAY, b).start()

    def mix(i):
        for b in range(BLOCKS):
            @pl.when(i == b)
            def _():
                mix_block(b)

    def down(half, quarter):
        cols = pl.ds(pl.multiple_of(half * 1024 + quarter * 512, 512), 512)
        return jnp.dot(om_v[...], wod_v[:, cols], preferred_element_type=F32)

    def pair_product(slot, quarter, b):
        part = down(1 - core, quarter).astype(BF16)
        for s in range(2):
            d2d_src[slot, 2 * b + s] = part[s * HALF:(s + 1) * HALF]

    def down_rest(i):
        def rest(b, first):
            norms = iter(range(ROWS // 16) if first else ())

            def some_norms():
                for _ in range(6):
                    for r in norms:
                        norm_rows(1, r)
                        break

            pair_product(1, p2, b)
            some_norms()
            send_v[...] = down(core, 1 - p1)
            some_norms()
            keep = down(core, p1)
            some_norms()
            for s in range(2):
                h_keep[2 * b + s] = keep[s * HALF:(s + 1) * HALF]
            pair_copy(PAIR_KEEP, b).start()
            for kind, pair, index in ((RED_PASS, PAIR_PASS, 1 - p2), (RED_STAY, PAIR_STAY, p2)):
                with jax.named_scope("recv"):
                    pair_copy(pair, b).wait_recv()
                cols = quarter_cols(index)
                for s in range(2):
                    u = 2 * b + s
                    h_send[u, :, cols] = (send_v[pl.ds(s * HALF, HALF), cols] + d2d_dst[0, u, :, cols].astype(F32)).astype(BF16)
                for s in range(2):
                    copy_of(kind, 2 * b + s).start()

        @pl.when(i == 0)
        def _():
            wait_od[1].wait()
            load_x(1).wait()
            rest(0, True)
            load_tab.start()
            for n in range(2, BLOCKS):
                load_x(n).start()

        @pl.when(i > 0)
        def _():
            rest(i, False)

    def stage_b(u):
        with jax.named_scope("recv"):
            copy_of(RED_PASS, u).wait_recv()
            if u % 2 == 0:
                pair_copy(PAIR_KEEP, u // 2).wait_recv()
        p_send[u] = partial(u, quarter_cols(1 - p2)).astype(BF16)
        copy_of(RED_TWO, u).start()

    def partial(u, cols):
        return h_keep[u, :, cols] + d2d_dst[1, u, :, cols].astype(F32) + r1_dst[u, :, cols].astype(F32)

    def stage_c(u):
        with jax.named_scope("recv"):
            copy_of(RED_STAY, u).wait_recv()
            copy_of(RED_TWO, u).wait_recv()
        cols = quarter_cols(mine + p2)
        x_f = x_v[half_rows(u), cols].astype(F32)
        y_v[half_rows(u), cols] = (x_f + (partial(u, quarter_cols(p2)) + r2_dst[u].astype(F32))).astype(BF16)
        copy_of(GAT_ONE, u).start()
        copy_of(GAT_OWN, u).start()

    def stage_d(u):
        with jax.named_scope("recv"):
            copy_of(GAT_ONE, u).wait_recv()
        copy_of(GAT_PASS, u).start()
        copy_of(OUT_FIRST, u).start()

    def stage_e(u):
        with jax.named_scope("recv"):
            copy_of(GAT_OWN, u).wait_recv()
            copy_of(GAT_PASS, u).wait_recv()
        copy_of(OUT_SECOND, u).start()

    stages = {"b": stage_b, "c": stage_c, "d": stage_d, "e": stage_e}

    slots = {}
    for name in "bcde":
        for u in range(UNITS):
            slots.setdefault(STAGE_SLOTS[name][u], []).append((name, u))

    def communicate(slot):
        for name, u in slots.get(slot, ()):
            with jax.named_scope("stage_" + name):
                stages[name](u)

    def next_project(i):
        @pl.when(i < BLOCKS - 1)
        def _():
            project(i + 1)

    def step(i, carry):
        for point, part in enumerate((mix, down_rest, next_project)):
            with jax.named_scope(part.__name__):
                part(i)
            for b in range(BLOCKS):
                if 3 * b + point in slots:
                    @pl.when(i == b)
                    def _():
                        communicate(3 * b + point)

        return carry

    with jax.named_scope("first"):
        first_norm()
        project(0)
    lax.fori_loop(0, BLOCKS, step, 0)
    for slot in range(3 * BLOCKS, max(slots) + 1):
        communicate(slot)

    with jax.named_scope("finish"):
        for kind in (OUT_FIRST, OUT_SECOND):
            all_of(kind).wait_recv()
        for kind in range(11):
            all_of(kind).wait_send()


def store_kernel(y_v, k_v, v_v, y_out, k_out, v_out, sem):
    copies = [pltpu.make_async_copy(k_v, k_out, sem.at[0]), pltpu.make_async_copy(v_v, v_out, sem.at[1])]
    for b in range(BLOCKS):
        rows = pl.ds(b * ROWS, ROWS)
        copies.append(pltpu.make_async_copy(y_v.at[rows, :], y_out.at[rows, :], sem.at[2 + b]))
    for copy in copies:
        copy.start()
    for copy in copies:
        copy.wait()


def solution(mesh):
    table = rope_table()

    def local_layer(x_in, g_norm, w_q, w_k, w_v, w_o, w_gate, w_up, w_down):
        any_spec = pl.BlockSpec(memory_space=pl.ANY)
        y, k, v = pl.pallas_call(
            layer_kernel,
            out_shape=(pltpu.VMEM((TOKENS, WIDTH), BF16), pltpu.VMEM((TOKENS, HEAD_DIM), BF16), pltpu.VMEM((TOKENS, HEAD_DIM), BF16)),
            in_specs=[any_spec] * 10,
            out_specs=(pl.BlockSpec(memory_space=pltpu.VMEM),) * 3,
            scratch_shapes=[
                pltpu.VMEM((TOKENS, WIDTH), BF16),
                pltpu.VMEM((WIDTH,), BF16),
                pltpu.VMEM((8, WIDTH), F32),
                pltpu.VMEM((WIDTH, QCOLS + 2 * HEAD_DIM), BF16),
                pltpu.VMEM((WIDTH, FFCOLS), BF16),
                pltpu.VMEM((WIDTH, FFCOLS), BF16),
                pltpu.VMEM((KDOWN, WIDTH), BF16),
                pltpu.VMEM((TOKENS, HEAD_DIM), F32),
                pltpu.VMEM((2, ROWS, WIDTH), BF16),
                pltpu.VMEM((2 * ROWS, HEAD_DIM), BF16),
                pltpu.VMEM((2, ROWS, TOKENS), F32),
                pltpu.VMEM((2, ROWS, TOKENS), BF16),
                pltpu.VMEM((ROWS, KDOWN), BF16),
                pltpu.VMEM((2, UNITS, HALF, 512), BF16),
                pltpu.VMEM((2, UNITS, HALF, 512), BF16),
                pltpu.VMEM((UNITS, HALF, 512), BF16),
                pltpu.VMEM((UNITS, HALF, 512), F32),
                pltpu.VMEM((UNITS, HALF, 512), BF16),
                pltpu.VMEM((UNITS, HALF, 256), BF16),
                pltpu.VMEM((UNITS, HALF, 256), BF16),
                pltpu.VMEM((ROWS, 512), F32),
                pltpu.SemaphoreType.DMA((BLOCKS + 3,)),
                pltpu.SemaphoreType.DMA((9,)),
                pltpu.SemaphoreType.DMA((11,)),
                pltpu.SemaphoreType.DMA((3, BLOCKS)),
                pltpu.SemaphoreType.DMA((6, UNITS)),
                pltpu.SemaphoreType.DMA((2,)),
            ],
            compiler_params=pltpu.CompilerParams(collective_id=0, has_side_effects=True, vmem_limit_bytes=67043328 - 8 * 1024 * 1024),
        )(x_in, g_norm, w_q, w_k, w_v, w_o, w_gate, w_up, w_down, jnp.asarray(table))
        y, k, v = pl.pallas_call(
            store_kernel,
            out_shape=(jax.ShapeDtypeStruct((TOKENS, WIDTH), BF16), jax.ShapeDtypeStruct((TOKENS, HEAD_DIM), BF16),
                       jax.ShapeDtypeStruct((TOKENS, HEAD_DIM), BF16)),
            in_specs=[any_spec] * 3,
            out_specs=(any_spec,) * 3,
            scratch_shapes=[pltpu.SemaphoreType.DMA((2 + BLOCKS,))],
            compiler_params=pltpu.CompilerParams(vmem_limit_bytes=1024 * 1024),
        )(*(pltpu.with_memory_space_constraint(part, pltpu.VMEM) for part in (y, k, v)))
        return y, k.reshape(TOKENS, 1, HEAD_DIM), v.reshape(TOKENS, 1, HEAD_DIM)

    return jax.shard_map(local_layer, mesh=mesh, in_specs=(P('dp', None), P(None), P(None, 'tp'), P(None, None), P(None, None), P('tp', None), P(None, 'tp'), P(None, 'tp'), P('tp', None)), out_specs=(P('dp', None), P('dp', 'tp', None), P('dp', 'tp', None)), check_vma=False)
```
